256 devices in a mesh: dp: 16 (over z_hi, x), blk: 16 (over y, z_lo, core).
Axes of the slice: x: 4, y: 4, z: 8 (z_hi: 4, z_lo: 2; z = z_hi * 2 + z_lo), core: 2. Of those that a mesh axis runs over, the one named last changes fastest.
Arguments:
- queries: bfloat16 [16, 2048, 2048], P('dp', 'blk'), may hold values from -6 to 6
- keys: bfloat16 [16, 2048, 512], P('dp', 'blk'), may hold values from -6 to 6
- values: bfloat16 [16, 2048, 512], P('dp', 'blk'), may hold values from -6 to 6
- out_grad: bfloat16 [16, 2048, 2048], P('dp', 'blk'), may hold values from -6 to 6
- layer_input: bfloat16 [16, 2048, 4096], P('dp', 'blk'), may hold values from -6 to 6
- lengths: int32 [16, 3], P('dp'), may hold values from 128 to 1792, as said below
Outputs:
- query_grad: bfloat16 [16, 2048, 2048], P('dp', 'blk')
- key_grad: bfloat16 [16, 2048, 512], P('dp', 'blk')
- value_grad: bfloat16 [16, 2048, 512], P('dp', 'blk')
- weight_grad: float32 [4096, 1024], P(('dp', 'blk'))
The draws below stay inside these ranges and needn't reach their ends.
Inputs may be any that keep to these rules, and one draw needn't show every extreme that they name: `lengths`: each row sums to 2048; the chosen and rejected counts lie between 128 and 384.
All inputs are finite; a program needn't handle non-finite values.
Results may differ from the reference program's by a relative error of at most 0.023.
Values may be sent and summed in bfloat16 or wider, within the bound.
A program may use at most 128 MiB of HBM per device.

```python
import math
import jax
import jax.numpy as jnp
from jax import lax

D = 4096
H = 16
KV = 4
HEAD = 128
TOK_DEV = 128
SEQ_LEN = 2048
SEQS = 16
N_BLK = 16


def draw_queries(key, part):
    own_key = jax.random.fold_in(key, 1)
    normal_key = jax.random.fold_in(own_key, 0)
    values_drawn = jax.random.normal(normal_key, (SEQS, SEQ_LEN, H * HEAD), jnp.float32)
    return jnp.clip(values_drawn, -6.0, 6.0).astype(jnp.bfloat16)


def draw_keys(key, part):
    own_key = jax.random.fold_in(key, 2)
    normal_key = jax.random.fold_in(own_key, 0)
    values_drawn = jax.random.normal(normal_key, (SEQS, SEQ_LEN, KV * HEAD), jnp.float32)
    return jnp.clip(values_drawn, -6.0, 6.0).astype(jnp.bfloat16)


def draw_lengths(key, part):
    first_key, second_key = jax.random.split(jax.random.fold_in(key, 5))
    lowest = SEQ_LEN // 16
    highest = 3 * SEQ_LEN // 16 + 1
    chosen_len = jax.random.randint(first_key, (SEQS,), lowest, highest)
    rejected_len = jax.random.randint(second_key, (SEQS,), lowest, highest)
    prompt_len = SEQ_LEN - chosen_len - rejected_len
    return jnp.stack([prompt_len, chosen_len, rejected_len], axis=1).astype(jnp.int32)


def block_levels(key, dims, pieces, least, top_value):
    def one(axis_at, parts):
        draws = jax.random.uniform(jax.random.fold_in(jax.random.fold_in(key, 6), axis_at), (parts,), jnp.float32, least / len(pieces), top_value / len(pieces))
        return jnp.repeat(jnp.exp(draws), dims[axis_at] // parts).reshape((-1,) + (1,) * (len(dims) - axis_at - 1))

    loudness = one(*pieces[0])
    for cut in pieces[1:]:
        loudness = loudness * one(*cut)
    return loudness


def normal_values(rng, shape, deviation, bound, cuts=(), kind=jnp.bfloat16):
    level = block_levels(rng, shape, cuts, -0.22, 0.18) if cuts else 1.0
    entries = jax.random.normal(rng, shape, jnp.float32) * deviation * level
    return jnp.minimum(jnp.maximum(entries, -bound), bound).astype(kind)


def setup_inputs(seed: int = 0) -> dict:
    key_list = jax.random.split(jax.random.key(seed), 7)
    return {
        "queries": draw_queries(jax.random.fold_in(key_list[6], 71), 0),
        "keys": draw_keys(jax.random.fold_in(key_list[6], 71), 0),
        "values": normal_values(key_list[2], (SEQS, SEQ_LEN, KV * HEAD), 1.0, 6.0, ((0, 16), (1, 16))),
        "out_grad": normal_values(key_list[3], (SEQS, SEQ_LEN, H * HEAD), 1.0, 6.0, ((0, 16), (1, 16))),
        "layer_input": normal_values(key_list[4], (SEQS, SEQ_LEN, D), 1.0, 6.0, ((0, 16), (1, 16))),
        "lengths": draw_lengths(jax.random.fold_in(key_list[6], 71), 0),
    }


rope_base = 500000.0
masked_fill = -1e+30

def stored_positions(stored_rows, shard_rows, shard_count):
    half_rows = shard_rows // 2
    block_number = stored_rows // half_rows
    holder = block_number // 2
    upper_half = block_number % 2
    position_block = jnp.where(upper_half == 1, 2 * shard_count - 1 - holder, holder)
    return (position_block * half_rows + stored_rows % half_rows).astype(jnp.int32)

def allowed_pairs(query_pos, key_pos, prompt_len, chosen_len):
    causal = key_pos[None, :] <= query_pos[:, None]
    reject_start = prompt_len + chosen_len
    query_rejected = query_pos >= reject_start
    key_chosen = jnp.logical_and(key_pos >= prompt_len, key_pos < reject_start)
    return jnp.logical_and(causal, jnp.logical_not(jnp.logical_and(query_rejected[:, None], key_chosen[None, :])))

def rope_inverse(grad_sum, positions):
    half_dim = HEAD // 2
    frequency = jnp.exp(-(2.0 * jnp.arange(half_dim, dtype=jnp.float32) / HEAD) * math.log(rope_base))
    angles = positions.astype(jnp.float32)[:, None] * frequency[None, :]
    cosine = jnp.concatenate([jnp.cos(angles), jnp.cos(angles)], axis=-1)[:, None, :]
    sine = jnp.concatenate([jnp.sin(angles), jnp.sin(angles)], axis=-1)[:, None, :]
    grad_heads = grad_sum.reshape(grad_sum.shape[0], -1, HEAD)
    rotated = jnp.concatenate([-grad_heads[..., half_dim:], grad_heads[..., :half_dim]], axis=-1)
    return (grad_heads * cosine - rotated * sine).reshape(grad_sum.shape[0], -1).astype(jnp.bfloat16)

def one_sequence(operands):
    queries, keys, values, out_grad, lengths = operands
    seq_len = queries.shape[0]
    group_heads = H // KV
    scale = 1.0 / math.sqrt(HEAD)
    positions = stored_positions(jnp.arange(seq_len, dtype=jnp.int32), TOK_DEV, N_BLK)
    allowed = allowed_pairs(positions, positions, lengths[0], lengths[1])
    query_heads = queries.reshape(seq_len, KV, group_heads, HEAD).transpose(1, 2, 0, 3).astype(jnp.float32)
    grad_heads = out_grad.reshape(seq_len, KV, group_heads, HEAD).transpose(1, 2, 0, 3).astype(jnp.float32)
    key_heads = keys.reshape(seq_len, KV, HEAD).transpose(1, 0, 2).astype(jnp.float32)
    value_heads = values.reshape(seq_len, KV, HEAD).transpose(1, 0, 2).astype(jnp.float32)

    def one_group(group_operands):
        group_query, group_key, group_value, group_grad = group_operands
        scores = scale * jnp.einsum('hqe,ke->hqk', group_query, group_key)
        row_max = lax.optimization_barrier(jnp.max(jnp.where(allowed[None], scores, masked_fill), axis=-1))
        weights = jnp.where(allowed[None], jnp.exp(scores - row_max[..., None]), 0.0)
        row_sum = lax.optimization_barrier(jnp.sum(weights, axis=-1))
        attn_out = jnp.einsum('hqk,ke->hqe', weights, group_value, precision=lax.Precision.HIGHEST) / row_sum[..., None]
        log_total = row_max + jnp.log(row_sum)
        delta = lax.optimization_barrier(jnp.sum(group_grad * attn_out, axis=-1))
        probs = jnp.where(allowed[None], jnp.exp(scores - log_total[..., None]), 0.0)
        prob_half = probs.astype(jnp.bfloat16)
        prob_grad = jnp.einsum('hqe,ke->hqk', group_grad, group_value)
        score_grad = (scale * probs * (prob_grad - delta[..., None])).astype(jnp.bfloat16)
        query_grad = jnp.einsum('hqk,ke->hqe', score_grad.astype(jnp.float32), group_key)
        score_shards = score_grad.astype(jnp.float32).reshape(group_heads, N_BLK, TOK_DEV, seq_len)
        prob_shards = prob_half.astype(jnp.float32).reshape(group_heads, N_BLK, TOK_DEV, seq_len)
        query_shards = group_query.reshape(group_heads, N_BLK, TOK_DEV, HEAD)
        grad_shards = group_grad.reshape(group_heads, N_BLK, TOK_DEV, HEAD)
        key_parts = lax.optimization_barrier(jnp.einsum('hdqk,hdqe->dke', score_shards, query_shards).astype(jnp.bfloat16))
        value_parts = lax.optimization_barrier(jnp.einsum('hdqk,hdqe->dke', prob_shards, grad_shards).astype(jnp.bfloat16))
        key_sum = lax.optimization_barrier(jnp.sum(key_parts.astype(jnp.float32), axis=0))
        value_sum = lax.optimization_barrier(jnp.sum(value_parts.astype(jnp.float32), axis=0))
        return (query_grad, key_sum, value_sum)
    query_grad, key_sum, value_sum = lax.map(one_group, (query_heads, key_heads, value_heads, grad_heads))
    query_grad = query_grad.transpose(2, 0, 1, 3).reshape(seq_len, H * HEAD).astype(jnp.bfloat16)
    key_sum = key_sum.transpose(1, 0, 2).reshape(seq_len, KV * HEAD)
    value_sum = value_sum.transpose(1, 0, 2).reshape(seq_len, KV * HEAD)
    key_pre = rope_inverse(key_sum, positions)
    value_grad = value_sum.astype(jnp.bfloat16)
    grad_cols = jnp.concatenate([key_pre, value_grad], axis=1)
    return (query_grad, key_sum.astype(jnp.bfloat16), value_grad, grad_cols)

def reference(queries, keys, values, out_grad, layer_input, lengths):
    query_grad, key_grad, value_grad, grad_cols = lax.map(one_sequence, (queries, keys, values, out_grad, lengths))
    features = layer_input.shape[2]
    weight_grad = jnp.dot(layer_input.reshape(-1, features).T, grad_cols.reshape(-1, grad_cols.shape[2]), preferred_element_type=jnp.float32)
    return (query_grad, key_grad, value_grad, weight_grad)
```

```python
import math

import jax
import jax.numpy as jnp
from jax import lax
from jax.experimental import pallas as pl
from jax.experimental.pallas import tpu as pltpu
from jax.sharding import PartitionSpec as P

MESH = pl.DeviceIdType.MESH
F32 = jnp.float32
BF16 = jnp.bfloat16
HEAD = 128
ROPE_BASE = 500000.0
MASKED = -1e30
FAR = 1 << 20
COPIES = 64
LOCALS = 16


def nn(a, b):
    return jnp.dot(a, b, preferred_element_type=F32)


def nt(a, b):
    return lax.dot_general(a, b, (((1,), (1,)), ((), ())), preferred_element_type=F32)


def kernel(
    len_ref, q_in, do_in, k_in, v_in, x_in,
    dq_out, dk_out, dv_out, w_out,
    qbuf, dobuf, kv, xv, xt, xbuf, qs, dos, kt, s_scr, dp_scr, p_t, ds_t, dqacc, dqbuf,
    dkvf, dkvb, ra, rb, rm, rp, gbuf, dkbuf, cosb, sinb, wacc, wb1, r1, wb2, r2, wfin,
    send, recv, loc,
):
    b = lax.axis_index("blk")
    dp = lax.axis_index("dp")
    y, w = b // 4, b % 4
    core = w % 2
    zhi, xx = dp // 4, dp % 4
    yp, y2, ym = (y + 1) % 4, (y + 2) % 4, (y + 3) % 4
    scale = 1.0 / math.sqrt(HEAD)
    prompt_len = len_ref[0]
    reject_start = len_ref[0] + len_ref[1]

    count = [0, 0]
    pending = []

    def remote(src, dst, device):
        i = count[0]
        count[0] += 1
        copy = pltpu.make_async_remote_copy(
            src_ref=src, dst_ref=dst, send_sem=send.at[i], recv_sem=recv.at[i],
            device_id=device, device_id_type=MESH,
        )
        copy.start()
        pending.append(copy)
        return copy

    def local(src, dst):
        i = count[1]
        count[1] += 1
        copy = pltpu.make_async_copy(src, dst, loc.at[i])
        copy.start()
        return copy

    def at_blk(yy, ww):
        return {"blk": 4 * yy + ww}

    def tile(i, size):
        return pl.ds(pl.multiple_of(i * size, size), size)

    barrier = pltpu.get_barrier_semaphore()
    for d in range(1, 4):
        pl.semaphore_signal(barrier, 1, device_id=at_blk(y, (w + d) % 4), device_id_type=MESH)
        pl.semaphore_signal(barrier, 1, device_id=at_blk((y + d) % 4, w), device_id_type=MESH)
        pl.semaphore_signal(
            barrier, 1, device_id={"dp": 4 * zhi + (xx + d) % 4}, device_id_type=MESH
        )
        pl.semaphore_signal(
            barrier, 1, device_id={"dp": 4 * ((zhi + d) % 4) + xx}, device_id_type=MESH
        )
    x_local = local(x_in, xv)
    kv_slots = (tile(4 * y + w, 64), tile(4 * (7 - y) + 3 - w, 64))
    own_kv = []
    for half in range(2):
        for part, ref in ((0, k_in), (1, v_in)):
            own_kv.append(
                local(
                    ref.at[pl.ds(64 * half, 64), tile(w, 128)],
                    kv.at[kv_slots[half], pl.ds(128 * part, 128)],
                )
            )
    own_q = [
        local(q_in.at[:, tile(w, 512)], qbuf.at[w]),
        local(do_in.at[:, tile(w, 512)], dobuf.at[w]),
    ]
    pl.semaphore_wait(barrier, 12)

    kv_first = []
    for d in (2, 1, 3):
        ww = (w + d) % 4
        for half in range(2):
            for part, ref in ((0, k_in), (1, v_in)):
                kv_first.append(
                    remote(
                        ref.at[pl.ds(64 * half, 64), tile(ww, 128)],
                        kv.at[kv_slots[half], pl.ds(128 * part, 128)],
                        at_blk(y, ww),
                    )
                )
    q_first = []
    for d in (2, 1, 3):
        ww = (w + d) % 4
        q_first.append(remote(q_in.at[:, tile(ww, 512)], qbuf.at[w], at_blk(y, ww)))
        q_first.append(remote(do_in.at[:, tile(ww, 512)], dobuf.at[w], at_blk(y, ww)))

    x_local.wait()

    def transpose_x(i, carry):
        block = xv[:, tile(i, 128)].T.reshape(2, 64, 128)
        xt[i // 2, pl.ds((i % 2) * 2, 2)] = block
        return carry

    lax.fori_loop(0, 32, transpose_x, 0)

    for copy in own_kv:
        copy.wait()
    for copy in kv_first:
        copy.wait_recv()
    kv_plus, kv_minus = [], []
    for yy, group in ((yp, kv_plus), (ym, kv_minus)):
        for slot in (tile(y, 256), tile(7 - y, 256)):
            group.append(remote(kv.at[slot], kv.at[slot], at_blk(yy, w)))
    column = tile(w, 128)
    x_first = []
    for d in (2, 1, 3):
        yy = (y + d) % 4
        x_first.append(remote(xt.at[:, yy], xbuf.at[y, :, :, column], at_blk(yy, w)))
    xbuf[y, :, :, column] = xt[:, y]

    lane_row = lax.broadcasted_iota(jnp.int32, (1, HEAD), 1)
    frequency = jnp.exp(
        -(2.0 * (lane_row % 64).astype(F32) / HEAD) * math.log(ROPE_BASE)
    )
    for half, block in ((0, y), (1, 7 - y)):
        position = 256 * block + lax.broadcasted_iota(jnp.int32, (256, HEAD), 0)
        angles = position.astype(F32) * frequency
        cosb[half] = jnp.cos(angles)
        sinb[half] = jnp.where(lane_row < 64, jnp.sin(angles), -jnp.sin(angles))

    for copy in kv_plus:
        copy.wait_recv()
    slot = tile(ym, 256)
    kv_second = [remote(kv.at[slot], kv.at[slot], at_blk(yp, w))]
    for copy in kv_minus:
        copy.wait_recv()
    slot = tile(7 - yp, 256)
    kv_second.append(remote(kv.at[slot], kv.at[slot], at_blk(ym, w)))

    for copy in own_q:
        copy.wait()
    for copy in q_first:
        copy.wait_recv()

    def stack(c, carry):
        half, h = c // 4, c % 4
        for ww in range(4):
            qs[c, pl.ds(64 * ww, 64)] = qbuf[ww, tile(half, 64), tile(h, 128)]
            dos[c, pl.ds(64 * ww, 64)] = dobuf[ww, tile(half, 64), tile(h, 128)]
        return carry

    lax.fori_loop(0, 8, stack, 0)

    for copy in kv_second:
        copy.wait_recv()

    def transpose_k(j, carry):
        kt[j] = kv[tile(j, 256), pl.ds(0, 128)].T
        return carry

    lax.fori_loop(0, 8, transpose_k, 0)

    for copy in x_first:
        copy.wait_recv()
    core_mate = at_blk(y, w + 1 - 2 * core)
    z_mate = at_blk(y, (w + 2) % 4)
    x_second = [
        remote(xbuf.at[:, :, :, column], xbuf.at[:, :, :, column], z_mate),
        remote(xbuf.at[:, :, :, column], xbuf.at[:, :, :, column], core_mate),
    ]

    lane = lax.broadcasted_iota(jnp.int32, (1, 256), 1)
    lane_high = (3 - lane // 64) * 64 + lane % 64
    rows = lax.broadcasted_iota(jnp.int32, (256, 256), 0)

    def chunk(c, carry):
        half, h = c // 4, c % 4
        diagonal = y + half * (7 - 2 * y)
        blocks = diagonal + 1
        query_pos = 256 * diagonal + lane + half * (lane_high - lane)
        rejected = query_pos >= reject_start
        query = qs[c]
        grad = dos[c]
        columns = tile(c, 256)

        def scores(j, top):
            s = nt(kv[tile(j, 256), pl.ds(0, 128)], query)
            key_pos = 256 * j + rows
            chosen = jnp.logical_and(key_pos >= prompt_len, key_pos < reject_start)
            shown = jnp.where(rejected, jnp.where(chosen, FAR, key_pos), key_pos)
            s = jnp.where(shown <= query_pos, s, MASKED)
            s_scr[j] = s
            return jnp.maximum(top, jnp.max(s.reshape(32, 8, 256), axis=0))

        top = lax.fori_loop(0, blocks, scores, jnp.full((8, 256), MASKED, F32))
        top = jnp.max(top, axis=0, keepdims=True)

        def weights(j, sums):
            total, dot_total = sums
            p = jnp.exp((s_scr[j] - top) * scale)
            d = nt(kv[tile(j, 256), pl.ds(128, 128)], grad)
            s_scr[j] = p
            dp_scr[j] = d
            total = total + jnp.sum(p.reshape(32, 8, 256), axis=0)
            dot_total = dot_total + jnp.sum((p * d).reshape(32, 8, 256), axis=0)
            return total, dot_total

        zero = jnp.zeros((8, 256), F32)
        total, dot_total = lax.fori_loop(0, blocks, weights, (zero, zero))
        inverse = 1.0 / jnp.sum(total, axis=0, keepdims=True)
        delta = jnp.sum(dot_total, axis=0, keepdims=True) * inverse
        dqacc[...] = jnp.zeros_like(dqacc)

        def gradients(j, carry):
            p = s_scr[j] * inverse
            ds = ((scale * p) * (dp_scr[j] - delta)).astype(BF16)
            p_t[j, :, columns] = p.astype(BF16)
            ds_t[j, :, columns] = ds
            dqacc[...] += nn(kt[j], ds)
            return carry

        lax.fori_loop(0, blocks, gradients, 0)
        dq = dqacc[...].T.astype(BF16)
        for ww in range(4):
            dqbuf[ww, tile(half, 64), tile(h, 128)] = dq[64 * ww : 64 * ww + 64]
        return carry

    lax.fori_loop(0, 8, chunk, 0)

    own_out, far_out = [local(dqbuf.at[w], dq_out.at[:, tile(w, 512)])], []
    for d in (2, 1, 3):
        ww = (w + d) % 4
        far_out.append(remote(dqbuf.at[ww], dq_out.at[:, tile(w, 512)], at_blk(y, ww)))

    def key_block(j):
        def product(half):
            lanes = pl.ds(1024 * half, 1024)
            dk = nn(ds_t[j, :, lanes], qs[pl.ds(4 * half, 4)].reshape(1024, 128))
            dv = nn(p_t[j, :, lanes], dos[pl.ds(4 * half, 4)].reshape(1024, 128))
            return dk, dv

        @pl.when(j <= 7 - y)
        def _():
            dk, dv = product(1)
            dkvf[j, :, pl.ds(0, 128)] = dk
            dkvf[j, :, pl.ds(128, 128)] = dv

        @pl.when(j > 7 - y)
        def _():
            dkvf[j] = jnp.zeros((256, 256), F32)

        @pl.when(j <= y)
        def _():
            dk, dv = product(0)
            dkvf[j, :, pl.ds(0, 128)] += dk
            dkvf[j, :, pl.ds(128, 128)] += dv

    def key_blocks(yy):
        def one(half, carry):
            key_block(yy + half * (7 - 2 * yy))
            return carry

        lax.fori_loop(0, 2, one, 0)

    key_blocks(y2)
    for j in (y2, 7 - y2):
        dkvb[j] = dkvf[j].astype(BF16)
    far_plus = remote(dkvb.at[y2], ra, at_blk(yp, w))
    far_minus = remote(dkvb.at[7 - y2], rb, at_blk(ym, w))
    key_blocks(yp)
    far_plus.wait_recv()
    dkvb[yp] = (dkvf[yp] + ra[...].astype(F32)).astype(BF16)
    dkvb[7 - yp] = dkvf[7 - yp].astype(BF16)
    near = [
        remote(dkvb.at[yp], rm.at[0], at_blk(yp, w)),
        remote(dkvb.at[7 - yp], rm.at[1], at_blk(yp, w)),
    ]
    key_blocks(ym)
    far_minus.wait_recv()
    dkvb[ym] = dkvf[ym].astype(BF16)
    dkvb[7 - ym] = (dkvf[7 - ym] + rb[...].astype(F32)).astype(BF16)
    near.append(remote(dkvb.at[ym], rp.at[0], at_blk(ym, w)))
    near.append(remote(dkvb.at[7 - ym], rp.at[1], at_blk(ym, w)))
    key_blocks(y)

    x_second[0].wait_recv()
    other = tile((w + 2) % 4, 128)
    x_third = remote(xbuf.at[:, :, :, other], xbuf.at[:, :, :, other], core_mate)

    for copy in near:
        copy.wait_recv()
    for half, j in ((0, y), (1, 7 - y)):
        total = dkvf[j] + rm[half].astype(F32) + rp[half].astype(F32)
        key_sum = total[:, :128]
        value_grad = total[:, 128:].astype(BF16)
        key_grad = key_sum.astype(BF16)
        key_pre = (
            key_sum * cosb[half] + pltpu.roll(key_sum, 64, 1) * sinb[half]
        ).astype(BF16)
        for ww in range(4):
            at = 64 * ww if half == 0 else 64 * (3 - ww)
            dst = pl.ds(128 * ww + 64 * half, 64)
            gbuf[y, dst, pl.ds(0, 128)] = key_pre[at : at + 64]
            gbuf[y, dst, pl.ds(128, 128)] = value_grad[at : at + 64]
            dkbuf[ww, pl.ds(64 * half, 64)] = key_grad[at : at + 64]

    g_near = [
        remote(gbuf.at[y], gbuf.at[y], at_blk(yp, w)),
        remote(gbuf.at[y], gbuf.at[y], at_blk(ym, w)),
    ]
    own_out.append(local(dkbuf.at[w], dk_out.at[:, column]))
    own_out.append(local(gbuf.at[y, tile(w, 128), pl.ds(128, 128)], dv_out.at[:, column]))
    for d in (2, 1, 3):
        ww = (w + d) % 4
        far_out.append(remote(dkbuf.at[ww], dk_out.at[:, column], at_blk(y, ww)))
        far_out.append(
            remote(
                gbuf.at[y, tile(ww, 128), pl.ds(128, 128)], dv_out.at[:, column], at_blk(y, ww)
            )
        )

    x_second[1].wait_recv()
    x_third.wait_recv()

    def weight_rows(yy, x_at):
        left = [xbuf[yy, 4 * k + x_at] for k in range(4)]
        return nn(jnp.concatenate(left, axis=0), gbuf[yy])

    def first_rows(i, carry):
        wacc[i] = weight_rows(y, i)
        return carry

    lax.fori_loop(0, 4, first_rows, 0)
    g_near[0].wait_recv()
    g_far = [remote(gbuf.at[ym, pl.ds(0, 256)], gbuf.at[ym, pl.ds(0, 256)], at_blk(yp, w))]
    g_near[1].wait_recv()
    g_far.append(
        remote(gbuf.at[yp, pl.ds(256, 256)], gbuf.at[yp, pl.ds(256, 256)], at_blk(ym, w))
    )

    def more_rows(i, carry):
        wacc[i] += weight_rows(ym, i)
        wacc[i] += weight_rows(yp, i)
        return carry

    lax.fori_loop(0, 4, more_rows, 0)
    for copy in g_far:
        copy.wait_recv()
    x_sums = []
    for d in (2, 1, 3):
        x_at = (xx + d) % 4
        wb1[x_at] = (wacc[x_at] + weight_rows(y2, x_at)).astype(BF16)
        x_sums.append(remote(wb1.at[x_at], r1.at[d - 1], {"dp": 4 * zhi + x_at}))
    mine = wacc[xx] + weight_rows(y2, xx)
    for copy in x_sums:
        copy.wait_recv()
    for d in range(3):
        mine = mine + r1[d].astype(F32)
    wacc[0] = mine
    wb2[...] = mine.astype(BF16)
    z_sums = []
    for d in (2, 1, 3):
        z_at = (zhi + d) % 4
        z_sums.append(remote(wb2.at[tile(z_at, 64)], r2.at[d - 1], {"dp": 4 * z_at + xx}))
    total = wacc[0, tile(zhi, 64)]
    for copy in z_sums:
        copy.wait_recv()
    for d in range(3):
        total = total + r2[d].astype(F32)
    wfin[...] = total.reshape(4, 16, 256)
    for part in range(2):
        lanes = pl.ds(128 * part, 128)
        dst = w_out.at[:, tile(4 * part + w, 128)]
        own_out.append(local(wfin.at[w, :, lanes], dst))
        for d in (2, 1, 3):
            ww = (w + d) % 4
            far_out.append(remote(wfin.at[ww, :, lanes], dst, at_blk(y, ww)))
    for copy in own_out:
        copy.wait()
    for copy in far_out:
        copy.wait_recv()
    for copy in pending:
        copy.wait_send()


def body(queries, keys, values, out_grad, layer_input, lengths):
    seq = 2048
    anywhere = pl.BlockSpec(memory_space=pltpu.HBM)
    vmem = pltpu.VMEM
    outs = pl.pallas_call(
        kernel,
        out_shape=(
            jax.ShapeDtypeStruct((128, 2048), BF16),
            jax.ShapeDtypeStruct((128, 512), BF16),
            jax.ShapeDtypeStruct((128, 512), BF16),
            jax.ShapeDtypeStruct((16, 1024), F32),
        ),
        in_specs=[pl.BlockSpec(memory_space=pltpu.SMEM)] + [anywhere] * 5,
        out_specs=(anywhere,) * 4,
        scratch_shapes=[
            vmem((4, 128, 512), BF16),
            vmem((4, 128, 512), BF16),
            vmem((2048, 256), BF16),
            vmem((128, 4096), BF16),
            vmem((16, 4, 64, 128), BF16),
            vmem((4, 16, 64, 512), BF16),
            vmem((8, 256, 128), BF16),
            vmem((8, 256, 128), BF16),
            vmem((8, 128, 256), BF16),
            vmem((8, 256, 256), F32),
            vmem((8, 256, 256), F32),
            vmem((8, 256, seq), BF16),
            vmem((8, 256, seq), BF16),
            vmem((128, 256), F32),
            vmem((4, 128, 512), BF16),
            vmem((8, 256, 256), F32),
            vmem((8, 256, 256), BF16),
            vmem((256, 256), BF16),
            vmem((256, 256), BF16),
            vmem((2, 256, 256), BF16),
            vmem((2, 256, 256), BF16),
            vmem((4, 512, 256), BF16),
            vmem((4, 128, 128), BF16),
            vmem((2, 256, 128), F32),
            vmem((2, 256, 128), F32),
            vmem((4, 256, 256), F32),
            vmem((4, 256, 256), BF16),
            vmem((3, 256, 256), BF16),
            vmem((256, 256), BF16),
            vmem((3, 64, 256), BF16),
            vmem((4, 16, 256), F32),
            pltpu.SemaphoreType.DMA((COPIES,)),
            pltpu.SemaphoreType.DMA((COPIES,)),
            pltpu.SemaphoreType.DMA((LOCALS,)),
        ],
        compiler_params=pltpu.CompilerParams(
            collective_id=0, has_side_effects=True, vmem_limit_bytes=60 * 1024 * 1024
        ),
        name="attention_backward",
    )(lengths[0], queries[0], out_grad[0], keys[0], values[0], layer_input[0])
    return (outs[0][None], outs[1][None], outs[2][None], outs[3])


def solution(mesh):
    placed = (P("dp", "blk", None),) * 5 + (P("dp", None),)
    return jax.shard_map(
        body,
        mesh=mesh,
        in_specs=placed,
        out_specs=(P("dp", "blk", None),) * 3 + (P(("dp", "blk"), None),),
        check_vma=False,
    )
```

```python
import math

import jax
import jax.numpy as jnp
from jax import lax
from jax.experimental import pallas as pl
from jax.experimental.pallas import tpu as pltpu
from jax.sharding import PartitionSpec as P

MESH = pl.DeviceIdType.MESH
F32 = jnp.float32
BF16 = jnp.bfloat16
HEAD = 128
ROPE_BASE = 500000.0
MASKED = -1e30
FAR = 1 << 20
COPIES = 128
LOCALS = 16


def nn(a, b):
    return jnp.dot(a, b, preferred_element_type=F32)


def nt(a, b):
    return lax.dot_general(a, b, (((1,), (1,)), ((), ())), preferred_element_type=F32)


def kernel(
    len_ref, q_in, do_in, k_in, v_in, x_in,
    dq_out, dk_out, dv_out, w_out,
    qbuf, dobuf, kv, xv, xt, xbuf, qs, dos, qsn, dosn, kt, p_f, dp_s, p_t, ds_t, inv_s, dqacc,
    dqbuf, part_f, part_b, far_a, far_b, near_m, near_p, gbuf, dkbuf, cosb, sinb, wacc, wb1, r1,
    r2, w_stage, send, recv, loc,
):
    b = lax.axis_index("blk")
    dp = lax.axis_index("dp")
    y, w = b // 4, b % 4
    core = w % 2
    zhi, xx = dp // 4, dp % 4
    yp, y2, ym = (y + 1) % 4, (y + 2) % 4, (y + 3) % 4
    scale = 1.0 / math.sqrt(HEAD)
    prompt_len = len_ref[0]
    reject_start = len_ref[0] + len_ref[1]

    count = [0, 0]
    pending = []

    def remote(src, dst, device):
        i = count[0]
        count[0] += 1
        copy = pltpu.make_async_remote_copy(
            src_ref=src, dst_ref=dst, send_sem=send.at[i], recv_sem=recv.at[i],
            device_id=device, device_id_type=MESH,
        )
        copy.start()
        pending.append(copy)
        return copy

    def local(src, dst):
        i = count[1]
        count[1] += 1
        copy = pltpu.make_async_copy(src, dst, loc.at[i])
        copy.start()
        return copy

    def at_blk(yy, ww):
        return {"blk": 4 * yy + ww}

    def at_owner(zz, ww):
        return {"dp": 4 * zz + xx, "blk": 4 * y + ww}

    def tile(i, size):
        return pl.ds(pl.multiple_of(i * size, size), size)

    barrier = pltpu.get_barrier_semaphore()
    for d in range(1, 4):
        for device in (at_blk((y + d) % 4, w), {"dp": 4 * zhi + (xx + d) % 4}):
            pl.semaphore_signal(barrier, 1, device_id=device, device_id_type=MESH)
    for dz in range(4):
        for d in range(4):
            if dz or d:
                pl.semaphore_signal(
                    barrier, 1, device_id=at_owner((zhi + dz) % 4, (w + d) % 4),
                    device_id_type=MESH,
                )
    x_local = local(x_in, xv)
    kv_slots = (tile(4 * y + w, 64), tile(4 * (7 - y) + 3 - w, 64))
    own_kv = []
    for half in range(2):
        for part, ref in ((0, k_in), (1, v_in)):
            own_kv.append(
                local(
                    ref.at[pl.ds(64 * half, 64), tile(w, 128)],
                    kv.at[kv_slots[half], pl.ds(128 * part, 128)],
                )
            )
    own_q = [
        local(q_in.at[:, tile(w, 512)], qbuf.at[w]),
        local(do_in.at[:, tile(w, 512)], dobuf.at[w]),
    ]
    pl.semaphore_wait(barrier, 21)

    kv_first = []
    for d in (2, 1, 3):
        ww = (w + d) % 4
        for half in range(2):
            for part, ref in ((0, k_in), (1, v_in)):
                kv_first.append(
                    remote(
                        ref.at[pl.ds(64 * half, 64), tile(ww, 128)],
                        kv.at[kv_slots[half], pl.ds(128 * part, 128)],
                        at_blk(y, ww),
                    )
                )
    q_first = []
    for d in (2, 1, 3):
        ww = (w + d) % 4
        q_first.append(remote(q_in.at[:, tile(ww, 512)], qbuf.at[w], at_blk(y, ww)))
        q_first.append(remote(do_in.at[:, tile(ww, 512)], dobuf.at[w], at_blk(y, ww)))

    x_local.wait()

    def transpose_x(i, carry):
        block = xv[:, tile(i, 128)].T.reshape(2, 64, 128)
        xt[i // 2, pl.ds((i % 2) * 2, 2)] = block
        return carry

    lax.fori_loop(0, 32, transpose_x, 0)
    column = tile(w, 128)
    other = tile((w + 2) % 4, 128)
    core_mate = at_blk(y, w + 1 - 2 * core)
    z_mate = at_blk(y, (w + 2) % 4)
    xbuf[y, :, :, column] = xt[:, y]

    for copy in own_kv:
        copy.wait()
    for copy in kv_first:
        copy.wait_recv()
    kv_plus, kv_minus = [], []
    for yy, group in ((yp, kv_plus), (ym, kv_minus)):
        for slot in (tile(y, 256), tile(7 - y, 256)):
            group.append(remote(kv.at[slot], kv.at[slot], at_blk(yy, w)))
    x_far = [remote(xt.at[:, y], xbuf.at[y, :, :, column], z_mate)]
    x_mate = [remote(xt.at[:, y], xbuf.at[y, :, :, column], core_mate)]

    lane_row = lax.broadcasted_iota(jnp.int32, (1, HEAD), 1)
    frequency = jnp.exp(
        -(2.0 * (lane_row % 64).astype(F32) / HEAD) * math.log(ROPE_BASE)
    )
    for half, block in ((0, y), (1, 7 - y)):
        position = 256 * block + lax.broadcasted_iota(jnp.int32, (256, HEAD), 0)
        angles = position.astype(F32) * frequency
        cosb[half] = jnp.cos(angles)
        sinb[half] = jnp.where(lane_row < 64, jnp.sin(angles), -jnp.sin(angles))

    for copy in kv_plus:
        copy.wait_recv()
    slot = tile(ym, 256)
    kv_second = [remote(kv.at[slot], kv.at[slot], at_blk(yp, w))]
    for copy in kv_minus:
        copy.wait_recv()
    slot = tile(7 - yp, 256)
    kv_second.append(remote(kv.at[slot], kv.at[slot], at_blk(ym, w)))
    x_first = []
    for d in (1, 3, 2):
        yy = (y + d) % 4
        x_first.append(remote(xt.at[:, yy], xbuf.at[y, :, :, column], at_blk(yy, w)))

    for copy in own_q:
        copy.wait()
    for copy in q_first:
        copy.wait_recv()

    def stack(c, carry):
        half, h = c // 4, c % 4
        for ww in range(4):
            qs[c, pl.ds(64 * ww, 64)] = qbuf[ww, tile(half, 64), tile(h, 128)]
            dos[c, pl.ds(64 * ww, 64)] = dobuf[ww, tile(half, 64), tile(h, 128)]
        return carry

    lax.fori_loop(0, 8, stack, 0)

    for copy in kv_second:
        copy.wait_recv()

    lane = lax.broadcasted_iota(jnp.int32, (1, 256), 1)
    lane_high = (3 - lane // 64) * 64 + lane % 64
    rows = lax.broadcasted_iota(jnp.int32, (256, 256), 0)
    zero = jnp.zeros((8, 256), F32)

    def softmax_half(half, carry):
        diagonal = y + half * (7 - 2 * y)
        blocks = diagonal + 1
        query_pos = 256 * diagonal + lane + half * (lane_high - lane)
        rejected = query_pos >= reject_start

        def scores(j, tops):
            key_pos = 256 * j + rows
            chosen = jnp.logical_and(key_pos >= prompt_len, key_pos < reject_start)
            shown = jnp.where(rejected, jnp.where(chosen, FAR, key_pos), key_pos)
            bias = jnp.where(shown <= query_pos, 0.0, MASKED)
            key = kv[tile(j, 256), pl.ds(0, 128)]
            out = []
            for h in range(4):
                s = nt(key, qs[4 * half + h]) + bias
                p_f[4 * half + j, h] = s
                out.append(jnp.maximum(tops[h], jnp.max(s.reshape(32, 8, 256), axis=0)))
            return tuple(out)

        tops = lax.fori_loop(0, blocks, scores, (jnp.full((8, 256), MASKED, F32),) * 4)
        tops = [jnp.max(t, axis=0, keepdims=True) for t in tops]

        def weights(j, sums):
            out = []
            for h in range(4):
                p = jnp.exp2((p_f[4 * half + j, h] - tops[h]) * (scale * math.log2(math.e)))
                p_f[4 * half + j, h] = p
                p_t[4 * half + j, :, pl.ds(256 * h, 256)] = p.astype(BF16)
                out.append(sums[h] + jnp.sum(p.reshape(32, 8, 256), axis=0))
            return tuple(out)

        sums = lax.fori_loop(0, blocks, weights, (zero,) * 4)
        for h in range(4):
            inverse = 1.0 / jnp.sum(sums[h], axis=0, keepdims=True)
            inv_s[4 * half + h] = jnp.broadcast_to(inverse, (8, 256))
            per_row = jnp.broadcast_to(inverse, (128, 256)).T
            c = 4 * half + h
            dosn[c] = (dos[c].astype(F32) * per_row).astype(BF16)
            qsn[c] = (qs[c].astype(F32) * (per_row * scale)).astype(BF16)
        return carry

    lax.fori_loop(0, 2, softmax_half, 0)

    def sums_for(yy, left, right):
        g = (yy - y + 4) // 5
        low = nn(left[4 + yy], right[pl.ds(4, 4)].reshape(1024, 128))
        more = nn(
            left[g * (11 - yy) + (1 - g) * yy], right[pl.ds(4 * g, 4)].reshape(1024, 128)
        )
        keep = g.astype(F32)
        return low + more * (1.0 - keep), more * keep

    def own_sums(left, right):
        low = nn(left[4 + y], right[pl.ds(4, 4)].reshape(1024, 128))
        low = low + nn(left[y], right[pl.ds(0, 4)].reshape(1024, 128))
        return low, nn(left[11 - y], right[pl.ds(4, 4)].reshape(1024, 128))

    def reduce_first(part, left, right):
        low, high = sums_for(y2, left, right)
        part_b[part, y2, 0] = low.astype(BF16)
        part_b[part, y2, 1] = high.astype(BF16)
        return (
            remote(part_b.at[part, y2, 0], far_a.at[part], at_blk(yp, w)),
            remote(part_b.at[part, y2, 1], far_b.at[part], at_blk(ym, w)),
        )

    def reduce_middle(part, left, right):
        for yy in (yp, ym):
            low, high = sums_for(yy, left, right)
            part_f[part, yy, 0] = low
            part_f[part, yy, 1] = high

    def reduce_second(part, far):
        out = []
        far[0].wait_recv()
        part_b[part, yp, 0] = (part_f[part, yp, 0] + far_a[part].astype(F32)).astype(BF16)
        part_b[part, yp, 1] = part_f[part, yp, 1].astype(BF16)
        out.append(remote(part_b.at[part, yp], near_m.at[part], at_blk(yp, w)))
        far[1].wait_recv()
        part_b[part, ym, 0] = part_f[part, ym, 0].astype(BF16)
        part_b[part, ym, 1] = (part_f[part, ym, 1] + far_b[part].astype(F32)).astype(BF16)
        out.append(remote(part_b.at[part, ym], near_p.at[part], at_blk(ym, w)))
        return out

    def reduce_own(part, left, right):
        low, high = own_sums(left, right)
        part_f[part, y, 0] = low
        part_f[part, y, 1] = high

    far_v = reduce_first(1, p_t, dosn)
    reduce_middle(1, p_t, dosn)

    def transpose_k(j, carry):
        kt[j] = kv[tile(j, 256), pl.ds(0, 128)].T
        return carry

    lax.fori_loop(0, 8, transpose_k, 0)

    def score_grads(half):
        diagonal = y + half * (7 - 2 * y)
        blocks = diagonal + 1

        def products(j, sums):
            value = kv[tile(j, 256), pl.ds(128, 128)]
            out = []
            for h in range(4):
                d = nt(value, dos[4 * half + h])
                dp_s[j, h] = d
                pd = p_f[4 * half + j, h] * d
                out.append(sums[h] + jnp.sum(pd.reshape(32, 8, 256), axis=0))
            return tuple(out)

        sums = lax.fori_loop(0, blocks, products, (zero,) * 4)
        deltas = [
            jnp.sum(sums[h], axis=0, keepdims=True) * inv_s[4 * half + h, pl.ds(0, 1)]
            for h in range(4)
        ]
        dqacc[...] = jnp.zeros_like(dqacc)

        def grads(j, carry):
            key = kt[j]
            for h in range(4):
                ds = (p_f[4 * half + j, h] * (dp_s[j, h] - deltas[h])).astype(BF16)
                ds_t[4 * half + j, :, pl.ds(256 * h, 256)] = ds
                dqacc[h] += nn(key, ds)
            return carry

        lax.fori_loop(0, blocks, grads, 0)
        for h in range(4):
            dq = dqacc[h] * (inv_s[4 * half + h, pl.ds(0, 1)] * scale)
            dq = dq.T.astype(BF16)
            for ww in range(4):
                dqbuf[ww, pl.ds(64 * half, 64), pl.ds(128 * h, 128)] = dq[64 * ww : 64 * ww + 64]

    score_grads(1)
    for k, yy in ((0, ym), (1, yp)):
        x_first[k].wait_recv()
        x_far.append(remote(xbuf.at[yy, :, :, column], xbuf.at[yy, :, :, column], z_mate))
        x_mate.append(remote(xbuf.at[yy, :, :, column], xbuf.at[yy, :, :, column], core_mate))
    near_v = reduce_second(1, far_v)
    score_grads(0)

    far_k = reduce_first(0, ds_t, qsn)
    reduce_middle(0, ds_t, qsn)
    x_first[2].wait_recv()
    x_far.append(remote(xbuf.at[y2, :, :, column], xbuf.at[y2, :, :, column], z_mate))
    x_mate.append(remote(xbuf.at[y2, :, :, column], xbuf.at[y2, :, :, column], core_mate))
    own_out, far_out = [local(dqbuf.at[w], dq_out.at[:, tile(w, 512)])], []
    for d in (2, 1, 3):
        ww = (w + d) % 4
        far_out.append(remote(dqbuf.at[ww], dq_out.at[:, tile(w, 512)], at_blk(y, ww)))
    near_k = reduce_second(0, far_k)
    reduce_own(1, p_t, dosn)
    for copy in near_v:
        copy.wait_recv()

    def gathered(part, half):
        own = part_f[part, y, half]
        return own + near_m[part, half].astype(F32) + near_p[part, half].astype(F32)

    for half in range(2):
        value_grad = gathered(1, half).astype(BF16)
        for ww in range(4):
            at = 64 * ww if half == 0 else 64 * (3 - ww)
            gbuf[1, y, pl.ds(128 * ww + 64 * half, 64)] = value_grad[at : at + 64]

    def gather_near(part):
        return [
            remote(gbuf.at[part, y], gbuf.at[part, y], at_blk(yp, w)),
            remote(gbuf.at[part, y], gbuf.at[part, y], at_blk(ym, w)),
        ]

    def gather_far(part, near):
        low, high = pl.ds(0, 256), pl.ds(256, 256)
        near[0].wait_recv()
        first = remote(gbuf.at[part, ym, low], gbuf.at[part, ym, low], at_blk(yp, w))
        near[1].wait_recv()
        return [first, remote(gbuf.at[part, yp, high], gbuf.at[part, yp, high], at_blk(ym, w))]

    g_near_v = gather_near(1)
    reduce_own(0, ds_t, qsn)
    x_third = []
    for k, yy in ((0, y), (1, ym), (2, yp)):
        x_far[k].wait_recv()
        x_third.append(remote(xbuf.at[yy, :, :, other], xbuf.at[yy, :, :, other], core_mate))
    for copy in near_k:
        copy.wait_recv()
    for half in range(2):
        key_sum = gathered(0, half)
        key_grad = key_sum.astype(BF16)
        key_pre = (
            key_sum * cosb[half] + pltpu.roll(key_sum, 64, 1) * sinb[half]
        ).astype(BF16)
        for ww in range(4):
            at = 64 * ww if half == 0 else 64 * (3 - ww)
            gbuf[0, y, pl.ds(128 * ww + 64 * half, 64)] = key_pre[at : at + 64]
            dkbuf[ww, pl.ds(64 * half, 64)] = key_grad[at : at + 64]
    g_near_k = gather_near(0)
    g_far_v = gather_far(1, g_near_v)
    own_out.append(local(dkbuf.at[w], dk_out.at[:, column]))
    own_out.append(local(gbuf.at[1, y, tile(w, 128)], dv_out.at[:, column]))
    for d in (2, 1, 3):
        ww = (w + d) % 4
        far_out.append(remote(dkbuf.at[ww], dk_out.at[:, column], at_blk(y, ww)))
        far_out.append(
            remote(gbuf.at[1, y, tile(ww, 128)], dv_out.at[:, column], at_blk(y, ww))
        )
    x_far[3].wait_recv()
    x_third.append(remote(xbuf.at[y2, :, :, other], xbuf.at[y2, :, :, other], core_mate))
    for copy in x_mate:
        copy.wait_recv()
    for copy in x_third[:3]:
        copy.wait_recv()

    def weight_rows(part, yy, x_at):
        left = [xbuf[yy, 4 * k + x_at] for k in range(4)]
        return nn(jnp.concatenate(left, axis=0), gbuf[part, yy])

    def near_rows(part):
        def one(i, carry):
            rows_sum = weight_rows(part, y, i) + weight_rows(part, ym, i)
            wacc[part, i] = rows_sum + weight_rows(part, yp, i)
            return carry

        lax.fori_loop(0, 4, one, 0)

    def far_rows(part, far):
        for copy in far:
            copy.wait_recv()
        out = []
        for d in (2, 1, 3):
            x_at = (xx + d) % 4
            wb1[part, x_at] = (wacc[part, x_at] + weight_rows(part, y2, x_at)).astype(BF16)
            out.append(
                remote(wb1.at[part, x_at], r1.at[part, d - 1], {"dp": 4 * zhi + x_at})
            )
        wacc[part, xx] += weight_rows(part, y2, xx)
        return out

    def owner_sums(part, x_sums):
        total = wacc[part, xx]
        for copy in x_sums:
            copy.wait_recv()
        for d in range(3):
            total = total + r1[part, d].astype(F32)
        wb1[part, xx] = total.astype(BF16)
        out = []
        for dz in (2, 1, 3, 0):
            zz = (zhi + dz) % 4
            for d in (2, 1, 3, 0):
                ww = (w + d) % 4
                piece = pl.ds(pl.multiple_of(64 * zz + 16 * ww, 16), 16)
                if dz or d:
                    out.append(
                        remote(wb1.at[part, xx, piece], r2.at[part, zhi, w], at_owner(zz, ww))
                    )
                else:
                    r2[part, zhi, w] = wb1[part, xx, piece]
        return out

    near_rows(1)
    g_far_k = gather_far(0, g_near_k)
    x_third[3].wait_recv()
    x_sums_v = far_rows(1, g_far_v)
    near_rows(0)
    x_sums_k = far_rows(0, g_far_k)
    finals = owner_sums(1, x_sums_v)
    finals = finals + owner_sums(0, x_sums_k)
    for copy in finals:
        copy.wait_recv()
    for part in range(2):
        for ww in range(4):
            total = r2[part, 0, ww].astype(F32)
            for zz in range(1, 4):
                total = total + r2[part, zz, ww].astype(F32)
            w_stage[:, pl.ds(512 * part + 128 * ww, 128)] = total
    own_out.append(local(w_stage, w_out))
    for copy in own_out:
        copy.wait()
    for copy in far_out:
        copy.wait_recv()
    for copy in pending:
        copy.wait_send()


def body(queries, keys, values, out_grad, layer_input, lengths):
    anywhere = pl.BlockSpec(memory_space=pltpu.HBM)
    vmem = pltpu.VMEM
    outs = pl.pallas_call(
        kernel,
        out_shape=(
            jax.ShapeDtypeStruct((128, 2048), BF16),
            jax.ShapeDtypeStruct((128, 512), BF16),
            jax.ShapeDtypeStruct((128, 512), BF16),
            jax.ShapeDtypeStruct((16, 1024), F32),
        ),
        in_specs=[pl.BlockSpec(memory_space=pltpu.SMEM)] + [anywhere] * 5,
        out_specs=(anywhere,) * 4,
        scratch_shapes=[
            vmem((4, 128, 512), BF16),
            vmem((4, 128, 512), BF16),
            vmem((2048, 256), BF16),
            vmem((128, 4096), BF16),
            vmem((16, 4, 64, 128), BF16),
            vmem((4, 16, 64, 512), BF16),
            vmem((8, 256, 128), BF16),
            vmem((8, 256, 128), BF16),
            vmem((8, 256, 128), BF16),
            vmem((8, 256, 128), BF16),
            vmem((8, 128, 256), BF16),
            vmem((12, 4, 256, 256), F32),
            vmem((8, 4, 256, 256), F32),
            vmem((12, 256, 1024), BF16),
            vmem((12, 256, 1024), BF16),
            vmem((8, 8, 256), F32),
            vmem((4, 128, 256), F32),
            vmem((4, 128, 512), BF16),
            vmem((2, 4, 2, 256, 128), F32),
            vmem((2, 4, 2, 256, 128), BF16),
            vmem((2, 256, 128), BF16),
            vmem((2, 256, 128), BF16),
            vmem((2, 2, 256, 128), BF16),
            vmem((2, 2, 256, 128), BF16),
            vmem((2, 4, 512, 128), BF16),
            vmem((4, 128, 128), BF16),
            vmem((2, 256, 128), F32),
            vmem((2, 256, 128), F32),
            vmem((2, 4, 256, 128), F32),
            vmem((2, 4, 256, 128), BF16),
            vmem((2, 3, 256, 128), BF16),
            vmem((2, 4, 4, 16, 128), BF16),
            vmem((16, 1024), F32),
            pltpu.SemaphoreType.DMA((COPIES,)),
            pltpu.SemaphoreType.DMA((COPIES,)),
            pltpu.SemaphoreType.DMA((LOCALS,)),
        ],
        compiler_params=pltpu.CompilerParams(
            collective_id=0, has_side_effects=True, vmem_limit_bytes=60 * 1024 * 1024
        ),
        name="attention_backward",
    )(lengths[0], queries[0], out_grad[0], keys[0], values[0], layer_input[0])
    return (outs[0][None], outs[1][None], outs[2][None], outs[3])


def solution(mesh):
    placed = (P("dp", "blk", None),) * 5 + (P("dp", None),)
    return jax.shard_map(
        body,
        mesh=mesh,
        in_specs=placed,
        out_specs=(P("dp", "blk", None),) * 3 + (P(("dp", "blk"), None),),
        check_vma=False,
    )
```

```python
import math

import jax
import jax.numpy as jnp
from jax import lax
from jax.experimental import pallas as pl
from jax.experimental.pallas import tpu as pltpu
from jax.sharding import PartitionSpec as P

MESH = pl.DeviceIdType.MESH
F32 = jnp.float32
BF16 = jnp.bfloat16
HEAD = 128
ROPE_BASE = 500000.0
MASKED = -1e30
FAR = 1 << 20
COPIES = 128
LOCALS = 16


def nn(a, b):
    return jnp.dot(a, b, preferred_element_type=F32)


def nt(a, b):
    return lax.dot_general(a, b, (((1,), (1,)), ((), ())), preferred_element_type=F32)


def kernel(
    len_ref, q_in, do_in, k_in, v_in, x_in,
    dq_out, dk_out, dv_out, w_out,
    qbuf, dobuf, kv, xv, xt, xbuf, qs, dos, qsn, dosn, kt, p_f, dp_s, p_t, ds_t, inv_s, dqacc,
    dqbuf, part_f, part_b, near, gbuf, dkbuf, cosb, sinb, wacc, wb1, r1,
    r2, w_stage, send, recv, loc,
):
    b = lax.axis_index("blk")
    dp = lax.axis_index("dp")
    y, w = b // 4, b % 4
    core = w % 2
    zhi, xx = dp // 4, dp % 4
    yp, ym = (y + 1) % 4, (y + 3) % 4
    xp, x2, xm = (xx + 1) % 4, (xx + 2) % 4, (xx + 3) % 4
    scale = 1.0 / math.sqrt(HEAD)
    prompt_len = len_ref[0]
    reject_start = len_ref[0] + len_ref[1]

    count = [0, 0]
    pending = []

    def remote(src, dst, device):
        i = count[0]
        count[0] += 1
        copy = pltpu.make_async_remote_copy(
            src_ref=src, dst_ref=dst, send_sem=send.at[i], recv_sem=recv.at[i],
            device_id=device, device_id_type=MESH,
        )
        copy.start()
        pending.append(copy)
        return copy

    def local(src, dst):
        i = count[1]
        count[1] += 1
        copy = pltpu.make_async_copy(src, dst, loc.at[i])
        copy.start()
        return copy

    def at_blk(yy, ww):
        return {"blk": 4 * yy + ww}

    def at_x(to):
        return {"dp": 4 * zhi + to}

    def at_owner(zz, ww):
        return {"dp": 4 * zz + xx, "blk": 4 * y + ww}

    def tile(i, size):
        return pl.ds(pl.multiple_of(i * size, size), size)

    barrier = pltpu.get_barrier_semaphore()
    for d in range(1, 4):
        for device in (at_blk((y + d) % 4, w), {"dp": 4 * zhi + (xx + d) % 4}):
            pl.semaphore_signal(barrier, 1, device_id=device, device_id_type=MESH)
    for dz in range(4):
        for d in range(4):
            if dz or d:
                pl.semaphore_signal(
                    barrier, 1, device_id=at_owner((zhi + dz) % 4, (w + d) % 4),
                    device_id_type=MESH,
                )
    x_local = local(x_in, xv)
    kv_slots = (tile(4 * y + w, 64), tile(4 * (7 - y) + 3 - w, 64))
    own_kv = []
    for half in range(2):
        for part, ref in ((0, k_in), (1, v_in)):
            own_kv.append(
                local(
                    ref.at[pl.ds(64 * half, 64), tile(w, 128)],
                    kv.at[kv_slots[half], pl.ds(128 * part, 128)],
                )
            )
    own_q = [
        local(q_in.at[:, tile(w, 512)], qbuf.at[w]),
        local(do_in.at[:, tile(w, 512)], dobuf.at[w]),
    ]
    pl.semaphore_wait(barrier, 21)

    def row_slots(ww):
        return tile(4 * y + ww, 64), tile(4 * (7 - y) + 3 - ww, 64)

    kv_first = {}
    for d in (1, 3, 2):
        ww = (w + d) % 4
        kv_first[d] = []
        for half in range(2):
            for part, ref in ((0, k_in), (1, v_in)):
                kv_first[d].append(
                    remote(
                        ref.at[pl.ds(64 * half, 64), tile(ww, 128)],
                        kv.at[kv_slots[half], pl.ds(128 * part, 128)],
                        at_blk(y, ww),
                    )
                )
    q_first, do_first = [], []
    for ref, buf, group in ((q_in, qbuf, q_first), (do_in, dobuf, do_first)):
        for d in (1, 3, 2):
            ww = (w + d) % 4
            group.append(remote(ref.at[:, tile(ww, 512)], buf.at[w], at_blk(y, ww)))

    kv_plus, kv_minus = ([], []), ([], [])

    def spread(ww):
        slots = row_slots(ww)
        for half in range(2):
            kv_plus[half].append(remote(kv.at[slots[half]], kv.at[slots[half]], at_blk(yp, w)))
            slot = slots[1 - half]
            kv_minus[1 - half].append(remote(kv.at[slot], kv.at[slot], at_blk(ym, w)))

    for copy in own_kv:
        copy.wait()
    spread(w)

    x_local.wait()

    def transpose_x(i, carry):
        to = i % 8 // 2
        xt[to, i // 8, pl.ds((i % 2) * 2, 2)] = xv[:, tile(i, 128)].T.reshape(2, 64, 128)
        return carry

    lax.fori_loop(0, 32, transpose_x, 0)
    column = tile(w, 128)
    other = tile((w + 2) % 4, 128)
    core_mate = at_blk(y, w + 1 - 2 * core)
    z_mate = at_blk(y, (w + 2) % 4)
    x_first = []
    for d in (1, 3, 2):
        to = (xx + d) % 4
        x_first.append(remote(xt.at[to], xbuf.at[xx, :, :, :, column], at_x(to)))
    x_far = [remote(xt.at[xx], xbuf.at[xx, :, :, :, column], z_mate)]
    x_mate = [remote(xt.at[xx], xbuf.at[xx, :, :, :, column], core_mate)]

    for d in (1, 3, 2):
        for copy in kv_first[d]:
            copy.wait_recv()
        spread((w + 4 - d) % 4)
    xbuf[xx, :, :, :, column] = xt[xx]
    lane_row = lax.broadcasted_iota(jnp.int32, (1, HEAD), 1)
    frequency = jnp.exp(
        -(2.0 * (lane_row % 64).astype(F32) / HEAD) * math.log(ROPE_BASE)
    )
    for half, block in ((0, y), (1, 7 - y)):
        position = 256 * block + lax.broadcasted_iota(jnp.int32, (256, HEAD), 0)
        angles = position.astype(F32) * frequency
        cosb[half] = jnp.cos(angles)
        sinb[half] = jnp.where(lane_row < 64, jnp.sin(angles), -jnp.sin(angles))

    for copy in kv_plus[0]:
        copy.wait_recv()
    slot = tile(ym, 256)
    kv_second = [remote(kv.at[slot], kv.at[slot], at_blk(yp, w))]
    for copy in kv_minus[1]:
        copy.wait_recv()
    slot = tile(7 - yp, 256)
    kv_second.append(remote(kv.at[slot], kv.at[slot], at_blk(ym, w)))
    for copy in kv_plus[1] + kv_minus[0]:
        copy.wait_recv()

    own_q[0].wait()
    for copy in q_first:
        copy.wait_recv()

    def stack(buf, stacked):
        def one(c, carry):
            half, h = c // 4, c % 4
            for ww in range(4):
                stacked[c, pl.ds(64 * ww, 64)] = buf[ww, tile(half, 64), tile(h, 128)]
            return carry

        lax.fori_loop(0, 8, one, 0)

    stack(qbuf, qs)

    def forward_x(k, src):
        x_first[k].wait_recv()
        ref = xbuf.at[src, :, :, :, column]
        x_far.append(remote(ref, ref, z_mate))
        x_mate.append(remote(ref, ref, core_mate))

    forward_x(0, xm)
    forward_x(1, xp)
    for copy in kv_second:
        copy.wait_recv()

    lane = lax.broadcasted_iota(jnp.int32, (1, 256), 1)
    lane_high = (3 - lane // 64) * 64 + lane % 64
    rows = lax.broadcasted_iota(jnp.int32, (256, 256), 0)
    zero = jnp.zeros((8, 256), F32)

    def softmax_half(half, carry):
        diagonal = y + half * (7 - 2 * y)
        blocks = diagonal + 1
        query_pos = 256 * diagonal + lane + half * (lane_high - lane)
        rejected = query_pos >= reject_start

        def scores(j, tops):
            key_pos = 256 * j + rows
            chosen = jnp.logical_and(key_pos >= prompt_len, key_pos < reject_start)
            shown = jnp.where(rejected, jnp.where(chosen, FAR, key_pos), key_pos)
            bias = jnp.where(shown <= query_pos, 0.0, MASKED)
            key = kv[tile(j, 256), pl.ds(0, 128)]
            out = []
            for h in range(4):
                s = nt(key, qs[4 * half + h]) + bias
                p_f[4 * half + j, h] = s
                out.append(jnp.maximum(tops[h], jnp.max(s.reshape(32, 8, 256), axis=0)))
            return tuple(out)

        tops = lax.fori_loop(0, blocks, scores, (jnp.full((8, 256), MASKED, F32),) * 4)
        tops = [jnp.max(t, axis=0, keepdims=True) for t in tops]

        def weights(j, sums):
            out = []
            for h in range(4):
                p = jnp.exp2((p_f[4 * half + j, h] - tops[h]) * (scale * math.log2(math.e)))
                p_f[4 * half + j, h] = p
                p_t[4 * half + j, :, pl.ds(256 * h, 256)] = p.astype(BF16)
                out.append(sums[h] + jnp.sum(p.reshape(32, 8, 256), axis=0))
            return tuple(out)

        sums = lax.fori_loop(0, blocks, weights, (zero,) * 4)
        for h in range(4):
            inverse = 1.0 / jnp.sum(sums[h], axis=0, keepdims=True)
            inv_s[4 * half + h] = jnp.broadcast_to(inverse, (8, 256))
        return carry

    lax.fori_loop(0, 2, softmax_half, 0)

    forward_x(2, x2)
    own_q[1].wait()
    for copy in do_first:
        copy.wait_recv()
    stack(dobuf, dos)

    def scale_rows(c, carry):
        per_row = jnp.broadcast_to(inv_s[c, pl.ds(0, 1)], (128, 256)).T
        dosn[c] = (dos[c].astype(F32) * per_row).astype(BF16)
        qsn[c] = (qs[c].astype(F32) * (per_row * scale)).astype(BF16)
        return carry

    lax.fori_loop(0, 8, scale_rows, 0)
    def sums_for(yy, left, right):
        g = (yy - y + 4) // 5
        low = nn(left[4 + yy], right[pl.ds(4, 4)].reshape(1024, 128))
        more = nn(
            left[g * (11 - yy) + (1 - g) * yy], right[pl.ds(4 * g, 4)].reshape(1024, 128)
        )
        keep = g.astype(F32)
        return low + more * (1.0 - keep), more * keep

    def own_sums(left, right):
        low = nn(left[4 + y], right[pl.ds(4, 4)].reshape(1024, 128))
        low = low + nn(left[y], right[pl.ds(0, 4)].reshape(1024, 128))
        return low, nn(left[11 - y], right[pl.ds(4, 4)].reshape(1024, 128))

    def reduce_send(part, left, right):
        out = []
        for d in (2, 1, 3):
            yy = (y + d) % 4
            low, high = sums_for(yy, left, right)
            part_b[part, yy, 0] = low.astype(BF16)
            part_b[part, yy, 1] = high.astype(BF16)
            out.append(remote(part_b.at[part, yy], near.at[part, d - 1], at_blk(yy, w)))
        return out

    def reduce_own(part, left, right):
        low, high = own_sums(left, right)
        part_f[part, 0] = low
        part_f[part, 1] = high

    near_v = reduce_send(1, p_t, dosn)

    def transpose_k(j, carry):
        kt[j] = kv[tile(j, 256), pl.ds(0, 128)].T
        return carry

    lax.fori_loop(0, 8, transpose_k, 0)

    def score_grads(half):
        diagonal = y + half * (7 - 2 * y)
        blocks = diagonal + 1

        def products(j, sums):
            value = kv[tile(j, 256), pl.ds(128, 128)]
            out = []
            for h in range(4):
                d = nt(value, dos[4 * half + h])
                dp_s[j, h] = d
                pd = p_f[4 * half + j, h] * d
                out.append(sums[h] + jnp.sum(pd.reshape(32, 8, 256), axis=0))
            return tuple(out)

        sums = lax.fori_loop(0, blocks, products, (zero,) * 4)
        deltas = [
            jnp.sum(sums[h], axis=0, keepdims=True) * inv_s[4 * half + h, pl.ds(0, 1)]
            for h in range(4)
        ]
        dqacc[...] = jnp.zeros_like(dqacc)

        def grads(j, carry):
            key = kt[j]
            for h in range(4):
                ds = (p_f[4 * half + j, h] * (dp_s[j, h] - deltas[h])).astype(BF16)
                ds_t[4 * half + j, :, pl.ds(256 * h, 256)] = ds
                dqacc[h] += nn(key, ds)
            return carry

        lax.fori_loop(0, blocks, grads, 0)
        for h in range(4):
            dq = dqacc[h] * (inv_s[4 * half + h, pl.ds(0, 1)] * scale)
            dq = dq.T.astype(BF16)
            for ww in range(4):
                dqbuf[ww, pl.ds(64 * half, 64), pl.ds(128 * h, 128)] = dq[64 * ww : 64 * ww + 64]

    score_grads(1)
    score_grads(0)

    near_k = reduce_send(0, ds_t, qsn)
    own_out, far_out = [local(dqbuf.at[w], dq_out.at[:, tile(w, 512)])], []
    for d in (2, 1, 3):
        ww = (w + d) % 4
        far_out.append(remote(dqbuf.at[ww], dq_out.at[:, tile(w, 512)], at_blk(y, ww)))
    reduce_own(1, p_t, dosn)
    for copy in near_v:
        copy.wait_recv()

    def gathered(part, half):
        total = part_f[part, half]
        for d in range(3):
            total = total + near[part, d, half].astype(F32)
        return total

    for half in range(2):
        value_grad = gathered(1, half).astype(BF16)
        for ww in range(4):
            at = 64 * ww if half == 0 else 64 * (3 - ww)
            gbuf[1, xx, pl.ds(128 * ww + 64 * half, 64)] = value_grad[at : at + 64]

    def gather(part):
        ref = gbuf.at[part, xx]
        return [remote(ref, ref, at_x((xx + d) % 4)) for d in (2, 1, 3)]

    g_v = gather(1)
    reduce_own(0, ds_t, qsn)
    x_third = []

    def third_x(k, src):
        x_far[k].wait_recv()
        ref = xbuf.at[src, :, :, :, other]
        x_third.append(remote(ref, ref, core_mate))

    third_x(0, xx)
    for copy in near_k:
        copy.wait_recv()
    for half in range(2):
        key_sum = gathered(0, half)
        key_grad = key_sum.astype(BF16)
        key_pre = (
            key_sum * cosb[half] + pltpu.roll(key_sum, 64, 1) * sinb[half]
        ).astype(BF16)
        for ww in range(4):
            at = 64 * ww if half == 0 else 64 * (3 - ww)
            gbuf[0, xx, pl.ds(128 * ww + 64 * half, 64)] = key_pre[at : at + 64]
            dkbuf[ww, pl.ds(64 * half, 64)] = key_grad[at : at + 64]
    g_k = gather(0)
    third_x(1, xm)
    third_x(2, xp)
    own_out.append(local(dkbuf.at[w], dk_out.at[:, column]))
    own_out.append(local(gbuf.at[1, xx, tile(w, 128)], dv_out.at[:, column]))
    third_x(3, x2)
    for d in (2, 1, 3):
        ww = (w + d) % 4
        far_out.append(remote(dkbuf.at[ww], dk_out.at[:, column], at_blk(y, ww)))
        far_out.append(
            remote(gbuf.at[1, xx, tile(ww, 128)], dv_out.at[:, column], at_blk(y, ww))
        )
    for copy in x_mate + x_third:
        copy.wait_recv()

    def weight_rows(part, src, to):
        left = [xbuf[src, k, to] for k in range(4)]
        return nn(jnp.concatenate(left, axis=0), gbuf[part, src])

    def own_rows(part):
        def one(i, carry):
            wacc[part, i] = weight_rows(part, xx, i)
            return carry

        lax.fori_loop(0, 4, one, 0)

    def near_rows(part):
        def one(i, carry):
            wacc[part, i] += weight_rows(part, xm, i) + weight_rows(part, xp, i)
            return carry

        lax.fori_loop(0, 4, one, 0)

    def far_rows(part):
        out = []
        for d in (2, 1, 3):
            to = (y + d) % 4
            wb1[part, to] = (wacc[part, to] + weight_rows(part, x2, to)).astype(BF16)
            out.append(remote(wb1.at[part, to], r1.at[part, d - 1], at_blk(to, w)))
        wacc[part, y] += weight_rows(part, x2, y)
        return out

    def owner_sums(part, y_sums):
        total = wacc[part, y]
        for copy in y_sums:
            copy.wait_recv()
        for d in range(3):
            total = total + r1[part, d].astype(F32)
        wb1[part, y] = total.astype(BF16)
        out = []
        for dz in (2, 1, 3, 0):
            zz = (zhi + dz) % 4
            for d in (2, 1, 3, 0):
                ww = (w + d) % 4
                piece = pl.ds(pl.multiple_of(64 * zz + 16 * ww, 16), 16)
                if dz or d:
                    out.append(
                        remote(wb1.at[part, y, piece], r2.at[part, zhi, w], at_owner(zz, ww))
                    )
                else:
                    r2[part, zhi, w] = wb1[part, y, piece]
        return out

    own_rows(1)
    own_rows(0)
    for copy in g_v:
        copy.wait_recv()
    near_rows(1)
    y_sums_v = far_rows(1)
    for copy in g_k[1:]:
        copy.wait_recv()
    near_rows(0)
    g_k[0].wait_recv()
    y_sums_k = far_rows(0)
    finals = owner_sums(1, y_sums_v)
    finals = finals + owner_sums(0, y_sums_k)
    for copy in finals:
        copy.wait_recv()
    for part in range(2):
        for ww in range(4):
            total = r2[part, 0, ww].astype(F32)
            for zz in range(1, 4):
                total = total + r2[part, zz, ww].astype(F32)
            w_stage[:, pl.ds(512 * part + 128 * ww, 128)] = total
    own_out.append(local(w_stage, w_out))
    for copy in own_out:
        copy.wait()
    for copy in far_out:
        copy.wait_recv()
    for copy in pending:
        copy.wait_send()


def body(queries, keys, values, out_grad, layer_input, lengths):
    anywhere = pl.BlockSpec(memory_space=pltpu.HBM)
    vmem = pltpu.VMEM
    outs = pl.pallas_call(
        kernel,
        out_shape=(
            jax.ShapeDtypeStruct((128, 2048), BF16),
            jax.ShapeDtypeStruct((128, 512), BF16),
            jax.ShapeDtypeStruct((128, 512), BF16),
            jax.ShapeDtypeStruct((16, 1024), F32),
        ),
        in_specs=[pl.BlockSpec(memory_space=pltpu.SMEM)] + [anywhere] * 5,
        out_specs=(anywhere,) * 4,
        scratch_shapes=[
            vmem((4, 128, 512), BF16),
            vmem((4, 128, 512), BF16),
            vmem((2048, 256), BF16),
            vmem((128, 4096), BF16),
            vmem((4, 4, 4, 64, 128), BF16),
            vmem((4, 4, 4, 64, 512), BF16),
            vmem((8, 256, 128), BF16),
            vmem((8, 256, 128), BF16),
            vmem((8, 256, 128), BF16),
            vmem((8, 256, 128), BF16),
            vmem((8, 128, 256), BF16),
            vmem((12, 4, 256, 256), F32),
            vmem((8, 4, 256, 256), F32),
            vmem((12, 256, 1024), BF16),
            vmem((12, 256, 1024), BF16),
            vmem((8, 8, 256), F32),
            vmem((4, 128, 256), F32),
            vmem((4, 128, 512), BF16),
            vmem((2, 2, 256, 128), F32),
            vmem((2, 4, 2, 256, 128), BF16),
            vmem((2, 3, 2, 256, 128), BF16),
            vmem((2, 4, 512, 128), BF16),
            vmem((4, 128, 128), BF16),
            vmem((2, 256, 128), F32),
            vmem((2, 256, 128), F32),
            vmem((2, 4, 256, 128), F32),
            vmem((2, 4, 256, 128), BF16),
            vmem((2, 3, 256, 128), BF16),
            vmem((2, 4, 4, 16, 128), BF16),
            vmem((16, 1024), F32),
            pltpu.SemaphoreType.DMA((COPIES,)),
            pltpu.SemaphoreType.DMA((COPIES,)),
            pltpu.SemaphoreType.DMA((LOCALS,)),
        ],
        compiler_params=pltpu.CompilerParams(
            collective_id=0, has_side_effects=True, vmem_limit_bytes=60 * 1024 * 1024
        ),
        name="attention_backward",
    )(lengths[0], queries[0], out_grad[0], keys[0], values[0], layer_input[0])
    return (outs[0][None], outs[1][None], outs[2][None], outs[3])


def solution(mesh):
    placed = (P("dp", "blk", None),) * 5 + (P("dp", None),)
    return jax.shard_map(
        body,
        mesh=mesh,
        in_specs=placed,
        out_specs=(P("dp", "blk", None),) * 3 + (P(("dp", "blk"), None),),
        check_vma=False,
    )
```

```python
import math

import jax
import jax.numpy as jnp
from jax import lax
from jax.experimental import pallas as pl
from jax.experimental.pallas import tpu as pltpu
from jax.sharding import PartitionSpec as P

MESH = pl.DeviceIdType.MESH
F32 = jnp.float32
BF16 = jnp.bfloat16
HEAD = 128
ROPE_BASE = 500000.0
MASKED = -1e30
FAR = 1 << 20
COPIES = 128
LOCALS = 16


def nn(a, b):
    return jnp.dot(a, b, preferred_element_type=F32)


def nt(a, b):
    return lax.dot_general(a, b, (((1,), (1,)), ((), ())), preferred_element_type=F32)


def kernel(
    len_ref, q_in, do_in, k_in, v_in, x_in,
    dq_out, dk_out, dv_out, w_out,
    qbuf, dobuf, kv, xv, xt, xbuf, qs, dos, qsn, dosn, kt, p_f, dp_s, p_t, ds_t, top_s, inv_s, del_s, dqacc,
    dqbuf, part_f, part_b, near, gbuf, dkbuf, cosb, sinb, wb1, r1,
    r2, w_stage, send, recv, loc,
):
    b = lax.axis_index("blk")
    dp = lax.axis_index("dp")
    y, w = b // 4, b % 4
    core = w % 2
    zhi, xx = dp // 4, dp % 4
    yp, ym = (y + 1) % 4, (y + 3) % 4
    xp, x2, xm = (xx + 1) % 4, (xx + 2) % 4, (xx + 3) % 4
    scale = 1.0 / math.sqrt(HEAD)
    prompt_len = len_ref[0]
    reject_start = len_ref[0] + len_ref[1]

    count = [0, 0]
    pending = []

    def remote(src, dst, device):
        i = count[0]
        count[0] += 1
        copy = pltpu.make_async_remote_copy(
            src_ref=src, dst_ref=dst, send_sem=send.at[i], recv_sem=recv.at[i],
            device_id=device, device_id_type=MESH,
        )
        copy.start()
        pending.append(copy)
        return copy

    def local(src, dst):
        i = count[1]
        count[1] += 1
        copy = pltpu.make_async_copy(src, dst, loc.at[i])
        copy.start()
        return copy

    def at_blk(yy, ww):
        return {"blk": 4 * yy + ww}

    def at_x(to):
        return {"dp": 4 * zhi + to}

    def at_owner(zz, ww):
        return {"dp": 4 * zz + xx, "blk": 4 * y + ww}

    def tile(i, size):
        return pl.ds(pl.multiple_of(i * size, size), size)

    barrier = pltpu.get_barrier_semaphore()
    for d in range(1, 4):
        for device in (at_blk((y + d) % 4, w), {"dp": 4 * zhi + (xx + d) % 4}):
            pl.semaphore_signal(barrier, 1, device_id=device, device_id_type=MESH)
    for dz in range(4):
        for d in range(4):
            if dz or d:
                pl.semaphore_signal(
                    barrier, 1, device_id=at_owner((zhi + dz) % 4, (w + d) % 4),
                    device_id_type=MESH,
                )
    x_local = local(x_in, xv)
    kv_slots = (tile(4 * y + w, 64), tile(4 * (7 - y) + 3 - w, 64))
    own_kv = []
    for half in range(2):
        for part, ref in ((0, k_in), (1, v_in)):
            own_kv.append(
                local(
                    ref.at[pl.ds(64 * half, 64), tile(w, 128)],
                    kv.at[kv_slots[half], pl.ds(128 * part, 128)],
                )
            )
    own_q = [
        local(q_in.at[:, tile(w, 512)], qbuf.at[w]),
        local(do_in.at[:, tile(w, 512)], dobuf.at[w]),
    ]
    pl.semaphore_wait(barrier, 21)

    def row_slots(ww):
        return tile(4 * y + ww, 64), tile(4 * (7 - y) + 3 - ww, 64)

    kv_first = {}
    for d in (1, 3, 2):
        ww = (w + d) % 4
        kv_first[d] = []
        for half in range(2):
            for part, ref in ((0, k_in), (1, v_in)):
                kv_first[d].append(
                    remote(
                        ref.at[pl.ds(64 * half, 64), tile(ww, 128)],
                        kv.at[kv_slots[half], pl.ds(128 * part, 128)],
                        at_blk(y, ww),
                    )
                )
    q_first, do_first = [], []
    for ref, buf, group in ((q_in, qbuf, q_first), (do_in, dobuf, do_first)):
        for d in (1, 3, 2):
            ww = (w + d) % 4
            group.append(remote(ref.at[:, tile(ww, 512)], buf.at[w], at_blk(y, ww)))

    kv_plus, kv_minus = ([], []), ([], [])

    def spread(ww):
        slots = row_slots(ww)
        for half in range(2):
            kv_plus[half].append(remote(kv.at[slots[half]], kv.at[slots[half]], at_blk(yp, w)))
            slot = slots[1 - half]
            kv_minus[1 - half].append(remote(kv.at[slot], kv.at[slot], at_blk(ym, w)))

    for copy in own_kv:
        copy.wait()
    spread(w)

    x_local.wait()

    def transpose_x(i, carry):
        to = i % 8 // 2
        xt[to, pl.ds((i % 2) * 2, 2), i // 8] = xv[:, tile(i, 128)].T.reshape(2, 64, 128)
        return carry

    lax.fori_loop(0, 32, transpose_x, 0)
    column = tile(w, 128)
    other = tile((w + 2) % 4, 128)
    core_mate = at_blk(y, w + 1 - 2 * core)
    z_mate = at_blk(y, (w + 2) % 4)
    x_first = []
    for d in (1, 3, 2):
        to = (xx + d) % 4
        x_first.append(remote(xt.at[to], xbuf.at[:, 4 - d, :, :, column], at_x(to)))
    x_far = [remote(xt.at[xx], xbuf.at[:, 0, :, :, column], z_mate)]
    x_mate = [remote(xt.at[xx], xbuf.at[:, 0, :, :, column], core_mate)]

    for d in (1, 3, 2):
        for copy in kv_first[d]:
            copy.wait_recv()
        spread((w + 4 - d) % 4)
    xbuf[:, 0, :, :, column] = xt[xx]
    lane_row = lax.broadcasted_iota(jnp.int32, (1, HEAD), 1)
    frequency = jnp.exp(
        -(2.0 * (lane_row % 64).astype(F32) / HEAD) * math.log(ROPE_BASE)
    )
    for half, block in ((0, y), (1, 7 - y)):
        position = 256 * block + lax.broadcasted_iota(jnp.int32, (256, HEAD), 0)
        angles = position.astype(F32) * frequency
        cosb[half] = jnp.cos(angles)
        sinb[half] = jnp.where(lane_row < 64, jnp.sin(angles), -jnp.sin(angles))

    kv_second = []
    for k, d in enumerate((0, 1, 3, 2)):
        ww = (w + 4 - d) % 4
        kv_plus[0][k].wait_recv()
        slot = tile(4 * ym + ww, 64)
        kv_second.append(remote(kv.at[slot], kv.at[slot], at_blk(yp, w)))
        kv_minus[1][k].wait_recv()
        slot = tile(4 * (7 - yp) + 3 - ww, 64)
        kv_second.append(remote(kv.at[slot], kv.at[slot], at_blk(ym, w)))
    for copy in kv_plus[1] + kv_minus[0]:
        copy.wait_recv()

    own_q[0].wait()
    for copy in q_first:
        copy.wait_recv()

    def stack(buf, stacked):
        def one(c, carry):
            half, h = c // 4, c % 4
            for ww in range(4):
                stacked[c, pl.ds(64 * ww, 64)] = buf[ww, tile(half, 64), tile(h, 128)]
            return carry

        lax.fori_loop(0, 8, one, 0, unroll=True)

    stack(qbuf, qs)

    for copy in kv_second:
        copy.wait_recv()

    lane = lax.broadcasted_iota(jnp.int32, (1, 256), 1)
    lane_high = (3 - lane // 64) * 64 + lane % 64
    rows = lax.broadcasted_iota(jnp.int32, (256, 256), 0)
    zero = jnp.zeros((8, 256), F32)

    def softmax_half(half, carry):
        diagonal = y + half * (7 - 2 * y)
        blocks = diagonal + 1
        query_pos = 256 * diagonal + lane + half * (lane_high - lane)
        rejected = query_pos >= reject_start

        def scores(j, tops):
            key_pos = 256 * j + rows
            chosen = jnp.logical_and(key_pos >= prompt_len, key_pos < reject_start)
            shown = jnp.where(rejected, jnp.where(chosen, FAR, key_pos), key_pos)
            bias = jnp.where(shown <= query_pos, 0.0, MASKED)
            key = kv[tile(j, 256), pl.ds(0, 128)]
            out = []
            for h in range(4):
                s = nt(key, qs[4 * half + h]) + bias
                p_f[4 * half + j, h] = s
                out.append(jnp.maximum(tops[h], jnp.max(s.reshape(32, 8, 256), axis=0)))
            return tuple(out)

        tops = lax.fori_loop(0, blocks, scores, (jnp.full((8, 256), MASKED, F32),) * 4)
        for h in range(4):
            top_s[4 * half + h] = jnp.broadcast_to(
                jnp.max(tops[h], axis=0, keepdims=True), (8, 256)
            )
        return carry

    lax.fori_loop(0, 2, softmax_half, 0)

    order = (2, 1, 3, 0)
    for copy in x_first:
        copy.wait_recv()
    for d in order:
        ref = xbuf.at[(y + d) % 4, pl.ds(1, 3), :, :, column]
        x_far.append(remote(ref, ref, z_mate))
        x_mate.append(remote(ref, ref, core_mate))

    own_q[1].wait()
    for copy in do_first:
        copy.wait_recv()
    stack(dobuf, dos)

    def weights_half(half, carry):
        blocks = y + half * (7 - 2 * y) + 1
        tops = [top_s[4 * half + h, pl.ds(0, 1)] for h in range(4)]

        def weights(j, sums):
            value = kv[tile(j, 256), pl.ds(128, 128)]
            slot = 4 * half + j
            totals, dots = [], []
            for h in range(4):
                p = jnp.exp2((p_f[slot, h] - tops[h]) * (scale * math.log2(math.e)))
                p_f[slot, h] = p
                p_t[slot, :, pl.ds(256 * h, 256)] = p.astype(BF16)
                totals.append(sums[0][h] + jnp.sum(p.reshape(32, 8, 256), axis=0))
                d = nt(value, dos[4 * half + h])
                dp_s[slot, h] = d
                dots.append(sums[1][h] + jnp.sum((p * d).reshape(32, 8, 256), axis=0))
            return tuple(totals), tuple(dots)

        totals, dots = lax.fori_loop(0, blocks, weights, ((zero,) * 4, (zero,) * 4))
        for h in range(4):
            inverse = 1.0 / jnp.sum(totals[h], axis=0, keepdims=True)
            delta = jnp.sum(dots[h], axis=0, keepdims=True) * inverse
            inv_s[4 * half + h] = jnp.broadcast_to(inverse, (8, 256))
            del_s[4 * half + h] = jnp.broadcast_to(delta, (8, 256))
        return carry

    lax.fori_loop(0, 2, weights_half, 0)

    def scale_rows(c, carry):
        per_row = jnp.broadcast_to(inv_s[c, pl.ds(0, 1)], (128, 256)).T
        dosn[c] = (dos[c].astype(F32) * per_row).astype(BF16)
        qsn[c] = (qs[c].astype(F32) * (per_row * scale)).astype(BF16)
        return carry

    lax.fori_loop(0, 8, scale_rows, 0, unroll=True)
    def sums_for(yy, left, right):
        g = (yy - y + 4) // 5
        low = nn(left[4 + yy], right[pl.ds(4, 4)].reshape(1024, 128))
        more = nn(
            left[g * (11 - yy) + (1 - g) * yy], right[pl.ds(4 * g, 4)].reshape(1024, 128)
        )
        keep = g.astype(F32)
        return low + more * (1.0 - keep), more * keep

    def own_sums(left, right):
        low = nn(left[4 + y], right[pl.ds(4, 4)].reshape(1024, 128))
        low = low + nn(left[y], right[pl.ds(0, 4)].reshape(1024, 128))
        return low, nn(left[11 - y], right[pl.ds(4, 4)].reshape(1024, 128))

    def reduce_send(part, left, right):
        out = []
        for d in (2, 1, 3):
            yy = (y + d) % 4
            low, high = sums_for(yy, left, right)
            part_b[part, yy, 0] = low.astype(BF16)
            part_b[part, yy, 1] = high.astype(BF16)
            out.append(remote(part_b.at[part, yy], near.at[part, d - 1], at_blk(yy, w)))
        return out

    def reduce_own(part, left, right):
        low, high = own_sums(left, right)
        part_f[part, 0] = low
        part_f[part, 1] = high

    near_v = reduce_send(1, p_t, dosn)

    def grads_half(half, carry):
        blocks = y + half * (7 - 2 * y) + 1
        deltas = [del_s[4 * half + h, pl.ds(0, 1)] for h in range(4)]

        def grads(j, carry):
            slot = 4 * half + j
            for h in range(4):
                ds = p_f[slot, h] * (dp_s[slot, h] - deltas[h])
                ds_t[slot, :, pl.ds(256 * h, 256)] = ds.astype(BF16)
            return carry

        return lax.fori_loop(0, blocks, grads, carry)

    lax.fori_loop(0, 2, grads_half, 0)

    near_k = reduce_send(0, ds_t, qsn)
    reduce_own(1, p_t, dosn)
    for copy in near_v:
        copy.wait_recv()

    def gathered(part, half):
        total = part_f[part, half]
        for d in range(3):
            total = total + near[part, d, half].astype(F32)
        return total

    for half in range(2):
        value_grad = gathered(1, half).astype(BF16)
        for ww in range(4):
            at = 64 * ww if half == 0 else 64 * (3 - ww)
            rows_at = pl.ds(128 * ww + 64 * half, 64)
            gbuf[0, rows_at, pl.ds(128, 128)] = value_grad[at : at + 64]

    def gather(part):
        lanes = pl.ds(128 * part, 128)
        return [
            remote(gbuf.at[0, :, lanes], gbuf.at[4 - d, :, lanes], at_x((xx + d) % 4))
            for d in (2, 1, 3)
        ]

    g_v = gather(1)
    reduce_own(0, ds_t, qsn)
    def transpose_k(j, carry):
        kt[j] = kv[tile(j, 256), pl.ds(0, 128)].T
        return carry

    lax.fori_loop(0, 8, transpose_k, 0, unroll=2)

    def query_half(half, carry):
        blocks = y + half * (7 - 2 * y) + 1
        dqacc[...] = jnp.zeros_like(dqacc)

        def one(j, carry):
            for h in range(4):
                dqacc[h] += nn(kt[j], ds_t[4 * half + j, :, pl.ds(256 * h, 256)])
            return carry

        lax.fori_loop(0, blocks, one, 0)
        for h in range(4):
            dq = dqacc[h] * (inv_s[4 * half + h, pl.ds(0, 1)] * scale)
            dq = dq.T.astype(BF16)
            for ww in range(4):
                dqbuf[ww, tile(half, 64), pl.ds(128 * h, 128)] = dq[64 * ww : 64 * ww + 64]
        return carry

    lax.fori_loop(0, 2, query_half, 0)
    own_out, far_out = [local(dqbuf.at[w], dq_out.at[:, tile(w, 512)])], []
    for d in (2, 1, 3):
        ww = (w + d) % 4
        far_out.append(remote(dqbuf.at[ww], dq_out.at[:, tile(w, 512)], at_blk(y, ww)))
    x_third = []

    def third_x(k):
        x_far[k].wait_recv()
        if k == 0:
            ref = xbuf.at[:, 0, :, :, other]
        else:
            ref = xbuf.at[(y + order[k - 1]) % 4, pl.ds(1, 3), :, :, other]
        x_third.append(remote(ref, ref, core_mate))

    third_x(0)
    for copy in near_k:
        copy.wait_recv()
    for half in range(2):
        key_sum = gathered(0, half)
        key_grad = key_sum.astype(BF16)
        key_pre = (
            key_sum * cosb[half] + pltpu.roll(key_sum, 64, 1) * sinb[half]
        ).astype(BF16)
        for ww in range(4):
            at = 64 * ww if half == 0 else 64 * (3 - ww)
            gbuf[0, pl.ds(128 * ww + 64 * half, 64), pl.ds(0, 128)] = key_pre[at : at + 64]
            dkbuf[ww, pl.ds(64 * half, 64)] = key_grad[at : at + 64]
    g_k = gather(0)
    third_x(1)
    values_out = pl.ds(128, 128)
    own_out.append(local(dkbuf.at[w], dk_out.at[:, column]))
    own_out.append(local(gbuf.at[0, tile(w, 128), values_out], dv_out.at[:, column]))
    for d in (2, 1, 3):
        ww = (w + d) % 4
        far_out.append(remote(dkbuf.at[ww], dk_out.at[:, column], at_blk(y, ww)))
        far_out.append(
            remote(gbuf.at[0, tile(ww, 128), values_out], dv_out.at[:, column], at_blk(y, ww))
        )

    third_x(2)
    for copy in g_v + g_k:
        copy.wait_recv()

    def weight_tile(to):
        total = nn(xbuf[to, 0].reshape(256, 512), gbuf[0])
        for rel in range(1, 4):
            total = total + nn(xbuf[to, rel].reshape(256, 512), gbuf[rel])
        return total

    y_sums = []
    x_mate[0].wait_recv()
    x_third[0].wait_recv()
    for k, d in enumerate(order[:3]):
        to = (y + d) % 4
        x_mate[k + 1].wait_recv()
        x_third[k + 1].wait_recv()
        wb1[to] = weight_tile(to).astype(BF16)
        y_sums.append(remote(wb1.at[to], r1.at[d - 1], at_blk(to, w)))
        if k:
            third_x(k + 2)
    x_mate[4].wait_recv()
    x_third[4].wait_recv()
    total = weight_tile(y)
    for copy in y_sums:
        copy.wait_recv()
    for d in range(3):
        total = total + r1[d].astype(F32)
    wb1[y] = total.astype(BF16)
    finals = []
    for dz in (2, 1, 3, 0):
        zz = (zhi + dz) % 4
        for d in (2, 1, 3, 0):
            ww = (w + d) % 4
            piece = pl.ds(pl.multiple_of(64 * zz + 16 * ww, 16), 16)
            if dz or d:
                finals.append(remote(wb1.at[y, piece], r2.at[zhi, w], at_owner(zz, ww)))
            else:
                r2[zhi, w] = wb1[y, piece]
    for copy in finals:
        copy.wait_recv()
    for ww in range(4):
        total = r2[0, ww].astype(F32)
        for zz in range(1, 4):
            total = total + r2[zz, ww].astype(F32)
        for part in range(2):
            lanes = pl.ds(512 * part + 128 * ww, 128)
            w_stage[:, lanes] = total[:, 128 * part : 128 * part + 128]
    own_out.append(local(w_stage, w_out))
    for copy in own_out:
        copy.wait()
    for copy in far_out:
        copy.wait_recv()
    for copy in pending:
        copy.wait_send()


def body(queries, keys, values, out_grad, layer_input, lengths):
    anywhere = pl.BlockSpec(memory_space=pltpu.HBM)
    vmem = pltpu.VMEM
    outs = pl.pallas_call(
        kernel,
        out_shape=(
            jax.ShapeDtypeStruct((128, 2048), BF16),
            jax.ShapeDtypeStruct((128, 512), BF16),
            jax.ShapeDtypeStruct((128, 512), BF16),
            jax.ShapeDtypeStruct((16, 1024), F32),
        ),
        in_specs=[pl.BlockSpec(memory_space=pltpu.SMEM)] + [anywhere] * 5,
        out_specs=(anywhere,) * 4,
        scratch_shapes=[
            vmem((4, 128, 512), BF16),
            vmem((4, 128, 512), BF16),
            vmem((2048, 256), BF16),
            vmem((128, 4096), BF16),
            vmem((4, 4, 4, 64, 128), BF16),
            vmem((4, 4, 4, 64, 512), BF16),
            vmem((8, 256, 128), BF16),
            vmem((8, 256, 128), BF16),
            vmem((8, 256, 128), BF16),
            vmem((8, 256, 128), BF16),
            vmem((8, 128, 256), BF16),
            vmem((12, 4, 256, 256), F32),
            vmem((12, 4, 256, 256), F32),
            vmem((12, 256, 1024), BF16),
            vmem((12, 256, 1024), BF16),
            vmem((8, 8, 256), F32),
            vmem((8, 8, 256), F32),
            vmem((8, 8, 256), F32),
            vmem((4, 128, 256), F32),
            vmem((4, 128, 512), BF16),
            vmem((2, 2, 256, 128), F32),
            vmem((2, 4, 2, 256, 128), BF16),
            vmem((2, 3, 2, 256, 128), BF16),
            vmem((4, 512, 256), BF16),
            vmem((4, 128, 128), BF16),
            vmem((2, 256, 128), F32),
            vmem((2, 256, 128), F32),
            vmem((4, 256, 256), BF16),
            vmem((3, 256, 256), BF16),
            vmem((4, 4, 16, 256), BF16),
            vmem((16, 1024), F32),
            pltpu.SemaphoreType.DMA((COPIES,)),
            pltpu.SemaphoreType.DMA((COPIES,)),
            pltpu.SemaphoreType.DMA((LOCALS,)),
        ],
        compiler_params=pltpu.CompilerParams(
            collective_id=0, has_side_effects=True, vmem_limit_bytes=62 * 1024 * 1024
        ),
        name="attention_backward",
    )(lengths[0], queries[0], out_grad[0], keys[0], values[0], layer_input[0])
    return (outs[0][None], outs[1][None], outs[2][None], outs[3])


def solution(mesh):
    placed = (P("dp", "blk", None),) * 5 + (P("dp", None),)
    return jax.shard_map(
        body,
        mesh=mesh,
        in_specs=placed,
        out_specs=(P("dp", "blk", None),) * 3 + (P(("dp", "blk"), None),),
        check_vma=False,
    )
```

```python
import math

import jax
import jax.numpy as jnp
from jax import lax
from jax.experimental import pallas as pl
from jax.experimental.pallas import tpu as pltpu
from jax.sharding import PartitionSpec as P

MESH = pl.DeviceIdType.MESH
F32 = jnp.float32
BF16 = jnp.bfloat16
HEAD = 128
ROPE_BASE = 500000.0
MASKED = -1e30
FAR = 1 << 20
COPIES = 144
LOCALS = 16


def nn(a, b):
    return jnp.dot(a, b, preferred_element_type=F32)


def nt(a, b):
    return lax.dot_general(a, b, (((1,), (1,)), ((), ())), preferred_element_type=F32)


def kernel(
    len_ref, q_in, do_in, k_in, v_in, x_in,
    dq_out, dk_out, dv_out, w_out,
    qbuf, dobuf, kv, xv, xt, xbuf, qs, dos, qsn, dosn, kt, p_f, dp_s, p_t, ds_t, top_s, inv_s, del_s, dqacc,
    dqbuf, part_f, part_b, far_a, far_b, near_m, near_p, gbuf, dkbuf, cosb, sinb, wacc, wb1, r1,
    r2, w_stage, send, recv, loc,
):
    b = lax.axis_index("blk")
    dp = lax.axis_index("dp")
    y, w = b // 4, b % 4
    core = w % 2
    zhi, xx = dp // 4, dp % 4
    yp, y2, ym = (y + 1) % 4, (y + 2) % 4, (y + 3) % 4
    xp, xm = (xx + 1) % 4, (xx + 3) % 4
    scale = 1.0 / math.sqrt(HEAD)
    prompt_len = len_ref[0]
    reject_start = len_ref[0] + len_ref[1]

    count = [0, 0]
    pending = []

    def remote(src, dst, device):
        i = count[0]
        count[0] += 1
        copy = pltpu.make_async_remote_copy(
            src_ref=src, dst_ref=dst, send_sem=send.at[i], recv_sem=recv.at[i],
            device_id=device, device_id_type=MESH,
        )
        copy.start()
        pending.append(copy)
        return copy

    def local(src, dst):
        i = count[1]
        count[1] += 1
        copy = pltpu.make_async_copy(src, dst, loc.at[i])
        copy.start()
        return copy

    def at_blk(yy, ww):
        return {"blk": 4 * yy + ww}

    def at_x(to):
        return {"dp": 4 * zhi + to}

    def at_owner(zz, ww):
        return {"dp": 4 * zz + xx, "blk": 4 * y + ww}

    def tile(i, size):
        return pl.ds(pl.multiple_of(i * size, size), size)

    barrier = pltpu.get_barrier_semaphore()
    for d in range(1, 4):
        for device in (at_blk((y + d) % 4, w), {"dp": 4 * zhi + (xx + d) % 4}):
            pl.semaphore_signal(barrier, 1, device_id=device, device_id_type=MESH)
    for dz in range(4):
        for d in range(4):
            if dz or d:
                pl.semaphore_signal(
                    barrier, 1, device_id=at_owner((zhi + dz) % 4, (w + d) % 4),
                    device_id_type=MESH,
                )
    x_local = local(x_in, xv)
    kv_slots = (tile(4 * y + w, 64), tile(4 * (7 - y) + 3 - w, 64))
    own_kv = []
    for half in range(2):
        for part, ref in ((0, k_in), (1, v_in)):
            own_kv.append(
                local(
                    ref.at[pl.ds(64 * half, 64), tile(w, 128)],
                    kv.at[kv_slots[half], pl.ds(128 * part, 128)],
                )
            )
    own_q = [
        local(q_in.at[:, tile(w, 512)], qbuf.at[w]),
        local(do_in.at[:, tile(w, 512)], dobuf.at[w]),
    ]
    pl.semaphore_wait(barrier, 21)

    def row_slots(ww):
        return tile(4 * y + ww, 64), tile(4 * (7 - y) + 3 - ww, 64)

    kv_first = {}
    for d in (1, 3, 2):
        ww = (w + d) % 4
        kv_first[d] = []
        for half in range(2):
            for part, ref in ((0, k_in), (1, v_in)):
                kv_first[d].append(
                    remote(
                        ref.at[pl.ds(64 * half, 64), tile(ww, 128)],
                        kv.at[kv_slots[half], pl.ds(128 * part, 128)],
                        at_blk(y, ww),
                    )
                )
    q_first, do_first = [], []
    for ref, buf, group in ((q_in, qbuf, q_first), (do_in, dobuf, do_first)):
        for d in (1, 3, 2):
            ww = (w + d) % 4
            group.append(remote(ref.at[:, tile(ww, 512)], buf.at[w], at_blk(y, ww)))

    kv_plus, kv_minus = ([], []), ([], [])

    def spread(ww):
        slots = row_slots(ww)
        for half in range(2):
            kv_plus[half].append(remote(kv.at[slots[half]], kv.at[slots[half]], at_blk(yp, w)))
            slot = slots[1 - half]
            kv_minus[1 - half].append(remote(kv.at[slot], kv.at[slot], at_blk(ym, w)))

    for copy in own_kv:
        copy.wait()
    spread(w)

    x_local.wait()

    def transpose_x(i, carry):
        to = i % 8 // 2
        xt[to, pl.ds((i % 2) * 2, 2), i // 8] = xv[:, tile(i, 128)].T.reshape(2, 64, 128)
        return carry

    lax.fori_loop(0, 32, transpose_x, 0)
    column = tile(w, 128)
    other = tile((w + 2) % 4, 128)
    core_mate = at_blk(y, w + 1 - 2 * core)
    z_mate = at_blk(y, (w + 2) % 4)
    x_first = []
    for d in (1, 3, 2):
        to = (xx + d) % 4
        x_first.append(remote(xt.at[to], xbuf.at[:, 4 - d, :, :, column], at_x(to)))
    x_far = [remote(xt.at[xx], xbuf.at[:, 0, :, :, column], z_mate)]
    x_mate = [remote(xt.at[xx], xbuf.at[:, 0, :, :, column], core_mate)]

    for d in (1, 3, 2):
        for copy in kv_first[d]:
            copy.wait_recv()
        spread((w + 4 - d) % 4)
    xbuf[:, 0, :, :, column] = xt[xx]
    lane_row = lax.broadcasted_iota(jnp.int32, (1, HEAD), 1)
    frequency = jnp.exp(
        -(2.0 * (lane_row % 64).astype(F32) / HEAD) * math.log(ROPE_BASE)
    )
    for half, block in ((0, y), (1, 7 - y)):
        position = 256 * block + lax.broadcasted_iota(jnp.int32, (256, HEAD), 0)
        angles = position.astype(F32) * frequency
        cosb[half] = jnp.cos(angles)
        sinb[half] = jnp.where(lane_row < 64, jnp.sin(angles), -jnp.sin(angles))

    kv_second = []
    for k, d in enumerate((0, 1, 3, 2)):
        ww = (w + 4 - d) % 4
        kv_plus[0][k].wait_recv()
        slot = tile(4 * ym + ww, 64)
        kv_second.append(remote(kv.at[slot], kv.at[slot], at_blk(yp, w)))
        kv_minus[1][k].wait_recv()
        slot = tile(4 * (7 - yp) + 3 - ww, 64)
        kv_second.append(remote(kv.at[slot], kv.at[slot], at_blk(ym, w)))
    for copy in kv_plus[1] + kv_minus[0]:
        copy.wait_recv()

    own_q[0].wait()
    for copy in q_first:
        copy.wait_recv()

    def stack(buf, stacked):
        def one(c, carry):
            half, h = c // 4, c % 4
            for ww in range(4):
                stacked[c, pl.ds(64 * ww, 64)] = buf[ww, tile(half, 64), tile(h, 128)]
            return carry

        lax.fori_loop(0, 8, one, 0, unroll=True)

    stack(qbuf, qs)

    for copy in kv_second:
        copy.wait_recv()

    lane = lax.broadcasted_iota(jnp.int32, (1, 256), 1)
    lane_high = (3 - lane // 64) * 64 + lane % 64
    rows = lax.broadcasted_iota(jnp.int32, (256, 256), 0)
    zero = jnp.zeros((8, 256), F32)

    def softmax_half(half, carry):
        diagonal = y + half * (7 - 2 * y)
        blocks = diagonal + 1
        query_pos = 256 * diagonal + lane + half * (lane_high - lane)
        rejected = query_pos >= reject_start

        def scores(j, tops):
            key_pos = 256 * j + rows
            chosen = jnp.logical_and(key_pos >= prompt_len, key_pos < reject_start)
            shown = jnp.where(rejected, jnp.where(chosen, FAR, key_pos), key_pos)
            bias = jnp.where(shown <= query_pos, 0.0, MASKED)
            key = kv[tile(j, 256), pl.ds(0, 128)]
            out = []
            for h in range(4):
                s = nt(key, qs[4 * half + h]) + bias
                p_f[4 * half + j, h] = s
                out.append(jnp.maximum(tops[h], jnp.max(s.reshape(32, 8, 256), axis=0)))
            return tuple(out)

        tops = lax.fori_loop(0, blocks, scores, (jnp.full((8, 256), MASKED, F32),) * 4)
        for h in range(4):
            top_s[4 * half + h] = jnp.broadcast_to(
                jnp.max(tops[h], axis=0, keepdims=True), (8, 256)
            )
        return carry

    lax.fori_loop(0, 2, softmax_half, 0)

    order = (2, 1, 3, 0)
    for copy in x_first:
        copy.wait_recv()
    for d in order:
        ref = xbuf.at[(y + d) % 4, pl.ds(1, 3), :, :, column]
        x_far.append(remote(ref, ref, z_mate))
        x_mate.append(remote(ref, ref, core_mate))

    own_q[1].wait()
    for copy in do_first:
        copy.wait_recv()
    stack(dobuf, dos)

    def weights_half(half, carry):
        blocks = y + half * (7 - 2 * y) + 1
        tops = [top_s[4 * half + h, pl.ds(0, 1)] for h in range(4)]

        def weights(j, sums):
            value = kv[tile(j, 256), pl.ds(128, 128)]
            slot = 4 * half + j
            totals, dots = [], []
            for h in range(4):
                p = jnp.exp2((p_f[slot, h] - tops[h]) * (scale * math.log2(math.e)))
                p_f[slot, h] = p
                p_t[slot, :, pl.ds(256 * h, 256)] = p.astype(BF16)
                totals.append(sums[0][h] + jnp.sum(p.reshape(32, 8, 256), axis=0))
                d = nt(value, dos[4 * half + h])
                dp_s[slot, h] = d
                dots.append(sums[1][h] + jnp.sum((p * d).reshape(32, 8, 256), axis=0))
            return tuple(totals), tuple(dots)

        totals, dots = lax.fori_loop(0, blocks, weights, ((zero,) * 4, (zero,) * 4))
        for h in range(4):
            inverse = 1.0 / jnp.sum(totals[h], axis=0, keepdims=True)
            delta = jnp.sum(dots[h], axis=0, keepdims=True) * inverse
            inv_s[4 * half + h] = jnp.broadcast_to(inverse, (8, 256))
            del_s[4 * half + h] = jnp.broadcast_to(delta, (8, 256))
        return carry

    lax.fori_loop(0, 2, weights_half, 0)

    def scale_rows(c, carry):
        per_row = jnp.broadcast_to(inv_s[c, pl.ds(0, 1)], (128, 256)).T
        dosn[c] = (dos[c].astype(F32) * per_row).astype(BF16)
        qsn[c] = (qs[c].astype(F32) * (per_row * scale)).astype(BF16)
        return carry

    lax.fori_loop(0, 8, scale_rows, 0, unroll=True)
    def sums_for(yy, left, right):
        g = (yy - y + 4) // 5
        low = nn(left[4 + yy], right[pl.ds(4, 4)].reshape(1024, 128))
        more = nn(
            left[g * (11 - yy) + (1 - g) * yy], right[pl.ds(4 * g, 4)].reshape(1024, 128)
        )
        keep = g.astype(F32)
        return low + more * (1.0 - keep), more * keep

    def own_sums(left, right):
        low = nn(left[4 + y], right[pl.ds(4, 4)].reshape(1024, 128))
        low = low + nn(left[y], right[pl.ds(0, 4)].reshape(1024, 128))
        return low, nn(left[11 - y], right[pl.ds(4, 4)].reshape(1024, 128))

    def reduce_first(part, left, right):
        low, high = sums_for(y2, left, right)
        part_b[part, y2, 0] = low.astype(BF16)
        part_b[part, y2, 1] = high.astype(BF16)
        return (
            remote(part_b.at[part, y2, 0], far_a.at[part], at_blk(yp, w)),
            remote(part_b.at[part, y2, 1], far_b.at[part], at_blk(ym, w)),
        )

    def reduce_middle(part, left, right):
        for yy in (yp, ym):
            low, high = sums_for(yy, left, right)
            part_f[part, yy, 0] = low
            part_f[part, yy, 1] = high

    def reduce_second(part, far):
        out = []
        far[0].wait_recv()
        part_b[part, yp, 0] = (part_f[part, yp, 0] + far_a[part].astype(F32)).astype(BF16)
        part_b[part, yp, 1] = part_f[part, yp, 1].astype(BF16)
        out.append(remote(part_b.at[part, yp], near_m.at[part], at_blk(yp, w)))
        far[1].wait_recv()
        part_b[part, ym, 0] = part_f[part, ym, 0].astype(BF16)
        part_b[part, ym, 1] = (part_f[part, ym, 1] + far_b[part].astype(F32)).astype(BF16)
        out.append(remote(part_b.at[part, ym], near_p.at[part], at_blk(ym, w)))
        return out

    def reduce_own(part, left, right):
        low, high = own_sums(left, right)
        part_f[part, y, 0] = low
        part_f[part, y, 1] = high

    far_v = reduce_first(1, p_t, dosn)
    reduce_middle(1, p_t, dosn)

    def grads_half(half, carry):
        blocks = y + half * (7 - 2 * y) + 1
        deltas = [del_s[4 * half + h, pl.ds(0, 1)] for h in range(4)]

        def grads(j, carry):
            slot = 4 * half + j
            for h in range(4):
                ds = p_f[slot, h] * (dp_s[slot, h] - deltas[h])
                ds_t[slot, :, pl.ds(256 * h, 256)] = ds.astype(BF16)
            return carry

        return lax.fori_loop(0, blocks, grads, carry)

    lax.fori_loop(0, 2, grads_half, 0)

    far_k = reduce_first(0, ds_t, qsn)
    reduce_middle(0, ds_t, qsn)
    near_v = reduce_second(1, far_v)
    reduce_own(1, p_t, dosn)
    reduce_own(0, ds_t, qsn)
    near_k = reduce_second(0, far_k)
    def transpose_k(j, carry):
        kt[j] = kv[tile(j, 256), pl.ds(0, 128)].T
        return carry

    lax.fori_loop(0, 8, transpose_k, 0, unroll=2)

    def query_half(half, carry):
        blocks = y + half * (7 - 2 * y) + 1
        dqacc[...] = jnp.zeros_like(dqacc)

        def one(j, carry):
            for h in range(4):
                dqacc[h] += nn(kt[j], ds_t[4 * half + j, :, pl.ds(256 * h, 256)])
            return carry

        lax.fori_loop(0, blocks, one, 0)
        for h in range(4):
            dq = dqacc[h] * (inv_s[4 * half + h, pl.ds(0, 1)] * scale)
            dq = dq.T.astype(BF16)
            for ww in range(4):
                dqbuf[ww, tile(half, 64), pl.ds(128 * h, 128)] = dq[64 * ww : 64 * ww + 64]
        return carry

    lax.fori_loop(0, 2, query_half, 0)
    own_out, far_out = [local(dqbuf.at[w], dq_out.at[:, tile(w, 512)])], []
    for d in (2, 1, 3):
        ww = (w + d) % 4
        far_out.append(remote(dqbuf.at[ww], dq_out.at[:, tile(w, 512)], at_blk(y, ww)))
    for copy in near_v:
        copy.wait_recv()

    def gathered(part, half):
        own = part_f[part, y, half]
        return own + near_m[part, half].astype(F32) + near_p[part, half].astype(F32)

    for half in range(2):
        value_grad = gathered(1, half).astype(BF16)
        for ww in range(4):
            at = 64 * ww if half == 0 else 64 * (3 - ww)
            rows_at = pl.ds(128 * ww + 64 * half, 64)
            gbuf[0, rows_at, pl.ds(128, 128)] = value_grad[at : at + 64]

    def gather_near(part):
        lanes = pl.ds(128 * part, 128)
        return [
            remote(gbuf.at[0, :, lanes], gbuf.at[3, :, lanes], at_x(xp)),
            remote(gbuf.at[0, :, lanes], gbuf.at[1, :, lanes], at_x(xm)),
        ]

    def gather_far(part, near):
        lanes = pl.ds(128 * part, 128)
        low, high = pl.ds(0, 256), pl.ds(256, 256)
        near[0].wait_recv()
        first = remote(gbuf.at[3, low, lanes], gbuf.at[2, low, lanes], at_x(xp))
        near[1].wait_recv()
        return [first, remote(gbuf.at[1, high, lanes], gbuf.at[2, high, lanes], at_x(xm))]

    g_v = gather_near(1)
    x_third = []

    def third_x(k):
        x_far[k].wait_recv()
        if k == 0:
            ref = xbuf.at[:, 0, :, :, other]
        else:
            ref = xbuf.at[(y + order[k - 1]) % 4, pl.ds(1, 3), :, :, other]
        x_third.append(remote(ref, ref, core_mate))

    third_x(0)
    for copy in near_k:
        copy.wait_recv()
    for half in range(2):
        key_sum = gathered(0, half)
        key_grad = key_sum.astype(BF16)
        key_pre = (
            key_sum * cosb[half] + pltpu.roll(key_sum, 64, 1) * sinb[half]
        ).astype(BF16)
        for ww in range(4):
            at = 64 * ww if half == 0 else 64 * (3 - ww)
            gbuf[0, pl.ds(128 * ww + 64 * half, 64), pl.ds(0, 128)] = key_pre[at : at + 64]
            dkbuf[ww, pl.ds(64 * half, 64)] = key_grad[at : at + 64]
    g_k = gather_near(0)
    third_x(1)
    values_out = pl.ds(128, 128)
    own_out.append(local(dkbuf.at[w], dk_out.at[:, column]))
    own_out.append(local(gbuf.at[0, tile(w, 128), values_out], dv_out.at[:, column]))
    for d in (2, 1, 3):
        ww = (w + d) % 4
        far_out.append(remote(dkbuf.at[ww], dk_out.at[:, column], at_blk(y, ww)))
        far_out.append(
            remote(gbuf.at[0, tile(ww, 128), values_out], dv_out.at[:, column], at_blk(y, ww))
        )

    far_g_v = gather_far(1, g_v)
    third_x(2)

    def weights_of(part, to, rels):
        lanes = pl.ds(128 * part, 128)
        total = nn(xbuf[to, rels[0]].reshape(256, 512), gbuf[rels[0], :, lanes])
        for rel in rels[1:]:
            total = total + nn(xbuf[to, rel].reshape(256, 512), gbuf[rel, :, lanes])
        return total

    def near_tile(part, d):
        to = (y + d) % 4
        wacc[part, to] = weights_of(part, to, (0, 1, 3))

    def far_tiles(part):
        out = []
        for d in order[:3]:
            to = (y + d) % 4
            wb1[part, to] = (wacc[part, to] + weights_of(part, to, (2,))).astype(BF16)
            out.append(remote(wb1.at[part, to], r1.at[part, d - 1], at_blk(to, w)))
        return out

    def owner_sums(part, own, y_sums):
        total = own
        for copy in y_sums:
            copy.wait_recv()
        for d in range(3):
            total = total + r1[part, d].astype(F32)
        wb1[part, y] = total.astype(BF16)
        out = []
        for dz in (2, 1, 3, 0):
            zz = (zhi + dz) % 4
            for d in (2, 1, 3, 0):
                ww = (w + d) % 4
                piece = pl.ds(pl.multiple_of(64 * zz + 16 * ww, 16), 16)
                if dz or d:
                    out.append(
                        remote(wb1.at[part, y, piece], r2.at[part, zhi, w], at_owner(zz, ww))
                    )
                else:
                    r2[part, zhi, w] = wb1[part, y, piece]
        return out

    for k in range(3):
        x_mate[k].wait_recv()
        x_third[k].wait_recv()
    near_tile(1, 2)
    near_tile(1, 1)
    third_x(3)
    far_g_k = gather_far(0, g_k)
    near_tile(0, 2)
    near_tile(0, 1)
    x_mate[3].wait_recv()
    x_third[3].wait_recv()
    near_tile(1, 3)
    for copy in far_g_v:
        copy.wait_recv()
    y_sums_v = far_tiles(1)
    near_tile(0, 3)
    for copy in far_g_k:
        copy.wait_recv()
    y_sums_k = far_tiles(0)
    third_x(4)
    x_mate[4].wait_recv()
    x_third[4].wait_recv()
    own_v = weights_of(1, y, (0, 1, 2, 3))
    wacc[0, y] = weights_of(0, y, (0, 1, 2, 3))
    finals = owner_sums(1, own_v, y_sums_v)
    finals = finals + owner_sums(0, wacc[0, y], y_sums_k)
    for copy in finals:
        copy.wait_recv()
    for part in range(2):
        for ww in range(4):
            total = r2[part, 0, ww].astype(F32)
            for zz in range(1, 4):
                total = total + r2[part, zz, ww].astype(F32)
            w_stage[:, pl.ds(512 * part + 128 * ww, 128)] = total
    own_out.append(local(w_stage, w_out))
    for copy in own_out:
        copy.wait()
    for copy in far_out:
        copy.wait_recv()
    for copy in pending:
        copy.wait_send()


def body(queries, keys, values, out_grad, layer_input, lengths):
    anywhere = pl.BlockSpec(memory_space=pltpu.HBM)
    vmem = pltpu.VMEM
    outs = pl.pallas_call(
        kernel,
        out_shape=(
            jax.ShapeDtypeStruct((128, 2048), BF16),
            jax.ShapeDtypeStruct((128, 512), BF16),
            jax.ShapeDtypeStruct((128, 512), BF16),
            jax.ShapeDtypeStruct((16, 1024), F32),
        ),
        in_specs=[pl.BlockSpec(memory_space=pltpu.SMEM)] + [anywhere] * 5,
        out_specs=(anywhere,) * 4,
        scratch_shapes=[
            vmem((4, 128, 512), BF16),
            vmem((4, 128, 512), BF16),
            vmem((2048, 256), BF16),
            vmem((128, 4096), BF16),
            vmem((4, 4, 4, 64, 128), BF16),
            vmem((4, 4, 4, 64, 512), BF16),
            vmem((8, 256, 128), BF16),
            vmem((8, 256, 128), BF16),
            vmem((8, 256, 128), BF16),
            vmem((8, 256, 128), BF16),
            vmem((8, 128, 256), BF16),
            vmem((12, 4, 256, 256), F32),
            vmem((12, 4, 256, 256), F32),
            vmem((12, 256, 1024), BF16),
            vmem((12, 256, 1024), BF16),
            vmem((8, 8, 256), F32),
            vmem((8, 8, 256), F32),
            vmem((8, 8, 256), F32),
            vmem((4, 128, 256), F32),
            vmem((4, 128, 512), BF16),
            vmem((2, 4, 2, 256, 128), F32),
            vmem((2, 4, 2, 256, 128), BF16),
            vmem((2, 256, 128), BF16),
            vmem((2, 256, 128), BF16),
            vmem((2, 2, 256, 128), BF16),
            vmem((2, 2, 256, 128), BF16),
            vmem((4, 512, 256), BF16),
            vmem((4, 128, 128), BF16),
            vmem((2, 256, 128), F32),
            vmem((2, 256, 128), F32),
            vmem((2, 4, 256, 128), F32),
            vmem((2, 4, 256, 128), BF16),
            vmem((2, 3, 256, 128), BF16),
            vmem((2, 4, 4, 16, 128), BF16),
            vmem((16, 1024), F32),
            pltpu.SemaphoreType.DMA((COPIES,)),
            pltpu.SemaphoreType.DMA((COPIES,)),
            pltpu.SemaphoreType.DMA((LOCALS,)),
        ],
        compiler_params=pltpu.CompilerParams(
            collective_id=0, has_side_effects=True, vmem_limit_bytes=62 * 1024 * 1024
        ),
        name="attention_backward",
    )(lengths[0], queries[0], out_grad[0], keys[0], values[0], layer_input[0])
    return (outs[0][None], outs[1][None], outs[2][None], outs[3])


def solution(mesh):
    placed = (P("dp", "blk", None),) * 5 + (P("dp", None),)
    return jax.shard_map(
        body,
        mesh=mesh,
        in_specs=placed,
        out_specs=(P("dp", "blk", None),) * 3 + (P(("dp", "blk"), None),),
        check_vma=False,
    )
```

```python
import math

import jax
import jax.numpy as jnp
from jax import lax
from jax.experimental import pallas as pl
from jax.experimental.pallas import tpu as pltpu
from jax.sharding import PartitionSpec as P

MESH = pl.DeviceIdType.MESH
F32 = jnp.float32
BF16 = jnp.bfloat16
HEAD = 128
ROPE_BASE = 500000.0
MASKED = -1e30
FAR = 1 << 20
SENDS = 11
ARRIVALS = 51
LOCALS = 17


def nn(a, b):
    return jnp.dot(a, b, preferred_element_type=F32)


def nt(a, b):
    return lax.dot_general(a, b, (((1,), (1,)), ((), ())), preferred_element_type=F32)


def kernel(
    len_ref, q_in, do_in, k_in, v_in, x_in,
    dq_out, dk_out, dv_out, w_out,
    kvin, qbuf, dobuf, kv, xv, xt, xbuf, qs, dos, qsn, dosn, kt, p_f, dp_s, p_t, ds_t, top_s, inv_s, del_s, dqacc,
    dqbuf, part_f, part_b, far_a, far_b, near_m, near_p, gbuf, dkbuf, cosb, sinb, wacc, wb1, r1,
    r2, w_stage, send, recv, loc,
):
    b = lax.axis_index("blk")
    dp = lax.axis_index("dp")
    y, w = b // 4, b % 4
    core = w % 2
    zhi, xx = dp // 4, dp % 4
    yp, y2, ym = (y + 1) % 4, (y + 2) % 4, (y + 3) % 4
    xp, xm = (xx + 1) % 4, (xx + 3) % 4
    scale = 1.0 / math.sqrt(HEAD)
    prompt_len = len_ref[0]
    reject_start = len_ref[0] + len_ref[1]

    count = [0, 0, 0]

    def covering(size):
        if size % 8192:
            return kv.at[pl.ds(0, size // 256), pl.ds(0, 128)]
        if size <= 1 << 20:
            return kv.at[pl.ds(0, size // 512)]
        return ds_t.at[pl.ds(0, size >> 19)]

    def bytes_of(ref):
        return math.prod(ref.shape) * ref.dtype.itemsize

    def wait_bytes(sem, size):
        ref = covering(size)
        pltpu.make_async_copy(ref, ref, sem).wait()

    class Sends:
        def __init__(self):
            self.at = count[2]
            self.size = 0
            count[2] += 1

        def wait(self):
            wait_bytes(send.at[self.at], self.size)

    class Arrivals:
        def __init__(self):
            self.at = count[0]
            self.size = 0
            count[0] += 1

        def wait_recv(self):
            wait_bytes(recv.at[self.at], self.size)

    def remote(src, dst, device, sends, arrivals=None):
        arrivals = arrivals or Arrivals()
        pltpu.make_async_remote_copy(
            src_ref=src, dst_ref=dst, send_sem=send.at[sends.at], recv_sem=recv.at[arrivals.at],
            device_id=device, device_id_type=MESH,
        ).start()
        sends.size += bytes_of(src)
        arrivals.size += bytes_of(src)
        return arrivals

    def local(src, dst):
        i = count[1]
        count[1] += 1
        copy = pltpu.make_async_copy(src, dst, loc.at[i])
        copy.start()
        return copy

    def at_blk(yy, ww):
        return {"blk": 4 * yy + ww}

    def at_x(to):
        return {"dp": 4 * zhi + to}

    def at_owner(zz, ww):
        return {"dp": 4 * zz + xx, "blk": 4 * y + ww}

    def tile(i, size):
        return pl.ds(pl.multiple_of(i * size, size), size)

    barrier = pltpu.get_barrier_semaphore()
    for d in range(1, 4):
        for device in (at_blk((y + d) % 4, w), {"dp": 4 * zhi + (xx + d) % 4}):
            pl.semaphore_signal(barrier, 1, device_id=device, device_id_type=MESH)
    for dz in range(4):
        for d in range(4):
            if dz or d:
                pl.semaphore_signal(
                    barrier, 1, device_id=at_owner((zhi + dz) % 4, (w + d) % 4),
                    device_id_type=MESH,
                )
    staged = [local(ref, kvin.at[part]) for part, ref in ((0, k_in), (1, v_in))]
    for ref, stage in ((q_in, p_t), (do_in, ds_t)):
        for side in range(2):
            staged.append(
                local(ref.at[:, pl.ds(1024 * side, 1024)], stage.at[0, pl.ds(128 * side, 128)])
            )
    x_local = local(x_in, xv)
    kv_slots = (tile(4 * y + w, 64), tile(4 * (7 - y) + 3 - w, 64))
    own_kv = []
    for half in range(2):
        for part, ref in ((0, k_in), (1, v_in)):
            own_kv.append(
                local(
                    ref.at[pl.ds(64 * half, 64), tile(w, 128)],
                    kv.at[kv_slots[half], pl.ds(128 * part, 128)],
                )
            )
    own_q = [
        local(q_in.at[:, tile(w, 512)], qbuf.at[w]),
        local(do_in.at[:, tile(w, 512)], dobuf.at[w]),
    ]
    pl.semaphore_wait(barrier, 21)

    def row_slots(ww):
        return tile(4 * y + ww, 64), tile(4 * (7 - y) + 3 - ww, 64)

    for copy in staged[:2]:
        copy.wait()
    kv_first = {}
    sends_kv = Sends()
    for d in (1, 3, 2):
        ww = (w + d) % 4
        kv_first[d] = Arrivals()
        for half in range(2):
            for part in range(2):
                remote(
                    kvin.at[part, pl.ds(64 * half, 64), tile(ww, 128)],
                    kv.at[kv_slots[half], pl.ds(128 * part, 128)],
                    at_blk(y, ww), sends_kv, kv_first[d],
                )
    for copy in staged[2:]:
        copy.wait()
    sends_q, sends_do, q_first, do_first = Sends(), Sends(), Arrivals(), Arrivals()
    for stage, buf, sends, group in (
        (p_t, qbuf, sends_q, q_first), (ds_t, dobuf, sends_do, do_first),
    ):
        for d in (1, 3, 2):
            ww = (w + d) % 4
            src = stage.at[0, tile(ww // 2, 128), tile(ww % 2, 512)]
            remote(src, buf.at[w], at_blk(y, ww), sends, group)

    sends_spread, kv_rest = Sends(), Arrivals()
    kv_plus, kv_minus = [], []

    def spread(ww):
        slots = row_slots(ww)
        low, high = kv.at[slots[0]], kv.at[slots[1]]
        kv_plus.append(remote(low, low, at_blk(yp, w), sends_spread))
        kv_minus.append(remote(high, high, at_blk(ym, w), sends_spread))
        remote(high, high, at_blk(yp, w), sends_spread, kv_rest)
        remote(low, low, at_blk(ym, w), sends_spread, kv_rest)

    for copy in own_kv:
        copy.wait()
    spread(w)

    x_local.wait()

    def transpose_x(i, carry):
        to = i % 8 // 2
        xt[to, pl.ds((i % 2) * 2, 2), i // 8] = xv[:, tile(i, 128)].T.reshape(2, 64, 128)
        return carry

    lax.fori_loop(0, 32, transpose_x, 0)
    column = tile(w, 128)
    other = tile((w + 2) % 4, 128)
    core_mate = at_blk(y, w + 1 - 2 * core)
    z_mate = at_blk(y, (w + 2) % 4)
    sends_x, sends_first, x_first = Sends(), Sends(), Arrivals()
    for d in (1, 3, 2):
        to = (xx + d) % 4
        remote(xt.at[to], xbuf.at[:, 4 - d, :, :, column], at_x(to), sends_first, x_first)
    x_far = [remote(xt.at[xx], xbuf.at[:, 0, :, :, column], z_mate, sends_x)]
    x_mate = [remote(xt.at[xx], xbuf.at[:, 0, :, :, column], core_mate, sends_x)]

    for d in (1, 3, 2):
        kv_first[d].wait_recv()
        spread((w + 4 - d) % 4)
    xbuf[:, 0, :, :, column] = xt[xx]
    lane_row = lax.broadcasted_iota(jnp.int32, (1, HEAD), 1)
    frequency = jnp.exp(
        -(2.0 * (lane_row % 64).astype(F32) / HEAD) * math.log(ROPE_BASE)
    )
    for half, block in ((0, y), (1, 7 - y)):
        position = 256 * block + lax.broadcasted_iota(jnp.int32, (256, HEAD), 0)
        angles = position.astype(F32) * frequency
        cosb[half] = jnp.cos(angles)
        sinb[half] = jnp.where(lane_row < 64, jnp.sin(angles), -jnp.sin(angles))

    kv_second = Arrivals()
    for k, d in enumerate((0, 1, 3, 2)):
        ww = (w + 4 - d) % 4
        kv_plus[k].wait_recv()
        ref = kv.at[tile(4 * ym + ww, 64)]
        remote(ref, ref, at_blk(yp, w), sends_spread, kv_second)
        kv_minus[k].wait_recv()
        ref = kv.at[tile(4 * (7 - yp) + 3 - ww, 64)]
        remote(ref, ref, at_blk(ym, w), sends_spread, kv_second)
    kv_rest.wait_recv()

    own_q[0].wait()
    q_first.wait_recv()

    def stack(buf, stacked):
        def one(c, carry):
            half, h = c // 4, c % 4
            for ww in range(4):
                stacked[c, pl.ds(64 * ww, 64)] = buf[ww, tile(half, 64), tile(h, 128)]
            return carry

        lax.fori_loop(0, 8, one, 0, unroll=True)

    stack(qbuf, qs)

    kv_second.wait_recv()

    lane = lax.broadcasted_iota(jnp.int32, (1, 256), 1)
    lane_high = (3 - lane // 64) * 64 + lane % 64
    rows = lax.broadcasted_iota(jnp.int32, (256, 256), 0)
    zero = jnp.zeros((8, 256), F32)

    def softmax_half(half, carry):
        diagonal = y + half * (7 - 2 * y)
        blocks = diagonal + 1
        query_pos = 256 * diagonal + lane + half * (lane_high - lane)
        rejected = query_pos >= reject_start

        def scores(j, tops):
            key_pos = 256 * j + rows
            chosen = jnp.logical_and(key_pos >= prompt_len, key_pos < reject_start)
            shown = jnp.where(rejected, jnp.where(chosen, FAR, key_pos), key_pos)
            bias = jnp.where(shown <= query_pos, 0.0, MASKED)
            key = kv[tile(j, 256), pl.ds(0, 128)]
            out = []
            for h in range(4):
                s = nt(key, qs[4 * half + h]) + bias
                p_f[4 * half + j, h] = s
                out.append(jnp.maximum(tops[h], jnp.max(s.reshape(32, 8, 256), axis=0)))
            return tuple(out)

        tops = lax.fori_loop(0, blocks, scores, (jnp.full((8, 256), MASKED, F32),) * 4)
        for h in range(4):
            top_s[4 * half + h] = jnp.broadcast_to(
                jnp.max(tops[h], axis=0, keepdims=True), (8, 256)
            )
        return carry

    lax.fori_loop(0, 2, softmax_half, 0)

    own_q[1].wait()
    do_first.wait_recv()
    stack(dobuf, dos)

    def weights_half(half, carry):
        blocks = y + half * (7 - 2 * y) + 1
        tops = [top_s[4 * half + h, pl.ds(0, 1)] for h in range(4)]

        def weights(j, sums):
            value = kv[tile(j, 256), pl.ds(128, 128)]
            slot = 4 * half + j
            totals, dots = [], []
            for h in range(4):
                p = jnp.exp2((p_f[slot, h] - tops[h]) * (scale * math.log2(math.e)))
                p_f[slot, h] = p
                p_t[slot, :, pl.ds(256 * h, 256)] = p.astype(BF16)
                totals.append(sums[0][h] + jnp.sum(p.reshape(32, 8, 256), axis=0))
                d = nt(value, dos[4 * half + h])
                dp_s[slot, h] = d
                dots.append(sums[1][h] + jnp.sum((p * d).reshape(32, 8, 256), axis=0))
            return tuple(totals), tuple(dots)

        totals, dots = lax.fori_loop(0, blocks, weights, ((zero,) * 4, (zero,) * 4))
        for h in range(4):
            inverse = 1.0 / jnp.sum(totals[h], axis=0, keepdims=True)
            delta = jnp.sum(dots[h], axis=0, keepdims=True) * inverse
            inv_s[4 * half + h] = jnp.broadcast_to(inverse, (8, 256))
            del_s[4 * half + h] = jnp.broadcast_to(delta, (8, 256))
        return carry

    sends_q.wait()
    weights_half(0, 0)
    order = (2, 1, 3, 0)
    x_first.wait_recv()
    for d in order:
        ref = xbuf.at[(y + d) % 4, pl.ds(1, 3), :, :, column]
        x_far.append(remote(ref, ref, z_mate, sends_x))
        x_mate.append(remote(ref, ref, core_mate, sends_x))
    weights_half(1, 0)

    def scale_rows(c, carry):
        per_row = jnp.broadcast_to(inv_s[c, pl.ds(0, 1)], (128, 256)).T
        dosn[c] = (dos[c].astype(F32) * per_row).astype(BF16)
        qsn[c] = (qs[c].astype(F32) * (per_row * scale)).astype(BF16)
        return carry

    lax.fori_loop(0, 8, scale_rows, 0, unroll=True)
    def sums_for(yy, left, right):
        g = (yy - y + 4) // 5
        low = nn(left[4 + yy], right[pl.ds(4, 4)].reshape(1024, 128))
        more = nn(
            left[g * (11 - yy) + (1 - g) * yy], right[pl.ds(4 * g, 4)].reshape(1024, 128)
        )
        keep = g.astype(F32)
        return low + more * (1.0 - keep), more * keep

    def own_sums(left, right):
        low = nn(left[4 + y], right[pl.ds(4, 4)].reshape(1024, 128))
        low = low + nn(left[y], right[pl.ds(0, 4)].reshape(1024, 128))
        return low, nn(left[11 - y], right[pl.ds(4, 4)].reshape(1024, 128))

    def reduce_first(part, left, right):
        low, high = sums_for(y2, left, right)
        part_b[part, y2, 0] = low.astype(BF16)
        part_b[part, y2, 1] = high.astype(BF16)
        return (
            remote(part_b.at[part, y2, 0], far_a.at[part], at_blk(yp, w), sends_sum),
            remote(part_b.at[part, y2, 1], far_b.at[part], at_blk(ym, w), sends_sum),
        )

    def reduce_middle(part, left, right):
        for yy in (yp, ym):
            low, high = sums_for(yy, left, right)
            part_f[part, yy, 0] = low
            part_f[part, yy, 1] = high

    def reduce_second(part, far):
        out = []
        far[0].wait_recv()
        part_b[part, yp, 0] = (part_f[part, yp, 0] + far_a[part].astype(F32)).astype(BF16)
        part_b[part, yp, 1] = part_f[part, yp, 1].astype(BF16)
        out.append(remote(part_b.at[part, yp], near_m.at[part], at_blk(yp, w), sends_sum))
        far[1].wait_recv()
        part_b[part, ym, 0] = part_f[part, ym, 0].astype(BF16)
        part_b[part, ym, 1] = (part_f[part, ym, 1] + far_b[part].astype(F32)).astype(BF16)
        out.append(remote(part_b.at[part, ym], near_p.at[part], at_blk(ym, w), sends_sum))
        return out

    def reduce_own(part, left, right):
        low, high = own_sums(left, right)
        part_f[part, y, 0] = low
        part_f[part, y, 1] = high

    sends_sum = Sends()
    far_v = reduce_first(1, p_t, dosn)
    reduce_middle(1, p_t, dosn)

    sends_do.wait()
    def grads_half(half, carry):
        blocks = y + half * (7 - 2 * y) + 1
        deltas = [del_s[4 * half + h, pl.ds(0, 1)] for h in range(4)]

        def grads(j, carry):
            slot = 4 * half + j
            for h in range(4):
                ds = p_f[slot, h] * (dp_s[slot, h] - deltas[h])
                ds_t[slot, :, pl.ds(256 * h, 256)] = ds.astype(BF16)
            return carry

        return lax.fori_loop(0, blocks, grads, carry)

    lax.fori_loop(0, 2, grads_half, 0)

    far_k = reduce_first(0, ds_t, qsn)
    reduce_middle(0, ds_t, qsn)
    near_v = reduce_second(1, far_v)
    reduce_own(1, p_t, dosn)
    reduce_own(0, ds_t, qsn)
    near_k = reduce_second(0, far_k)
    def transpose_k(j, carry):
        kt[j] = kv[tile(j, 256), pl.ds(0, 128)].T
        return carry

    lax.fori_loop(0, 8, transpose_k, 0, unroll=2)

    def query_half(half, carry):
        blocks = y + half * (7 - 2 * y) + 1
        dqacc[...] = jnp.zeros_like(dqacc)

        def one(j, carry):
            for h in range(4):
                dqacc[h] += nn(kt[j], ds_t[4 * half + j, :, pl.ds(256 * h, 256)])
            return carry

        lax.fori_loop(0, blocks, one, 0)
        for h in range(4):
            dq = dqacc[h] * (inv_s[4 * half + h, pl.ds(0, 1)] * scale)
            dq = dq.T.astype(BF16)
            for ww in range(4):
                dqbuf[ww, tile(half, 64), pl.ds(128 * h, 128)] = dq[64 * ww : 64 * ww + 64]
        return carry

    lax.fori_loop(0, 2, query_half, 0)
    for copy in near_v:
        copy.wait_recv()

    def gathered(part, half):
        own = part_f[part, y, half]
        return own + near_m[part, half].astype(F32) + near_p[part, half].astype(F32)

    for half in range(2):
        value_grad = gathered(1, half).astype(BF16)
        for ww in range(4):
            at = 64 * ww if half == 0 else 64 * (3 - ww)
            rows_at = pl.ds(128 * ww + 64 * half, 64)
            gbuf[0, rows_at, pl.ds(128, 128)] = value_grad[at : at + 64]

    def gather_near(part):
        lanes = pl.ds(128 * part, 128)
        return [
            remote(gbuf.at[0, :, lanes], gbuf.at[3, :, lanes], at_x(xp), sends_g),
            remote(gbuf.at[0, :, lanes], gbuf.at[1, :, lanes], at_x(xm), sends_g),
        ]

    def gather_far(part, near):
        lanes = pl.ds(128 * part, 128)
        low, high = pl.ds(0, 256), pl.ds(256, 256)
        near[0].wait_recv()
        src, dst = gbuf.at[3, low, lanes], gbuf.at[2, low, lanes]
        first = remote(src, dst, at_x(xp), sends_g)
        near[1].wait_recv()
        src, dst = gbuf.at[1, high, lanes], gbuf.at[2, high, lanes]
        return [first, remote(src, dst, at_x(xm), sends_g)]

    sends_g = Sends()
    g_v = gather_near(1)
    x_third = []

    def third_x(k):
        x_far[k].wait_recv()
        if k == 0:
            ref = xbuf.at[:, 0, :, :, other]
        else:
            ref = xbuf.at[(y + order[k - 1]) % 4, pl.ds(1, 3), :, :, other]
        x_third.append(remote(ref, ref, core_mate, sends_x))

    third_x(0)
    for copy in near_k:
        copy.wait_recv()
    for half in range(2):
        key_sum = gathered(0, half)
        key_grad = key_sum.astype(BF16)
        key_pre = (
            key_sum * cosb[half] + pltpu.roll(key_sum, 64, 1) * sinb[half]
        ).astype(BF16)
        for ww in range(4):
            at = 64 * ww if half == 0 else 64 * (3 - ww)
            gbuf[0, pl.ds(128 * ww + 64 * half, 64), pl.ds(0, 128)] = key_pre[at : at + 64]
            dkbuf[ww, pl.ds(64 * half, 64)] = key_grad[at : at + 64]
    g_k = gather_near(0)
    third_x(1)
    far_g_v = gather_far(1, g_v)
    third_x(2)

    def weights_of(part, to, rels):
        lanes = pl.ds(128 * part, 128)
        total = nn(xbuf[to, rels[0]].reshape(256, 512), gbuf[rels[0], :, lanes])
        for rel in rels[1:]:
            total = total + nn(xbuf[to, rel].reshape(256, 512), gbuf[rel, :, lanes])
        return total

    def near_tile(part, d):
        to = (y + d) % 4
        wacc[part, to] = weights_of(part, to, (0, 1, 3))

    def far_tiles(part):
        out = Arrivals()
        for d in order[:3]:
            to = (y + d) % 4
            wb1[part, to] = (wacc[part, to] + weights_of(part, to, (2,))).astype(BF16)
            remote(wb1.at[part, to], r1.at[part, d - 1], at_blk(to, w), sends_w, out)
        return out

    def owner_sums(part, own, y_sums):
        total = own
        y_sums.wait_recv()
        for d in range(3):
            total = total + r1[part, d].astype(F32)
        wb1[part, y] = total.astype(BF16)
        for dz in (2, 1, 3, 0):
            zz = (zhi + dz) % 4
            for d in (2, 1, 3, 0):
                ww = (w + d) % 4
                piece = pl.ds(pl.multiple_of(64 * zz + 16 * ww, 16), 16)
                if dz or d:
                    remote(
                        wb1.at[part, y, piece], r2.at[part, zhi, w], at_owner(zz, ww),
                        sends_last, finals,
                    )
                else:
                    r2[part, zhi, w] = wb1[part, y, piece]

    sends_w, sends_last, finals = Sends(), Sends(), Arrivals()
    for k in range(3):
        x_mate[k].wait_recv()
        x_third[k].wait_recv()
    near_tile(1, 2)
    near_tile(1, 1)
    third_x(3)
    sends_out, far_out = Sends(), Arrivals()
    values_out = pl.ds(128, 128)
    own_out = [
        local(dqbuf.at[w], dq_out.at[:, tile(w, 512)]),
        local(dkbuf.at[w], dk_out.at[:, column]),
        local(gbuf.at[0, tile(w, 128), values_out], dv_out.at[:, column]),
    ]
    for d in (2, 1, 3):
        ww = (w + d) % 4
        values = gbuf.at[0, tile(ww, 128), values_out]
        remote(dqbuf.at[ww], dq_out.at[:, tile(w, 512)], at_blk(y, ww), sends_out, far_out)
        remote(dkbuf.at[ww], dk_out.at[:, column], at_blk(y, ww), sends_out, far_out)
        remote(values, dv_out.at[:, column], at_blk(y, ww), sends_out, far_out)
    far_g_k = gather_far(0, g_k)
    near_tile(0, 2)
    near_tile(0, 1)
    x_mate[3].wait_recv()
    x_third[3].wait_recv()
    near_tile(1, 3)
    for copy in far_g_v:
        copy.wait_recv()
    y_sums_v = far_tiles(1)
    near_tile(0, 3)
    third_x(4)
    for copy in far_g_k:
        copy.wait_recv()
    y_sums_k = far_tiles(0)
    x_mate[4].wait_recv()
    x_third[4].wait_recv()
    own_v = weights_of(1, y, (0, 1, 2, 3))
    wacc[0, y] = weights_of(0, y, (0, 1, 2, 3))
    owner_sums(1, own_v, y_sums_v)
    owner_sums(0, wacc[0, y], y_sums_k)
    finals.wait_recv()
    for part in range(2):
        for ww in range(4):
            total = r2[part, 0, ww].astype(F32)
            for zz in range(1, 4):
                total = total + r2[part, zz, ww].astype(F32)
            w_stage[:, pl.ds(512 * part + 128 * ww, 128)] = total
    own_out.append(local(w_stage, w_out))
    for copy in own_out:
        copy.wait()
    far_out.wait_recv()
    assert count == [ARRIVALS, LOCALS, SENDS], count
    for sends in (
        sends_kv, sends_spread, sends_first, sends_x, sends_sum, sends_g, sends_out, sends_w,
        sends_last,
    ):
        sends.wait()


def body(queries, keys, values, out_grad, layer_input, lengths):
    anywhere = pl.BlockSpec(memory_space=pltpu.HBM)
    vmem = pltpu.VMEM
    outs = pl.pallas_call(
        kernel,
        out_shape=(
            jax.ShapeDtypeStruct((128, 2048), BF16),
            jax.ShapeDtypeStruct((128, 512), BF16),
            jax.ShapeDtypeStruct((128, 512), BF16),
            jax.ShapeDtypeStruct((16, 1024), F32),
        ),
        in_specs=[pl.BlockSpec(memory_space=pltpu.SMEM)] + [anywhere] * 5,
        out_specs=(anywhere,) * 4,
        scratch_shapes=[
            vmem((2, 128, 512), BF16),
            vmem((4, 128, 512), BF16),
            vmem((4, 128, 512), BF16),
            vmem((2048, 256), BF16),
            vmem((128, 4096), BF16),
            vmem((4, 4, 4, 64, 128), BF16),
            vmem((4, 4, 4, 64, 512), BF16),
            vmem((8, 256, 128), BF16),
            vmem((8, 256, 128), BF16),
            vmem((8, 256, 128), BF16),
            vmem((8, 256, 128), BF16),
            vmem((8, 128, 256), BF16),
            vmem((12, 4, 256, 256), F32),
            vmem((12, 4, 256, 256), F32),
            vmem((12, 256, 1024), BF16),
            vmem((12, 256, 1024), BF16),
            vmem((8, 8, 256), F32),
            vmem((8, 8, 256), F32),
            vmem((8, 8, 256), F32),
            vmem((4, 128, 256), F32),
            vmem((4, 128, 512), BF16),
            vmem((2, 4, 2, 256, 128), F32),
            vmem((2, 4, 2, 256, 128), BF16),
            vmem((2, 256, 128), BF16),
            vmem((2, 256, 128), BF16),
            vmem((2, 2, 256, 128), BF16),
            vmem((2, 2, 256, 128), BF16),
            vmem((4, 512, 256), BF16),
            vmem((4, 128, 128), BF16),
            vmem((2, 256, 128), F32),
            vmem((2, 256, 128), F32),
            vmem((2, 4, 256, 128), F32),
            vmem((2, 4, 256, 128), BF16),
            vmem((2, 3, 256, 128), BF16),
            vmem((2, 4, 4, 16, 128), BF16),
            vmem((16, 1024), F32),
            pltpu.SemaphoreType.DMA((SENDS,)),
            pltpu.SemaphoreType.DMA((ARRIVALS,)),
            pltpu.SemaphoreType.DMA((LOCALS,)),
        ],
        compiler_params=pltpu.CompilerParams(
            collective_id=0, has_side_effects=True, vmem_limit_bytes=62 * 1024 * 1024
        ),
        name="attention_backward",
    )(lengths[0], queries[0], out_grad[0], keys[0], values[0], layer_input[0])
    return (outs[0][None], outs[1][None], outs[2][None], outs[3])


def solution(mesh):
    placed = (P("dp", "blk", None),) * 5 + (P("dp", None),)
    return jax.shard_map(
        body,
        mesh=mesh,
        in_specs=placed,
        out_specs=(P("dp", "blk", None),) * 3 + (P(("dp", "blk"), None),),
        check_vma=False,
    )
```

```python
import math

import jax
import jax.numpy as jnp
from jax import lax
from jax.experimental import pallas as pl
from jax.experimental.pallas import tpu as pltpu
from jax.sharding import PartitionSpec as P

MESH = pl.DeviceIdType.MESH
F32 = jnp.float32
BF16 = jnp.bfloat16
HEAD = 128
ROPE_BASE = 500000.0
MASKED = -1e30
FAR = 1 << 20
SENDS = 11
ARRIVALS = 52
LOCALS = 17


def nn(a, b):
    return jnp.dot(a, b, preferred_element_type=F32)


def nt(a, b):
    return lax.dot_general(a, b, (((1,), (1,)), ((), ())), preferred_element_type=F32)


def kernel(
    len_ref, q_in, do_in, k_in, v_in, x_in,
    dq_out, dk_out, dv_out, w_out,
    kvin, qbuf, dobuf, kv, xv, xt, xbuf, qs, dos, qsn, dosn, kt, p_f, dp_s, p_t, ds_t, top_s, inv_s, del_s, dqacc,
    dqbuf, part_f, part_b, far_a, far_b, near_m, near_p, gbuf, dkbuf, cosb, sinb, wacc, wb1, r1,
    r2, w_stage, send, recv, loc,
):
    b = lax.axis_index("blk")
    dp = lax.axis_index("dp")
    y, w = b // 4, b % 4
    core = w % 2
    zhi, xx = dp // 4, dp % 4
    yp, y2, ym = (y + 1) % 4, (y + 2) % 4, (y + 3) % 4
    xp, xm = (xx + 1) % 4, (xx + 3) % 4
    scale = 1.0 / math.sqrt(HEAD)
    prompt_len = len_ref[0]
    reject_start = len_ref[0] + len_ref[1]

    count = [0, 0, 0]

    def covering(size):
        if size % 8192:
            return kv.at[pl.ds(0, size // 256), pl.ds(0, 128)]
        if size <= 1 << 20:
            return kv.at[pl.ds(0, size // 512)]
        return ds_t.at[pl.ds(0, size >> 19)]

    def bytes_of(ref):
        return math.prod(ref.shape) * ref.dtype.itemsize

    def wait_bytes(sem, size):
        ref = covering(size)
        pltpu.make_async_copy(ref, ref, sem).wait()

    class Sends:
        def __init__(self):
            self.at = count[2]
            self.size = 0
            count[2] += 1

        def wait(self):
            wait_bytes(send.at[self.at], self.size)

    class Arrivals:
        def __init__(self):
            self.at = count[0]
            self.size = 0
            count[0] += 1

        def wait_recv(self):
            wait_bytes(recv.at[self.at], self.size)

    def remote(src, dst, device, sends, arrivals=None):
        arrivals = arrivals or Arrivals()
        pltpu.make_async_remote_copy(
            src_ref=src, dst_ref=dst, send_sem=send.at[sends.at], recv_sem=recv.at[arrivals.at],
            device_id=device, device_id_type=MESH,
        ).start()
        sends.size += bytes_of(src)
        arrivals.size += bytes_of(src)
        return arrivals

    def local(src, dst):
        i = count[1]
        count[1] += 1
        copy = pltpu.make_async_copy(src, dst, loc.at[i])
        copy.start()
        return copy

    def at_blk(yy, ww):
        return {"blk": 4 * yy + ww}

    def at_x(to):
        return {"dp": 4 * zhi + to}

    def at_owner(zz, ww):
        return {"dp": 4 * zz + xx, "blk": 4 * y + ww}

    def tile(i, size):
        return pl.ds(pl.multiple_of(i * size, size), size)

    barrier = pltpu.get_barrier_semaphore()
    for d in range(1, 4):
        for device in (at_blk((y + d) % 4, w), {"dp": 4 * zhi + (xx + d) % 4}):
            pl.semaphore_signal(barrier, 1, device_id=device, device_id_type=MESH)
    for dz in range(4):
        for d in range(4):
            if dz or d:
                pl.semaphore_signal(
                    barrier, 1, device_id=at_owner((zhi + dz) % 4, (w + d) % 4),
                    device_id_type=MESH,
                )
    staged = [local(ref, kvin.at[part]) for part, ref in ((0, k_in), (1, v_in))]
    for ref, stage in ((q_in, p_t), (do_in, ds_t)):
        for side in range(2):
            staged.append(
                local(ref.at[:, pl.ds(1024 * side, 1024)], stage.at[0, pl.ds(128 * side, 128)])
            )
    x_local = local(x_in, xv)
    kv_slots = (tile(4 * y + w, 64), tile(4 * (7 - y) + 3 - w, 64))
    own_kv = []
    for half in range(2):
        for part, ref in ((0, k_in), (1, v_in)):
            own_kv.append(
                local(
                    ref.at[pl.ds(64 * half, 64), tile(w, 128)],
                    kv.at[kv_slots[half], pl.ds(128 * part, 128)],
                )
            )
    own_q = [
        local(q_in.at[:, tile(w, 512)], qbuf.at[w]),
        local(do_in.at[:, tile(w, 512)], dobuf.at[w]),
    ]
    pl.semaphore_wait(barrier, 21)

    def row_slots(ww):
        return tile(4 * y + ww, 64), tile(4 * (7 - y) + 3 - ww, 64)

    for copy in staged[:2]:
        copy.wait()
    kv_first = {}
    sends_kv = Sends()
    for d in (1, 3, 2):
        ww = (w + d) % 4
        kv_first[d] = Arrivals()
        for half in range(2):
            for part in range(2):
                remote(
                    kvin.at[part, pl.ds(64 * half, 64), tile(ww, 128)],
                    kv.at[kv_slots[half], pl.ds(128 * part, 128)],
                    at_blk(y, ww), sends_kv, kv_first[d],
                )
    for copy in staged[2:]:
        copy.wait()
    sends_q, sends_do, q_first = Sends(), Sends(), Arrivals()
    for d in (1, 3, 2):
        ww = (w + d) % 4
        src = p_t.at[0, tile(ww // 2, 128), tile(ww % 2, 512)]
        remote(src, qbuf.at[w], at_blk(y, ww), sends_q, q_first)
    do_first = {1: Arrivals(), 0: Arrivals()}
    for half in (1, 0):
        for d in (1, 3, 2):
            ww = (w + d) % 4
            src = ds_t.at[0, tile(2 * (ww // 2) + half, 64), tile(ww % 2, 512)]
            dst = dobuf.at[w, pl.ds(64 * half, 64)]
            remote(src, dst, at_blk(y, ww), sends_do, do_first[half])

    sends_spread, kv_rest = Sends(), Arrivals()
    kv_plus, kv_minus = [], []

    def spread(ww):
        slots = row_slots(ww)
        low, high = kv.at[slots[0]], kv.at[slots[1]]
        kv_plus.append(remote(low, low, at_blk(yp, w), sends_spread))
        kv_minus.append(remote(high, high, at_blk(ym, w), sends_spread))
        remote(high, high, at_blk(yp, w), sends_spread, kv_rest)
        remote(low, low, at_blk(ym, w), sends_spread, kv_rest)

    for copy in own_kv:
        copy.wait()
    spread(w)

    x_local.wait()

    def transpose_x(i, carry):
        to = i % 8 // 2
        xt[to, pl.ds((i % 2) * 2, 2), i // 8] = xv[:, tile(i, 128)].T.reshape(2, 64, 128)
        return carry

    lax.fori_loop(0, 32, transpose_x, 0)
    column = tile(w, 128)
    w_other = (w + 2) % 4
    core_mate = at_blk(y, w + 1 - 2 * core)
    z_mate = at_blk(y, (w + 2) % 4)
    sends_x, sends_first, x_first = Sends(), Sends(), Arrivals()
    for d in (1, 3, 2):
        to = (xx + d) % 4
        remote(xt.at[to], xbuf.at[:, 4 - d, w], at_x(to), sends_first, x_first)
    x_far = [remote(xt.at[xx], xbuf.at[:, 0, w], z_mate, sends_x)]
    x_mate = [remote(xt.at[xx], xbuf.at[:, 0, w], core_mate, sends_x)]

    for d in (1, 3, 2):
        kv_first[d].wait_recv()
        spread((w + 4 - d) % 4)
    xbuf[:, 0, w] = xt[xx]
    lane_row = lax.broadcasted_iota(jnp.int32, (1, HEAD), 1)
    frequency = jnp.exp(
        -(2.0 * (lane_row % 64).astype(F32) / HEAD) * math.log(ROPE_BASE)
    )
    for half, block in ((0, y), (1, 7 - y)):
        position = 256 * block + lax.broadcasted_iota(jnp.int32, (256, HEAD), 0)
        angles = position.astype(F32) * frequency
        cosb[half] = jnp.cos(angles)
        sinb[half] = jnp.where(lane_row < 64, jnp.sin(angles), -jnp.sin(angles))

    kv_second = Arrivals()
    for k, d in enumerate((0, 1, 3, 2)):
        ww = (w + 4 - d) % 4
        kv_plus[k].wait_recv()
        ref = kv.at[tile(4 * ym + ww, 64)]
        remote(ref, ref, at_blk(yp, w), sends_spread, kv_second)
        kv_minus[k].wait_recv()
        ref = kv.at[tile(4 * (7 - yp) + 3 - ww, 64)]
        remote(ref, ref, at_blk(ym, w), sends_spread, kv_second)
    kv_rest.wait_recv()

    own_q[0].wait()
    q_first.wait_recv()

    def stack(buf, stacked, halves):
        for half in halves:
            for h in range(4):
                for ww in range(4):
                    piece = buf[ww, pl.ds(64 * half, 64), pl.ds(128 * h, 128)]
                    stacked[4 * half + h, pl.ds(64 * ww, 64)] = piece

    stack(qbuf, qs, (0, 1))

    lane = lax.broadcasted_iota(jnp.int32, (1, 256), 1)
    lane_high = (3 - lane // 64) * 64 + lane % 64
    rows = lax.broadcasted_iota(jnp.int32, (256, 256), 0)
    zero = jnp.zeros((8, 256), F32)

    def score_block(half, j):
        diagonal = y + half * (7 - 2 * y)
        query_pos = 256 * diagonal + lane + half * (lane_high - lane)
        rejected = query_pos >= reject_start
        key_pos = 256 * j + rows
        chosen = jnp.logical_and(key_pos >= prompt_len, key_pos < reject_start)
        shown = jnp.where(rejected, jnp.where(chosen, FAR, key_pos), key_pos)
        bias = jnp.where(shown <= query_pos, 0.0, MASKED)
        key = kv[tile(j, 256), pl.ds(0, 128)]
        out = []
        for h in range(4):
            s = nt(key, qs[4 * half + h]) + bias
            p_f[4 * half + j, h] = s
            out.append(jnp.max(s.reshape(32, 8, 256), axis=0))
        return out

    last_high = (5 - y) // 4

    def scores_half(half, carry):
        def scores(t, tops):
            j = t + (t - y2 + 8) // 8
            j = j + (j - (7 - y2) + 8) // 8
            new = score_block(half, j)
            return tuple(jnp.maximum(tops[h], new[h]) for h in range(4))

        blocks = half * (7 - y - last_high) + (1 - half) * (y + last_high)
        tops = lax.fori_loop(0, blocks, scores, (jnp.full((8, 256), MASKED, F32),) * 4)
        for h in range(4):
            top_s[4 * half + h] = tops[h]
        return carry

    lax.fori_loop(0, 2, scores_half, 0)
    kv_second.wait_recv()

    def last_block(i, carry):
        half = i * last_high + (1 - i)
        j = half * i * (7 - y2) + (1 - half * i) * y2
        new = score_block(half, j)
        for h in range(4):
            top_s[4 * half + h] = jnp.maximum(top_s[4 * half + h], new[h])
        return carry

    lax.fori_loop(0, 2, last_block, 0)

    own_q[1].wait()
    sends_q.wait()
    do_first[1].wait_recv()
    stack(dobuf, dos, (1,))

    def weights_half(half, carry):
        blocks = y + half * (7 - 2 * y) + 1
        tops = [jnp.max(top_s[4 * half + h], axis=0, keepdims=True) for h in range(4)]

        def weights(j, sums):
            value = kv[tile(j, 256), pl.ds(128, 128)]
            slot = 4 * half + j
            totals, dots = [], []
            for h in range(4):
                p = jnp.exp2((p_f[slot, h] - tops[h]) * (scale * math.log2(math.e)))
                p_f[slot, h] = p
                p_t[slot, :, pl.ds(256 * h, 256)] = p.astype(BF16)
                totals.append(sums[0][h] + jnp.sum(p.reshape(32, 8, 256), axis=0))
                d = nt(value, dos[4 * half + h])
                dp_s[slot, h] = d
                dots.append(sums[1][h] + jnp.sum((p * d).reshape(32, 8, 256), axis=0))
            return tuple(totals), tuple(dots)

        totals, dots = lax.fori_loop(0, blocks, weights, ((zero,) * 4, (zero,) * 4))
        for h in range(4):
            inverse = 1.0 / jnp.sum(totals[h], axis=0, keepdims=True)
            delta = jnp.sum(dots[h], axis=0, keepdims=True) * inverse
            inv_s[4 * half + h] = jnp.broadcast_to(inverse, (8, 256))
            del_s[4 * half + h] = jnp.broadcast_to(delta, (8, 256))
        return carry

    weights_half(1, 0)
    order = (2, 1, 3, 0)
    x_first.wait_recv()
    for d in order:
        ref = xbuf.at[(y + d) % 4, pl.ds(1, 3), w]
        x_far.append(remote(ref, ref, z_mate, sends_x))
        x_mate.append(remote(ref, ref, core_mate, sends_x))
    do_first[0].wait_recv()
    stack(dobuf, dos, (0,))
    weights_half(0, 0)

    def scale_rows(c, carry):
        per_row = jnp.broadcast_to(inv_s[c, pl.ds(0, 1)], (128, 256)).T
        dosn[c] = (dos[c].astype(F32) * per_row).astype(BF16)
        qsn[c] = (qs[c].astype(F32) * (per_row * scale)).astype(BF16)
        return carry

    lax.fori_loop(0, 8, scale_rows, 0, unroll=True)
    def sums_for(yy, left, right):
        g = (yy - y + 4) // 5
        low = nn(left[4 + yy], right[pl.ds(4, 4)].reshape(1024, 128))
        more = nn(
            left[g * (11 - yy) + (1 - g) * yy], right[pl.ds(4 * g, 4)].reshape(1024, 128)
        )
        keep = g.astype(F32)
        return low + more * (1.0 - keep), more * keep

    def own_sums(left, right):
        low = nn(left[4 + y], right[pl.ds(4, 4)].reshape(1024, 128))
        low = low + nn(left[y], right[pl.ds(0, 4)].reshape(1024, 128))
        return low, nn(left[11 - y], right[pl.ds(4, 4)].reshape(1024, 128))

    def reduce_first(part, left, right):
        low, high = sums_for(y2, left, right)
        part_b[part, y2, 0] = low.astype(BF16)
        part_b[part, y2, 1] = high.astype(BF16)
        return (
            remote(part_b.at[part, y2, 0], far_a.at[part], at_blk(yp, w), sends_sum),
            remote(part_b.at[part, y2, 1], far_b.at[part], at_blk(ym, w), sends_sum),
        )

    def reduce_middle(part, left, right):
        for yy in (yp, ym):
            low, high = sums_for(yy, left, right)
            part_f[part, yy, 0] = low
            part_f[part, yy, 1] = high

    def reduce_second(part, far):
        out = []
        far[0].wait_recv()
        part_b[part, yp, 0] = (part_f[part, yp, 0] + far_a[part].astype(F32)).astype(BF16)
        part_b[part, yp, 1] = part_f[part, yp, 1].astype(BF16)
        out.append(remote(part_b.at[part, yp], near_m.at[part], at_blk(yp, w), sends_sum))
        far[1].wait_recv()
        part_b[part, ym, 0] = part_f[part, ym, 0].astype(BF16)
        part_b[part, ym, 1] = (part_f[part, ym, 1] + far_b[part].astype(F32)).astype(BF16)
        out.append(remote(part_b.at[part, ym], near_p.at[part], at_blk(ym, w), sends_sum))
        return out

    def reduce_own(part, left, right):
        low, high = own_sums(left, right)
        part_f[part, y, 0] = low
        part_f[part, y, 1] = high

    sends_sum = Sends()
    far_v = reduce_first(1, p_t, dosn)
    reduce_middle(1, p_t, dosn)

    sends_do.wait()
    def grads_half(half, carry):
        blocks = y + half * (7 - 2 * y) + 1
        deltas = [del_s[4 * half + h, pl.ds(0, 1)] for h in range(4)]

        def grads(j, carry):
            slot = 4 * half + j
            for h in range(4):
                ds = p_f[slot, h] * (dp_s[slot, h] - deltas[h])
                ds_t[slot, :, pl.ds(256 * h, 256)] = ds.astype(BF16)
            return carry

        return lax.fori_loop(0, blocks, grads, carry)

    lax.fori_loop(0, 2, grads_half, 0)

    far_k = reduce_first(0, ds_t, qsn)
    reduce_middle(0, ds_t, qsn)
    near_v = reduce_second(1, far_v)
    reduce_own(1, p_t, dosn)
    reduce_own(0, ds_t, qsn)
    near_k = reduce_second(0, far_k)
    def transpose_k(j, carry):
        kt[j] = kv[tile(j, 256), pl.ds(0, 128)].T
        return carry

    lax.fori_loop(0, 8, transpose_k, 0, unroll=2)

    def query_half(half, carry):
        blocks = y + half * (7 - 2 * y) + 1
        dqacc[...] = jnp.zeros_like(dqacc)

        def one(j, carry):
            for h in range(4):
                dqacc[h] += nn(kt[j], ds_t[4 * half + j, :, pl.ds(256 * h, 256)])
            return carry

        lax.fori_loop(0, blocks, one, 0)
        for h in range(4):
            dq = dqacc[h] * (inv_s[4 * half + h, pl.ds(0, 1)] * scale)
            dq = dq.T.astype(BF16)
            for ww in range(4):
                dqbuf[ww, tile(half, 64), pl.ds(128 * h, 128)] = dq[64 * ww : 64 * ww + 64]
        return carry

    lax.fori_loop(0, 2, query_half, 0)
    for copy in near_v:
        copy.wait_recv()

    def gathered(part, half):
        own = part_f[part, y, half]
        return own + near_m[part, half].astype(F32) + near_p[part, half].astype(F32)

    for half in range(2):
        value_grad = gathered(1, half).astype(BF16)
        for ww in range(4):
            at = 64 * ww if half == 0 else 64 * (3 - ww)
            rows_at = pl.ds(128 * ww + 64 * half, 64)
            gbuf[0, rows_at, pl.ds(128, 128)] = value_grad[at : at + 64]

    def gather_near(part):
        lanes = pl.ds(128 * part, 128)
        return [
            remote(gbuf.at[0, :, lanes], gbuf.at[3, :, lanes], at_x(xp), sends_g),
            remote(gbuf.at[0, :, lanes], gbuf.at[1, :, lanes], at_x(xm), sends_g),
        ]

    def gather_far(part, near):
        lanes = pl.ds(128 * part, 128)
        low, high = pl.ds(0, 256), pl.ds(256, 256)
        near[0].wait_recv()
        src, dst = gbuf.at[3, low, lanes], gbuf.at[2, low, lanes]
        first = remote(src, dst, at_x(xp), sends_g)
        near[1].wait_recv()
        src, dst = gbuf.at[1, high, lanes], gbuf.at[2, high, lanes]
        return [first, remote(src, dst, at_x(xm), sends_g)]

    sends_g = Sends()
    g_v = gather_near(1)
    x_third = []

    def third_x(k):
        x_far[k].wait_recv()
        if k == 0:
            ref = xbuf.at[:, 0, w_other]
        else:
            ref = xbuf.at[(y + order[k - 1]) % 4, pl.ds(1, 3), w_other]
        x_third.append(remote(ref, ref, core_mate, sends_x))

    third_x(0)
    for copy in near_k:
        copy.wait_recv()
    for half in range(2):
        key_sum = gathered(0, half)
        key_grad = key_sum.astype(BF16)
        key_pre = (
            key_sum * cosb[half] + pltpu.roll(key_sum, 64, 1) * sinb[half]
        ).astype(BF16)
        for ww in range(4):
            at = 64 * ww if half == 0 else 64 * (3 - ww)
            gbuf[0, pl.ds(128 * ww + 64 * half, 64), pl.ds(0, 128)] = key_pre[at : at + 64]
            dkbuf[ww, pl.ds(64 * half, 64)] = key_grad[at : at + 64]
    g_k = gather_near(0)
    third_x(1)
    far_g_v = gather_far(1, g_v)
    third_x(2)

    def weights_of(part, to, rels):
        lanes = pl.ds(128 * part, 128)
        total = None
        for rel in rels:
            left = [xbuf[to, rel, ww].reshape(256, 128) for ww in range(4)]
            term = nn(jnp.concatenate(left, axis=1), gbuf[rel, :, lanes])
            total = term if total is None else total + term
        return total

    def near_tile(part, d):
        to = (y + d) % 4
        wacc[part, to] = weights_of(part, to, (0, 1, 3))

    def far_tiles(part):
        out = Arrivals()
        for d in order[:3]:
            to = (y + d) % 4
            wb1[part, to] = (wacc[part, to] + weights_of(part, to, (2,))).astype(BF16)
            remote(wb1.at[part, to], r1.at[part, d - 1], at_blk(to, w), sends_w, out)
        return out

    def owner_sums(part, own, y_sums):
        total = own
        y_sums.wait_recv()
        for d in range(3):
            total = total + r1[part, d].astype(F32)
        wb1[part, y] = total.astype(BF16)
        for dz in (2, 1, 3, 0):
            zz = (zhi + dz) % 4
            for d in (2, 1, 3, 0):
                ww = (w + d) % 4
                piece = pl.ds(pl.multiple_of(64 * zz + 16 * ww, 16), 16)
                if dz or d:
                    remote(
                        wb1.at[part, y, piece], r2.at[part, zhi, w], at_owner(zz, ww),
                        sends_last, finals,
                    )
                else:
                    r2[part, zhi, w] = wb1[part, y, piece]

    sends_w, sends_last, finals = Sends(), Sends(), Arrivals()
    for k in range(3):
        x_mate[k].wait_recv()
        x_third[k].wait_recv()
    near_tile(1, 2)
    near_tile(1, 1)
    third_x(3)
    sends_out, far_out = Sends(), Arrivals()
    values_out = pl.ds(128, 128)
    own_out = [
        local(dqbuf.at[w], dq_out.at[:, tile(w, 512)]),
        local(dkbuf.at[w], dk_out.at[:, column]),
        local(gbuf.at[0, tile(w, 128), values_out], dv_out.at[:, column]),
    ]
    for d in (2, 1, 3):
        ww = (w + d) % 4
        values = gbuf.at[0, tile(ww, 128), values_out]
        remote(dqbuf.at[ww], dq_out.at[:, tile(w, 512)], at_blk(y, ww), sends_out, far_out)
        remote(dkbuf.at[ww], dk_out.at[:, column], at_blk(y, ww), sends_out, far_out)
        remote(values, dv_out.at[:, column], at_blk(y, ww), sends_out, far_out)
    far_g_k = gather_far(0, g_k)
    near_tile(0, 2)
    near_tile(0, 1)
    x_mate[3].wait_recv()
    x_third[3].wait_recv()
    near_tile(1, 3)
    for copy in far_g_v:
        copy.wait_recv()
    y_sums_v = far_tiles(1)
    near_tile(0, 3)
    third_x(4)
    for copy in far_g_k:
        copy.wait_recv()
    y_sums_k = far_tiles(0)
    x_mate[4].wait_recv()
    x_third[4].wait_recv()
    own_v = weights_of(1, y, (0, 1, 2, 3))
    wacc[0, y] = weights_of(0, y, (0, 1, 2, 3))
    owner_sums(1, own_v, y_sums_v)
    owner_sums(0, wacc[0, y], y_sums_k)
    finals.wait_recv()
    for part in range(2):
        for ww in range(4):
            total = r2[part, 0, ww].astype(F32)
            for zz in range(1, 4):
                total = total + r2[part, zz, ww].astype(F32)
            w_stage[:, pl.ds(512 * part + 128 * ww, 128)] = total
    own_out.append(local(w_stage, w_out))
    for copy in own_out:
        copy.wait()
    far_out.wait_recv()
    assert count == [ARRIVALS, LOCALS, SENDS], count
    for sends in (
        sends_kv, sends_spread, sends_first, sends_x, sends_sum, sends_g, sends_out, sends_w,
        sends_last,
    ):
        sends.wait()


def place(*refs):
    sources, targets, stages, sem_in, sem_out = refs[:4], refs[4:8], refs[8:12], *refs[12:]
    parts = []
    for source, target, stage in zip(sources, targets, stages, strict=True):
        for side in range(4 if source.shape[1] == 2048 else 1):
            at = pl.ds(side * 32, 32) if source.shape[1] == 2048 else slice(None)
            i = len(parts)
            arrive = pltpu.make_async_copy(source.at[at], stage.at[at], sem_in.at[i])
            arrive.start()
            leave = pltpu.make_async_copy(stage.at[at], target.at[at], sem_out.at[i])
            parts.append((arrive, leave))
    for arrive, leave in parts:
        arrive.wait()
        leave.start()
    for _, leave in parts:
        leave.wait()


def body(queries, keys, values, out_grad, layer_input, lengths):
    anywhere = pl.BlockSpec(memory_space=pltpu.HBM)
    vmem = pltpu.VMEM
    shapes = (
        jax.ShapeDtypeStruct((128, 2048), BF16),
        jax.ShapeDtypeStruct((128, 512), BF16),
        jax.ShapeDtypeStruct((128, 512), BF16),
        jax.ShapeDtypeStruct((16, 1024), F32),
    )
    outs = pl.pallas_call(
        kernel,
        out_shape=shapes,
        in_specs=[pl.BlockSpec(memory_space=pltpu.SMEM)] + [anywhere] * 5,
        out_specs=(anywhere,) * 4,
        scratch_shapes=[
            vmem((2, 128, 512), BF16),
            vmem((4, 128, 512), BF16),
            vmem((4, 128, 512), BF16),
            vmem((2048, 256), BF16),
            vmem((128, 4096), BF16),
            vmem((4, 4, 4, 64, 128), BF16),
            vmem((4, 4, 4, 4, 64, 128), BF16),
            vmem((8, 256, 128), BF16),
            vmem((8, 256, 128), BF16),
            vmem((8, 256, 128), BF16),
            vmem((8, 256, 128), BF16),
            vmem((8, 128, 256), BF16),
            vmem((12, 4, 256, 256), F32),
            vmem((12, 4, 256, 256), F32),
            vmem((12, 256, 1024), BF16),
            vmem((12, 256, 1024), BF16),
            vmem((8, 8, 256), F32),
            vmem((8, 8, 256), F32),
            vmem((8, 8, 256), F32),
            vmem((4, 128, 256), F32),
            vmem((4, 128, 512), BF16),
            vmem((2, 4, 2, 256, 128), F32),
            vmem((2, 4, 2, 256, 128), BF16),
            vmem((2, 256, 128), BF16),
            vmem((2, 256, 128), BF16),
            vmem((2, 2, 256, 128), BF16),
            vmem((2, 2, 256, 128), BF16),
            vmem((4, 512, 256), BF16),
            vmem((4, 128, 128), BF16),
            vmem((2, 256, 128), F32),
            vmem((2, 256, 128), F32),
            vmem((2, 4, 256, 128), F32),
            vmem((2, 4, 256, 128), BF16),
            vmem((2, 3, 256, 128), BF16),
            vmem((2, 4, 4, 16, 128), BF16),
            vmem((16, 1024), F32),
            pltpu.SemaphoreType.DMA((SENDS,)),
            pltpu.SemaphoreType.DMA((ARRIVALS,)),
            pltpu.SemaphoreType.DMA((LOCALS,)),
        ],
        compiler_params=pltpu.CompilerParams(
            collective_id=0, has_side_effects=True, vmem_limit_bytes=62 * 1024 * 1024
        ),
        name="attention_backward",
    )(lengths[0], queries[0], out_grad[0], keys[0], values[0], layer_input[0])
    outs = pl.pallas_call(
        place,
        out_shape=shapes,
        in_specs=[anywhere] * 4,
        out_specs=(anywhere,) * 4,
        scratch_shapes=[vmem(shape.shape, shape.dtype) for shape in shapes]
        + [pltpu.SemaphoreType.DMA((7,)), pltpu.SemaphoreType.DMA((7,))],
        name="place_outputs",
    )(*outs)
    return (outs[0][None], outs[1][None], outs[2][None], outs[3])


def solution(mesh):
    placed = (P("dp", "blk", None),) * 5 + (P("dp", None),)
    return jax.shard_map(
        body,
        mesh=mesh,
        in_specs=placed,
        out_specs=(P("dp", "blk", None),) * 3 + (P(("dp", "blk"), None),),
        check_vma=False,
    )
```

```python
import math

import jax
import jax.numpy as jnp
from jax import lax
from jax.experimental import pallas as pl
from jax.experimental.pallas import tpu as pltpu
from jax.sharding import PartitionSpec as P

MESH = pl.DeviceIdType.MESH
F32 = jnp.float32
BF16 = jnp.bfloat16
HEAD = 128
ROPE_BASE = 500000.0
MASKED = -1e30
FAR = 1 << 20
SENDS = 11
ARRIVALS = 52
LOCALS = 17


def nn(a, b):
    return jnp.dot(a, b, preferred_element_type=F32)


def nt(a, b):
    return lax.dot_general(a, b, (((1,), (1,)), ((), ())), preferred_element_type=F32)


def kernel(
    len_ref, q_in, do_in, k_in, v_in, x_in,
    dq_out, dk_out, dv_out, w_out,
    kvin, qbuf, dobuf, kv, xv, xt, xbuf, qs, dos, qsn, dosn, kt, p_f, dp_s, p_t, ds_t, top_s, inv_s, del_s, dqacc,
    dqbuf, part_f, part_b, far_a, far_b, near_m, near_p, gbuf, dkbuf, cosb, sinb, wacc, wb1, r1,
    r2, w_stage, send, recv, loc,
):
    b = lax.axis_index("blk")
    dp = lax.axis_index("dp")
    y, w = b // 4, b % 4
    core = w % 2
    zhi, xx = dp // 4, dp % 4
    yp, y2, ym = (y + 1) % 4, (y + 2) % 4, (y + 3) % 4
    xp, xm = (xx + 1) % 4, (xx + 3) % 4
    scale = 1.0 / math.sqrt(HEAD)
    prompt_len = len_ref[0]
    reject_start = len_ref[0] + len_ref[1]

    count = [0, 0, 0]

    def covering(size):
        if size % 8192:
            return kv.at[pl.ds(0, size // 256), pl.ds(0, 128)]
        if size <= 1 << 20:
            return kv.at[pl.ds(0, size // 512)]
        return ds_t.at[pl.ds(0, size >> 19)]

    def bytes_of(ref):
        return math.prod(ref.shape) * ref.dtype.itemsize

    def wait_bytes(sem, size):
        ref = covering(size)
        pltpu.make_async_copy(ref, ref, sem).wait()

    class Sends:
        def __init__(self):
            self.at = count[2]
            self.size = 0
            count[2] += 1

        def wait(self):
            wait_bytes(send.at[self.at], self.size)

    class Arrivals:
        def __init__(self):
            self.at = count[0]
            self.size = 0
            count[0] += 1

        def wait_recv(self):
            wait_bytes(recv.at[self.at], self.size)

    def remote(src, dst, device, sends, arrivals=None):
        arrivals = arrivals or Arrivals()
        pltpu.make_async_remote_copy(
            src_ref=src, dst_ref=dst, send_sem=send.at[sends.at], recv_sem=recv.at[arrivals.at],
            device_id=device, device_id_type=MESH,
        ).start()
        sends.size += bytes_of(src)
        arrivals.size += bytes_of(src)
        return arrivals

    def local(src, dst):
        i = count[1]
        count[1] += 1
        copy = pltpu.make_async_copy(src, dst, loc.at[i])
        copy.start()
        return copy

    def at_blk(yy, ww):
        return {"blk": 4 * yy + ww}

    def at_x(to):
        return {"dp": 4 * zhi + to}

    def at_owner(zz, ww):
        return {"dp": 4 * zz + xx, "blk": 4 * y + ww}

    def tile(i, size):
        return pl.ds(pl.multiple_of(i * size, size), size)

    barrier = pltpu.get_barrier_semaphore()
    for d in range(1, 4):
        for device in (at_blk((y + d) % 4, w), {"dp": 4 * zhi + (xx + d) % 4}):
            pl.semaphore_signal(barrier, 1, device_id=device, device_id_type=MESH)
    for dz in range(4):
        for d in range(4):
            if dz or d:
                pl.semaphore_signal(
                    barrier, 1, device_id=at_owner((zhi + dz) % 4, (w + d) % 4),
                    device_id_type=MESH,
                )
    staged = [local(ref, kvin.at[part]) for part, ref in ((0, k_in), (1, v_in))]
    for ref, stage in ((q_in, p_t), (do_in, ds_t)):
        for side in range(2):
            staged.append(
                local(ref.at[:, pl.ds(1024 * side, 1024)], stage.at[0, pl.ds(128 * side, 128)])
            )
    x_local = local(x_in, xv)
    kv_slots = (tile(4 * y + w, 64), tile(4 * (7 - y) + 3 - w, 64))
    own_kv = []
    for half in range(2):
        for part, ref in ((0, k_in), (1, v_in)):
            own_kv.append(
                local(
                    ref.at[pl.ds(64 * half, 64), tile(w, 128)],
                    kv.at[kv_slots[half], pl.ds(128 * part, 128)],
                )
            )
    own_q = [
        local(q_in.at[:, tile(w, 512)], qbuf.at[w]),
        local(do_in.at[:, tile(w, 512)], dobuf.at[w]),
    ]
    pl.semaphore_wait(barrier, 21)

    def row_slots(ww):
        return tile(4 * y + ww, 64), tile(4 * (7 - y) + 3 - ww, 64)

    for copy in staged[:2]:
        copy.wait()
    kv_first = {}
    sends_kv = Sends()
    for d in (1, 3, 2):
        ww = (w + d) % 4
        kv_first[d] = Arrivals()
        for half in range(2):
            for part in range(2):
                remote(
                    kvin.at[part, pl.ds(64 * half, 64), tile(ww, 128)],
                    kv.at[kv_slots[half], pl.ds(128 * part, 128)],
                    at_blk(y, ww), sends_kv, kv_first[d],
                )
    for copy in staged[2:]:
        copy.wait()
    sends_q, sends_do, q_first = Sends(), Sends(), Arrivals()
    for d in (1, 3, 2):
        ww = (w + d) % 4
        src = p_t.at[0, tile(ww // 2, 128), tile(ww % 2, 512)]
        remote(src, qbuf.at[w], at_blk(y, ww), sends_q, q_first)
    do_first = {1: Arrivals(), 0: Arrivals()}
    for half in (1, 0):
        for d in (1, 3, 2):
            ww = (w + d) % 4
            src = ds_t.at[0, tile(2 * (ww // 2) + half, 64), tile(ww % 2, 512)]
            dst = dobuf.at[w, pl.ds(64 * half, 64)]
            remote(src, dst, at_blk(y, ww), sends_do, do_first[half])

    sends_spread, kv_rest = Sends(), Arrivals()
    kv_plus, kv_minus = [], []

    def spread(ww):
        slots = row_slots(ww)
        low, high = kv.at[slots[0]], kv.at[slots[1]]
        kv_plus.append(remote(low, low, at_blk(yp, w), sends_spread))
        kv_minus.append(remote(high, high, at_blk(ym, w), sends_spread))
        remote(high, high, at_blk(yp, w), sends_spread, kv_rest)
        remote(low, low, at_blk(ym, w), sends_spread, kv_rest)

    for copy in own_kv:
        copy.wait()
    spread(w)

    x_local.wait()

    def transpose_x(i, carry):
        to = i % 8 // 2
        xt[to, pl.ds((i % 2) * 2, 2), i // 8] = xv[:, tile(i, 128)].T.reshape(2, 64, 128)
        return carry

    lax.fori_loop(0, 32, transpose_x, 0)
    column = tile(w, 128)
    w_other = (w + 2) % 4
    core_mate = at_blk(y, w + 1 - 2 * core)
    z_mate = at_blk(y, (w + 2) % 4)
    sends_x, sends_first, x_first = Sends(), Sends(), Arrivals()
    for d in (1, 3, 2):
        to = (xx + d) % 4
        remote(xt.at[to], xbuf.at[:, 4 - d, w], at_x(to), sends_first, x_first)
    x_far = [remote(xt.at[xx], xbuf.at[:, 0, w], z_mate, sends_x)]
    x_mate = [remote(xt.at[xx], xbuf.at[:, 0, w], core_mate, sends_x)]

    for d in (1, 3, 2):
        kv_first[d].wait_recv()
        spread((w + 4 - d) % 4)
    xbuf[:, 0, w] = xt[xx]
    lane_row = lax.broadcasted_iota(jnp.int32, (1, HEAD), 1)
    frequency = jnp.exp(
        -(2.0 * (lane_row % 64).astype(F32) / HEAD) * math.log(ROPE_BASE)
    )
    for half, block in ((0, y), (1, 7 - y)):
        position = 256 * block + lax.broadcasted_iota(jnp.int32, (256, HEAD), 0)
        angles = position.astype(F32) * frequency
        cosb[half] = jnp.cos(angles)
        sinb[half] = jnp.where(lane_row < 64, jnp.sin(angles), -jnp.sin(angles))

    kv_second = Arrivals()
    for k, d in enumerate((0, 1, 3, 2)):
        ww = (w + 4 - d) % 4
        kv_plus[k].wait_recv()
        ref = kv.at[tile(4 * ym + ww, 64)]
        remote(ref, ref, at_blk(yp, w), sends_spread, kv_second)
        kv_minus[k].wait_recv()
        ref = kv.at[tile(4 * (7 - yp) + 3 - ww, 64)]
        remote(ref, ref, at_blk(ym, w), sends_spread, kv_second)
    kv_rest.wait_recv()

    own_q[0].wait()
    q_first.wait_recv()

    def stack(buf, stacked, halves):
        for half in halves:
            for h in range(4):
                for ww in range(4):
                    piece = buf[ww, pl.ds(64 * half, 64), pl.ds(128 * h, 128)]
                    stacked[4 * half + h, pl.ds(64 * ww, 64)] = piece

    stack(qbuf, qs, (0, 1))

    lane = lax.broadcasted_iota(jnp.int32, (1, 256), 1)
    lane_high = (3 - lane // 64) * 64 + lane % 64
    rows = lax.broadcasted_iota(jnp.int32, (256, 256), 0)
    zero = jnp.zeros((8, 256), F32)

    def score_block(half, j):
        diagonal = y + half * (7 - 2 * y)
        query_pos = 256 * diagonal + lane + half * (lane_high - lane)
        rejected = query_pos >= reject_start
        key_pos = 256 * j + rows
        chosen = jnp.logical_and(key_pos >= prompt_len, key_pos < reject_start)
        shown = jnp.where(rejected, jnp.where(chosen, FAR, key_pos), key_pos)
        bias = jnp.where(shown <= query_pos, 0.0, MASKED)
        key = kv[tile(j, 256), pl.ds(0, 128)]
        out = []
        for h in range(4):
            s = nt(key, qs[4 * half + h]) + bias
            p_f[4 * half + j, h] = s
            out.append(jnp.max(s.reshape(32, 8, 256), axis=0))
        return out

    last_high = (5 - y) // 4

    def scores_half(half, carry):
        def scores(t, tops):
            j = t + (t - y2 + 8) // 8
            j = j + (j - (7 - y2) + 8) // 8
            new = score_block(half, j)
            return tuple(jnp.maximum(tops[h], new[h]) for h in range(4))

        blocks = half * (7 - y - last_high) + (1 - half) * (y + last_high)
        tops = lax.fori_loop(0, blocks, scores, (jnp.full((8, 256), MASKED, F32),) * 4)
        for h in range(4):
            top_s[4 * half + h] = tops[h]
        return carry

    lax.fori_loop(0, 2, scores_half, 0)
    kv_second.wait_recv()

    def last_block(i, carry):
        half = i * last_high + (1 - i)
        j = half * i * (7 - y2) + (1 - half * i) * y2
        new = score_block(half, j)
        for h in range(4):
            top_s[4 * half + h] = jnp.maximum(top_s[4 * half + h], new[h])
        return carry

    lax.fori_loop(0, 2, last_block, 0)

    own_q[1].wait()
    sends_q.wait()
    do_first[1].wait_recv()
    stack(dobuf, dos, (1,))

    def weights_half(half, carry):
        blocks = y + half * (7 - 2 * y) + 1
        tops = [jnp.max(top_s[4 * half + h], axis=0, keepdims=True) for h in range(4)]

        def weights(j, sums):
            value = kv[tile(j, 256), pl.ds(128, 128)]
            slot = 4 * half + j
            totals, dots = [], []
            for h in range(4):
                p = jnp.exp2((p_f[slot, h] - tops[h]) * (scale * math.log2(math.e)))
                p_f[slot, h] = p
                p_t[slot, :, pl.ds(256 * h, 256)] = p.astype(BF16)
                totals.append(sums[0][h] + jnp.sum(p.reshape(32, 8, 256), axis=0))
                d = nt(value, dos[4 * half + h])
                dp_s[slot, h] = d
                dots.append(sums[1][h] + jnp.sum((p * d).reshape(32, 8, 256), axis=0))
            return tuple(totals), tuple(dots)

        totals, dots = lax.fori_loop(0, blocks, weights, ((zero,) * 4, (zero,) * 4))
        for h in range(4):
            inverse = 1.0 / jnp.sum(totals[h], axis=0, keepdims=True)
            delta = jnp.sum(dots[h], axis=0, keepdims=True) * inverse
            inv_s[4 * half + h] = jnp.broadcast_to(inverse, (8, 256))
            del_s[4 * half + h] = jnp.broadcast_to(delta, (8, 256))
        return carry

    weights_half(1, 0)
    order = (2, 1, 3, 0)
    x_first.wait_recv()
    for d in order:
        ref = xbuf.at[(y + d) % 4, pl.ds(1, 3), w]
        x_far.append(remote(ref, ref, z_mate, sends_x))
        x_mate.append(remote(ref, ref, core_mate, sends_x))
    do_first[0].wait_recv()
    stack(dobuf, dos, (0,))
    weights_half(0, 0)

    def scale_rows(c, carry):
        per_row = jnp.broadcast_to(inv_s[c, pl.ds(0, 1)], (128, 256)).T
        dosn[c] = (dos[c].astype(F32) * per_row).astype(BF16)
        qsn[c] = (qs[c].astype(F32) * (per_row * scale)).astype(BF16)
        return carry

    lax.fori_loop(0, 8, scale_rows, 0, unroll=True)
    def sums_for(yy, left, right):
        g = (yy - y + 4) // 5
        low = nn(left[4 + yy], right[pl.ds(4, 4)].reshape(1024, 128))
        more = nn(
            left[g * (11 - yy) + (1 - g) * yy], right[pl.ds(4 * g, 4)].reshape(1024, 128)
        )
        keep = g.astype(F32)
        return low + more * (1.0 - keep), more * keep

    def own_sums(left, right):
        low = nn(left[4 + y], right[pl.ds(4, 4)].reshape(1024, 128))
        low = low + nn(left[y], right[pl.ds(0, 4)].reshape(1024, 128))
        return low, nn(left[11 - y], right[pl.ds(4, 4)].reshape(1024, 128))

    def reduce_first(part, left, right):
        low, high = sums_for(y2, left, right)
        part_b[part, y2, 0] = low.astype(BF16)
        part_b[part, y2, 1] = high.astype(BF16)
        return (
            remote(part_b.at[part, y2, 0], far_a.at[part], at_blk(yp, w), sends_sum),
            remote(part_b.at[part, y2, 1], far_b.at[part], at_blk(ym, w), sends_sum),
        )

    def reduce_middle(part, left, right):
        for yy in (yp, ym):
            low, high = sums_for(yy, left, right)
            part_f[part, yy, 0] = low
            part_f[part, yy, 1] = high

    def reduce_second(part, far):
        out = []
        far[0].wait_recv()
        part_b[part, yp, 0] = (part_f[part, yp, 0] + far_a[part].astype(F32)).astype(BF16)
        part_b[part, yp, 1] = part_f[part, yp, 1].astype(BF16)
        out.append(remote(part_b.at[part, yp], near_m.at[part], at_blk(yp, w), sends_sum))
        far[1].wait_recv()
        part_b[part, ym, 0] = part_f[part, ym, 0].astype(BF16)
        part_b[part, ym, 1] = (part_f[part, ym, 1] + far_b[part].astype(F32)).astype(BF16)
        out.append(remote(part_b.at[part, ym], near_p.at[part], at_blk(ym, w), sends_sum))
        return out

    def reduce_own(part, left, right):
        low, high = own_sums(left, right)
        part_f[part, y, 0] = low
        part_f[part, y, 1] = high

    sends_sum = Sends()
    far_v = reduce_first(1, p_t, dosn)
    reduce_middle(1, p_t, dosn)

    sends_do.wait()
    def grads_half(half, carry):
        blocks = y + half * (7 - 2 * y) + 1
        deltas = [del_s[4 * half + h, pl.ds(0, 1)] for h in range(4)]

        def grads(j, carry):
            slot = 4 * half + j
            for h in range(4):
                ds = p_f[slot, h] * (dp_s[slot, h] - deltas[h])
                ds_t[slot, :, pl.ds(256 * h, 256)] = ds.astype(BF16)
            return carry

        return lax.fori_loop(0, blocks, grads, carry)

    lax.fori_loop(0, 2, grads_half, 0)

    far_k = reduce_first(0, ds_t, qsn)
    reduce_middle(0, ds_t, qsn)
    near_v = reduce_second(1, far_v)
    reduce_own(1, p_t, dosn)
    reduce_own(0, ds_t, qsn)
    near_k = reduce_second(0, far_k)
    def transpose_k(j, carry):
        kt[j] = kv[tile(j, 256), pl.ds(0, 128)].T
        return carry

    lax.fori_loop(0, 8, transpose_k, 0, unroll=2)

    def query_half(half, carry):
        blocks = y + half * (7 - 2 * y) + 1
        dqacc[...] = jnp.zeros_like(dqacc)

        def one(j, carry):
            for h in range(4):
                dqacc[h] += nn(kt[j], ds_t[4 * half + j, :, pl.ds(256 * h, 256)])
            return carry

        lax.fori_loop(0, blocks, one, 0)
        for h in range(4):
            dq = dqacc[h] * (inv_s[4 * half + h, pl.ds(0, 1)] * scale)
            dq = dq.T.astype(BF16)
            for ww in range(4):
                dqbuf[ww, tile(half, 64), pl.ds(128 * h, 128)] = dq[64 * ww : 64 * ww + 64]
        return carry

    lax.fori_loop(0, 2, query_half, 0)
    sends_out, far_out = Sends(), Arrivals()
    own_out = [local(dqbuf.at[w], dq_out.at[:, tile(w, 512)])]
    for d in (2, 1, 3):
        ww = (w + d) % 4
        dst = dq_out.at[:, tile(w, 512)]
        remote(dqbuf.at[ww], dst, at_blk(y, ww), sends_out, far_out)
    for copy in near_v:
        copy.wait_recv()

    def gathered(part, half):
        own = part_f[part, y, half]
        return own + near_m[part, half].astype(F32) + near_p[part, half].astype(F32)

    for half in range(2):
        value_grad = gathered(1, half).astype(BF16)
        for ww in range(4):
            at = 64 * ww if half == 0 else 64 * (3 - ww)
            rows_at = pl.ds(128 * ww + 64 * half, 64)
            gbuf[0, rows_at, pl.ds(128, 128)] = value_grad[at : at + 64]

    low_rows, high_rows = pl.ds(0, 256), pl.ds(256, 256)

    def gather_near(part):
        lanes = pl.ds(128 * part, 128)
        low, high = gbuf.at[0, low_rows, lanes], gbuf.at[0, high_rows, lanes]
        plus = remote(low, gbuf.at[3, low_rows, lanes], at_x(xp), sends_g)
        minus = remote(high, gbuf.at[1, high_rows, lanes], at_x(xm), sends_g)
        rest = remote(high, gbuf.at[3, high_rows, lanes], at_x(xp), sends_g)
        remote(low, gbuf.at[1, low_rows, lanes], at_x(xm), sends_g, rest)
        return plus, minus, rest

    def gather_far(part, near):
        lanes = pl.ds(128 * part, 128)
        near[0].wait_recv()
        src, dst = gbuf.at[3, low_rows, lanes], gbuf.at[2, low_rows, lanes]
        far = remote(src, dst, at_x(xp), sends_g)
        near[1].wait_recv()
        src, dst = gbuf.at[1, high_rows, lanes], gbuf.at[2, high_rows, lanes]
        return remote(src, dst, at_x(xm), sends_g, far)

    sends_g = Sends()
    g_v = gather_near(1)
    x_third = []

    def third_x(k):
        x_far[k].wait_recv()
        if k == 0:
            ref = xbuf.at[:, 0, w_other]
        else:
            ref = xbuf.at[(y + order[k - 1]) % 4, pl.ds(1, 3), w_other]
        x_third.append(remote(ref, ref, core_mate, sends_x))

    third_x(0)
    third_x(1)
    for copy in near_k:
        copy.wait_recv()
    for half in range(2):
        key_sum = gathered(0, half)
        key_grad = key_sum.astype(BF16)
        key_pre = (
            key_sum * cosb[half] + pltpu.roll(key_sum, 64, 1) * sinb[half]
        ).astype(BF16)
        for ww in range(4):
            at = 64 * ww if half == 0 else 64 * (3 - ww)
            gbuf[0, pl.ds(128 * ww + 64 * half, 64), pl.ds(0, 128)] = key_pre[at : at + 64]
            dkbuf[ww, pl.ds(64 * half, 64)] = key_grad[at : at + 64]
    g_k = gather_near(0)
    values_out = pl.ds(128, 128)
    own_out.append(local(dkbuf.at[w], dk_out.at[:, column]))
    own_out.append(local(gbuf.at[0, tile(w, 128), values_out], dv_out.at[:, column]))
    for d in (2, 1, 3):
        ww = (w + d) % 4
        values = gbuf.at[0, tile(ww, 128), values_out]
        remote(dkbuf.at[ww], dk_out.at[:, column], at_blk(y, ww), sends_out, far_out)
        remote(values, dv_out.at[:, column], at_blk(y, ww), sends_out, far_out)
    far_g_v = gather_far(1, g_v)
    third_x(2)

    def weights_of(part, to, rels):
        lanes = pl.ds(128 * part, 128)
        total = None
        for rel in rels:
            left = [xbuf[to, rel, ww].reshape(256, 128) for ww in range(4)]
            term = nn(jnp.concatenate(left, axis=1), gbuf[rel, :, lanes])
            total = term if total is None else total + term
        return total

    def near_tile(part, d):
        to = (y + d) % 4
        wacc[part, to] = weights_of(part, to, (0, 1, 3))

    def far_tile(part, d, arrivals=None):
        to = (y + d) % 4
        wb1[part, to] = (wacc[part, to] + weights_of(part, to, (2,))).astype(BF16)
        dst = r1.at[part, d - 1]
        return remote(wb1.at[part, to], dst, at_blk(to, w), sends_w, arrivals)

    def owner_sums(part, own, y_sums):
        total = own
        y_sums.wait_recv()
        for d in range(3):
            total = total + r1[part, d].astype(F32)
        wb1[part, y] = total.astype(BF16)
        for dz in (2, 1, 3, 0):
            zz = (zhi + dz) % 4
            for d in (2, 1, 3, 0):
                ww = (w + d) % 4
                piece = pl.ds(pl.multiple_of(64 * zz + 16 * ww, 16), 16)
                if dz or d:
                    remote(
                        wb1.at[part, y, piece], r2.at[part, zhi, w], at_owner(zz, ww),
                        sends_last, finals,
                    )
                else:
                    r2[part, zhi, w] = wb1[part, y, piece]

    sends_w, sends_last, finals = Sends(), Sends(), Arrivals()
    def wait_x(k):
        x_mate[k].wait_recv()
        x_third[k].wait_recv()

    wait_x(0)
    wait_x(1)
    g_v[2].wait_recv()
    near_tile(1, 2)
    far_g_k = gather_far(0, g_k)
    g_k[2].wait_recv()
    near_tile(0, 2)
    third_x(3)
    wait_x(2)
    near_tile(1, 1)
    near_tile(0, 1)
    far_g_v.wait_recv()
    y_sums_v = far_tile(1, 2)
    far_tile(1, 1, y_sums_v)
    wait_x(3)
    near_tile(1, 3)
    far_tile(1, 3, y_sums_v)
    near_tile(0, 3)
    third_x(4)
    far_g_k.wait_recv()
    y_sums_k = far_tile(0, 2)
    far_tile(0, 1, y_sums_k)
    far_tile(0, 3, y_sums_k)
    x_mate[4].wait_recv()
    x_third[4].wait_recv()
    own_v = weights_of(1, y, (0, 1, 2, 3))
    wacc[0, y] = weights_of(0, y, (0, 1, 2, 3))
    owner_sums(1, own_v, y_sums_v)
    owner_sums(0, wacc[0, y], y_sums_k)
    finals.wait_recv()
    for part in range(2):
        for ww in range(4):
            total = r2[part, 0, ww].astype(F32)
            for zz in range(1, 4):
                total = total + r2[part, zz, ww].astype(F32)
            w_stage[:, pl.ds(512 * part + 128 * ww, 128)] = total
    own_out.append(local(w_stage, w_out))
    for copy in own_out:
        copy.wait()
    far_out.wait_recv()
    assert count == [ARRIVALS, LOCALS, SENDS], count
    for sends in (
        sends_kv, sends_spread, sends_first, sends_x, sends_sum, sends_g, sends_out, sends_w,
        sends_last,
    ):
        sends.wait()


def place(*refs):
    sources, targets, stages, sem_in, sem_out = refs[:4], refs[4:8], refs[8:12], *refs[12:]
    parts = []
    for source, target, stage in zip(sources, targets, stages, strict=True):
        for side in range(4 if source.shape[1] == 2048 else 1):
            at = pl.ds(side * 32, 32) if source.shape[1] == 2048 else slice(None)
            i = len(parts)
            arrive = pltpu.make_async_copy(source.at[at], stage.at[at], sem_in.at[i])
            arrive.start()
            leave = pltpu.make_async_copy(stage.at[at], target.at[at], sem_out.at[i])
            parts.append((arrive, leave))
    for arrive, leave in parts:
        arrive.wait()
        leave.start()
    for _, leave in parts:
        leave.wait()


def body(queries, keys, values, out_grad, layer_input, lengths):
    anywhere = pl.BlockSpec(memory_space=pltpu.HBM)
    vmem = pltpu.VMEM
    shapes = (
        jax.ShapeDtypeStruct((128, 2048), BF16),
        jax.ShapeDtypeStruct((128, 512), BF16),
        jax.ShapeDtypeStruct((128, 512), BF16),
        jax.ShapeDtypeStruct((16, 1024), F32),
    )
    outs = pl.pallas_call(
        kernel,
        out_shape=shapes,
        in_specs=[pl.BlockSpec(memory_space=pltpu.SMEM)] + [anywhere] * 5,
        out_specs=(anywhere,) * 4,
        scratch_shapes=[
            vmem((2, 128, 512), BF16),
            vmem((4, 128, 512), BF16),
            vmem((4, 128, 512), BF16),
            vmem((2048, 256), BF16),
            vmem((128, 4096), BF16),
            vmem((4, 4, 4, 64, 128), BF16),
            vmem((4, 4, 4, 4, 64, 128), BF16),
            vmem((8, 256, 128), BF16),
            vmem((8, 256, 128), BF16),
            vmem((8, 256, 128), BF16),
            vmem((8, 256, 128), BF16),
            vmem((8, 128, 256), BF16),
            vmem((12, 4, 256, 256), F32),
            vmem((12, 4, 256, 256), F32),
            vmem((12, 256, 1024), BF16),
            vmem((12, 256, 1024), BF16),
            vmem((8, 8, 256), F32),
            vmem((8, 8, 256), F32),
            vmem((8, 8, 256), F32),
            vmem((4, 128, 256), F32),
            vmem((4, 128, 512), BF16),
            vmem((2, 4, 2, 256, 128), F32),
            vmem((2, 4, 2, 256, 128), BF16),
            vmem((2, 256, 128), BF16),
            vmem((2, 256, 128), BF16),
            vmem((2, 2, 256, 128), BF16),
            vmem((2, 2, 256, 128), BF16),
            vmem((4, 512, 256), BF16),
            vmem((4, 128, 128), BF16),
            vmem((2, 256, 128), F32),
            vmem((2, 256, 128), F32),
            vmem((2, 4, 256, 128), F32),
            vmem((2, 4, 256, 128), BF16),
            vmem((2, 3, 256, 128), BF16),
            vmem((2, 4, 4, 16, 128), BF16),
            vmem((16, 1024), F32),
            pltpu.SemaphoreType.DMA((SENDS,)),
            pltpu.SemaphoreType.DMA((ARRIVALS,)),
            pltpu.SemaphoreType.DMA((LOCALS,)),
        ],
        compiler_params=pltpu.CompilerParams(
            collective_id=0, has_side_effects=True, vmem_limit_bytes=62 * 1024 * 1024
        ),
        name="attention_backward",
    )(lengths[0], queries[0], out_grad[0], keys[0], values[0], layer_input[0])
    outs = pl.pallas_call(
        place,
        out_shape=shapes,
        in_specs=[anywhere] * 4,
        out_specs=(anywhere,) * 4,
        scratch_shapes=[vmem(shape.shape, shape.dtype) for shape in shapes]
        + [pltpu.SemaphoreType.DMA((7,)), pltpu.SemaphoreType.DMA((7,))],
        name="place_outputs",
    )(*outs)
    return (outs[0][None], outs[1][None], outs[2][None], outs[3])


def solution(mesh):
    placed = (P("dp", "blk", None),) * 5 + (P("dp", None),)
    return jax.shard_map(
        body,
        mesh=mesh,
        in_specs=placed,
        out_specs=(P("dp", "blk", None),) * 3 + (P(("dp", "blk"), None),),
        check_vma=False,
    )
```

```python
import math

import jax
import jax.numpy as jnp
from jax import lax
from jax.experimental import pallas as pl
from jax.experimental.pallas import tpu as pltpu
from jax.sharding import PartitionSpec as P

MESH = pl.DeviceIdType.MESH
F32 = jnp.float32
BF16 = jnp.bfloat16
HEAD = 128
ROPE_BASE = 500000.0
MASKED = -1e30
FAR = 1 << 20
SENDS = 11
ARRIVALS = 52
LOCALS = 18


def nn(a, b):
    return jnp.dot(a, b, preferred_element_type=F32)


def nt(a, b):
    return lax.dot_general(a, b, (((1,), (1,)), ((), ())), preferred_element_type=F32)


def kernel(
    len_ref, q_in, do_in, k_in, v_in, x_in,
    dq_out, dk_out, dv_out, r2,
    kvin, qbuf, dobuf, kv, xv, xt, xbuf, qs, dos, qsn, dosn, kt, p_f, dp_s, p_t, ds_t, top_s, inv_s, del_s, dqacc,
    dqbuf, part_f, part_b, far_a, far_b, near_m, near_p, gbuf, dkbuf, cosb, sinb, wacc, wb1, r1,
    send, recv, loc,
):
    b = lax.axis_index("blk")
    dp = lax.axis_index("dp")
    y, w = b // 4, b % 4
    core = w % 2
    zhi, xx = dp // 4, dp % 4
    yp, y2, ym = (y + 1) % 4, (y + 2) % 4, (y + 3) % 4
    xp, xm = (xx + 1) % 4, (xx + 3) % 4
    scale = 1.0 / math.sqrt(HEAD)
    prompt_len = len_ref[0]
    reject_start = len_ref[0] + len_ref[1]

    count = [0, 0, 0]

    def covering(size):
        if size % 8192:
            return kv.at[pl.ds(0, size // 256), pl.ds(0, 128)]
        if size <= 1 << 20:
            return kv.at[pl.ds(0, size // 512)]
        return ds_t.at[pl.ds(0, size >> 19)]

    def bytes_of(ref):
        return math.prod(ref.shape) * ref.dtype.itemsize

    def wait_bytes(sem, size):
        ref = covering(size)
        pltpu.make_async_copy(ref, ref, sem).wait()

    class Sends:
        def __init__(self):
            self.at = count[2]
            self.size = 0
            count[2] += 1

        def wait(self):
            wait_bytes(send.at[self.at], self.size)

    class Arrivals:
        def __init__(self):
            self.at = count[0]
            self.size = 0
            count[0] += 1

        def wait_recv(self):
            wait_bytes(recv.at[self.at], self.size)

    def remote(src, dst, device, sends, arrivals=None):
        arrivals = arrivals or Arrivals()
        pltpu.make_async_remote_copy(
            src_ref=src, dst_ref=dst, send_sem=send.at[sends.at], recv_sem=recv.at[arrivals.at],
            device_id=device, device_id_type=MESH,
        ).start()
        sends.size += bytes_of(src)
        arrivals.size += bytes_of(src)
        return arrivals

    def local(src, dst):
        i = count[1]
        count[1] += 1
        copy = pltpu.make_async_copy(src, dst, loc.at[i])
        copy.start()
        return copy

    def at_blk(yy, ww):
        return {"blk": 4 * yy + ww}

    def at_x(to):
        return {"dp": 4 * zhi + to}

    def at_owner(zz, ww):
        return {"dp": 4 * zz + xx, "blk": 4 * y + ww}

    def tile(i, size):
        return pl.ds(pl.multiple_of(i * size, size), size)

    barrier = pltpu.get_barrier_semaphore()
    for d in range(1, 4):
        for device in (at_blk((y + d) % 4, w), {"dp": 4 * zhi + (xx + d) % 4}):
            pl.semaphore_signal(barrier, 1, device_id=device, device_id_type=MESH)
    for dz in range(4):
        for d in range(4):
            if dz or d:
                pl.semaphore_signal(
                    barrier, 1, device_id=at_owner((zhi + dz) % 4, (w + d) % 4),
                    device_id_type=MESH,
                )
    staged = [local(ref, kvin.at[part]) for part, ref in ((0, k_in), (1, v_in))]
    for ref, stage in ((q_in, p_t), (do_in, ds_t)):
        for side in range(2):
            staged.append(
                local(ref.at[:, pl.ds(1024 * side, 1024)], stage.at[0, pl.ds(128 * side, 128)])
            )
    x_local = local(x_in, xv)
    kv_slots = (tile(4 * y + w, 64), tile(4 * (7 - y) + 3 - w, 64))
    own_kv = []
    for half in range(2):
        for part, ref in ((0, k_in), (1, v_in)):
            own_kv.append(
                local(
                    ref.at[pl.ds(64 * half, 64), tile(w, 128)],
                    kv.at[kv_slots[half], pl.ds(128 * part, 128)],
                )
            )
    own_q = [
        local(q_in.at[:, tile(w, 512)], qbuf.at[w]),
        local(do_in.at[:, tile(w, 512)], dobuf.at[w]),
    ]
    pl.semaphore_wait(barrier, 21)

    def row_slots(ww):
        return tile(4 * y + ww, 64), tile(4 * (7 - y) + 3 - ww, 64)

    for copy in staged[:2]:
        copy.wait()
    kv_first = {}
    sends_kv = Sends()
    for d in (1, 3, 2):
        ww = (w + d) % 4
        kv_first[d] = Arrivals()
        for half in range(2):
            for part in range(2):
                remote(
                    kvin.at[part, pl.ds(64 * half, 64), tile(ww, 128)],
                    kv.at[kv_slots[half], pl.ds(128 * part, 128)],
                    at_blk(y, ww), sends_kv, kv_first[d],
                )
    for copy in staged[2:]:
        copy.wait()
    sends_q, sends_do, q_first = Sends(), Sends(), Arrivals()
    for d in (1, 3, 2):
        ww = (w + d) % 4
        src = p_t.at[0, tile(ww // 2, 128), tile(ww % 2, 512)]
        remote(src, qbuf.at[w], at_blk(y, ww), sends_q, q_first)
    do_first = {1: Arrivals(), 0: Arrivals()}
    for half in (1, 0):
        for d in (1, 3, 2):
            ww = (w + d) % 4
            src = ds_t.at[0, tile(2 * (ww // 2) + half, 64), tile(ww % 2, 512)]
            dst = dobuf.at[w, pl.ds(64 * half, 64)]
            remote(src, dst, at_blk(y, ww), sends_do, do_first[half])

    sends_spread, kv_rest = Sends(), Arrivals()
    kv_plus, kv_minus = [], []

    def spread(ww):
        slots = row_slots(ww)
        low, high = kv.at[slots[0]], kv.at[slots[1]]
        kv_plus.append(remote(low, low, at_blk(yp, w), sends_spread))
        kv_minus.append(remote(high, high, at_blk(ym, w), sends_spread))
        remote(high, high, at_blk(yp, w), sends_spread, kv_rest)
        remote(low, low, at_blk(ym, w), sends_spread, kv_rest)

    for copy in own_kv:
        copy.wait()
    spread(w)

    x_local.wait()

    def transpose_x(i, carry):
        to = i % 8 // 2
        xt[to, pl.ds((i % 2) * 2, 2), i // 8] = xv[:, tile(i, 128)].T.reshape(2, 64, 128)
        return carry

    lax.fori_loop(0, 32, transpose_x, 0)
    column = tile(w, 128)
    w_other = (w + 2) % 4
    core_mate = at_blk(y, w + 1 - 2 * core)
    z_mate = at_blk(y, (w + 2) % 4)
    sends_x, sends_first, x_first = Sends(), Sends(), Arrivals()
    for d in (1, 3, 2):
        to = (xx + d) % 4
        remote(xt.at[to], xbuf.at[:, 4 - d, w], at_x(to), sends_first, x_first)
    x_far = [remote(xt.at[xx], xbuf.at[:, 0, w], z_mate, sends_x)]
    x_mate = [remote(xt.at[xx], xbuf.at[:, 0, w], core_mate, sends_x)]

    for d in (1, 3, 2):
        kv_first[d].wait_recv()
        spread((w + 4 - d) % 4)
    xbuf[:, 0, w] = xt[xx]
    lane_row = lax.broadcasted_iota(jnp.int32, (1, HEAD), 1)
    frequency = jnp.exp(
        -(2.0 * (lane_row % 64).astype(F32) / HEAD) * math.log(ROPE_BASE)
    )
    for half, block in ((0, y), (1, 7 - y)):
        position = 256 * block + lax.broadcasted_iota(jnp.int32, (256, HEAD), 0)
        angles = position.astype(F32) * frequency
        cosb[half] = jnp.cos(angles)
        sinb[half] = jnp.where(lane_row < 64, jnp.sin(angles), -jnp.sin(angles))

    kv_second = Arrivals()
    for k, d in enumerate((0, 1, 3, 2)):
        ww = (w + 4 - d) % 4
        kv_plus[k].wait_recv()
        ref = kv.at[tile(4 * ym + ww, 64)]
        remote(ref, ref, at_blk(yp, w), sends_spread, kv_second)
        kv_minus[k].wait_recv()
        ref = kv.at[tile(4 * (7 - yp) + 3 - ww, 64)]
        remote(ref, ref, at_blk(ym, w), sends_spread, kv_second)
    kv_rest.wait_recv()

    own_q[0].wait()
    q_first.wait_recv()

    def stack(buf, stacked, halves):
        for half in halves:
            for h in range(4):
                for ww in range(4):
                    piece = buf[ww, pl.ds(64 * half, 64), pl.ds(128 * h, 128)]
                    stacked[4 * half + h, pl.ds(64 * ww, 64)] = piece

    stack(qbuf, qs, (0, 1))

    lane = lax.broadcasted_iota(jnp.int32, (1, 256), 1)
    lane_high = (3 - lane // 64) * 64 + lane % 64
    rows = lax.broadcasted_iota(jnp.int32, (256, 256), 0)
    zero = jnp.zeros((8, 256), F32)

    def score_block(half, j):
        diagonal = y + half * (7 - 2 * y)
        query_pos = 256 * diagonal + lane + half * (lane_high - lane)
        rejected = query_pos >= reject_start
        key_pos = 256 * j + rows
        chosen = jnp.logical_and(key_pos >= prompt_len, key_pos < reject_start)
        shown = jnp.where(rejected, jnp.where(chosen, FAR, key_pos), key_pos)
        bias = jnp.where(shown <= query_pos, 0.0, MASKED)
        key = kv[tile(j, 256), pl.ds(0, 128)]
        out = []
        for h in range(4):
            s = nt(key, qs[4 * half + h]) + bias
            p_f[4 * half + j, h] = s
            out.append(jnp.max(s.reshape(32, 8, 256), axis=0))
        return out

    last_high = (5 - y) // 4

    def scores_half(half, carry):
        def scores(t, tops):
            j = t + (t - y2 + 8) // 8
            j = j + (j - (7 - y2) + 8) // 8
            new = score_block(half, j)
            return tuple(jnp.maximum(tops[h], new[h]) for h in range(4))

        blocks = half * (7 - y - last_high) + (1 - half) * (y + last_high)
        tops = lax.fori_loop(0, blocks, scores, (jnp.full((8, 256), MASKED, F32),) * 4)
        for h in range(4):
            top_s[4 * half + h] = tops[h]
        return carry

    lax.fori_loop(0, 2, scores_half, 0)
    kv_second.wait_recv()

    def last_block(i, carry):
        half = i * last_high + (1 - i)
        j = half * i * (7 - y2) + (1 - half * i) * y2
        new = score_block(half, j)
        for h in range(4):
            top_s[4 * half + h] = jnp.maximum(top_s[4 * half + h], new[h])
        return carry

    lax.fori_loop(0, 2, last_block, 0)

    own_q[1].wait()
    sends_q.wait()
    do_first[1].wait_recv()
    stack(dobuf, dos, (1,))

    def weights_half(half, carry):
        blocks = y + half * (7 - 2 * y) + 1
        tops = [jnp.max(top_s[4 * half + h], axis=0, keepdims=True) for h in range(4)]

        def weights(j, sums):
            value = kv[tile(j, 256), pl.ds(128, 128)]
            slot = 4 * half + j
            totals, dots = [], []
            for h in range(4):
                p = jnp.exp2((p_f[slot, h] - tops[h]) * (scale * math.log2(math.e)))
                p_f[slot, h] = p
                p_t[slot, :, pl.ds(256 * h, 256)] = p.astype(BF16)
                totals.append(sums[0][h] + jnp.sum(p.reshape(32, 8, 256), axis=0))
                d = nt(value, dos[4 * half + h])
                dp_s[slot, h] = d
                dots.append(sums[1][h] + jnp.sum((p * d).reshape(32, 8, 256), axis=0))
            return tuple(totals), tuple(dots)

        totals, dots = lax.fori_loop(0, blocks, weights, ((zero,) * 4, (zero,) * 4))
        for h in range(4):
            inverse = 1.0 / jnp.sum(totals[h], axis=0, keepdims=True)
            delta = jnp.sum(dots[h], axis=0, keepdims=True) * inverse
            inv_s[4 * half + h] = jnp.broadcast_to(inverse, (8, 256))
            del_s[4 * half + h] = jnp.broadcast_to(delta, (8, 256))
        return carry

    weights_half(1, 0)
    order = (2, 1, 3, 0)
    x_first.wait_recv()
    for d in order:
        ref = xbuf.at[(y + d) % 4, pl.ds(1, 3), w]
        x_far.append(remote(ref, ref, z_mate, sends_x))
        x_mate.append(remote(ref, ref, core_mate, sends_x))
    do_first[0].wait_recv()
    stack(dobuf, dos, (0,))
    weights_half(0, 0)

    def scale_rows(c, carry):
        per_row = jnp.broadcast_to(inv_s[c, pl.ds(0, 1)], (128, 256)).T
        dosn[c] = (dos[c].astype(F32) * per_row).astype(BF16)
        qsn[c] = (qs[c].astype(F32) * (per_row * scale)).astype(BF16)
        return carry

    lax.fori_loop(0, 8, scale_rows, 0, unroll=True)
    def sums_for(yy, left, right):
        g = (yy - y + 4) // 5
        low = nn(left[4 + yy], right[pl.ds(4, 4)].reshape(1024, 128))
        more = nn(
            left[g * (11 - yy) + (1 - g) * yy], right[pl.ds(4 * g, 4)].reshape(1024, 128)
        )
        keep = g.astype(F32)
        return low + more * (1.0 - keep), more * keep

    def own_sums(left, right):
        low = nn(left[4 + y], right[pl.ds(4, 4)].reshape(1024, 128))
        low = low + nn(left[y], right[pl.ds(0, 4)].reshape(1024, 128))
        return low, nn(left[11 - y], right[pl.ds(4, 4)].reshape(1024, 128))

    def reduce_first(part, left, right):
        low, high = sums_for(y2, left, right)
        part_b[part, y2, 0] = low.astype(BF16)
        part_b[part, y2, 1] = high.astype(BF16)
        return (
            remote(part_b.at[part, y2, 0], far_a.at[part], at_blk(yp, w), sends_sum),
            remote(part_b.at[part, y2, 1], far_b.at[part], at_blk(ym, w), sends_sum),
        )

    def reduce_middle(part, left, right):
        for yy in (yp, ym):
            low, high = sums_for(yy, left, right)
            part_f[part, yy, 0] = low
            part_f[part, yy, 1] = high

    def reduce_second(part, far):
        out = []
        far[0].wait_recv()
        part_b[part, yp, 0] = (part_f[part, yp, 0] + far_a[part].astype(F32)).astype(BF16)
        part_b[part, yp, 1] = part_f[part, yp, 1].astype(BF16)
        out.append(remote(part_b.at[part, yp], near_m.at[part], at_blk(yp, w), sends_sum))
        far[1].wait_recv()
        part_b[part, ym, 0] = part_f[part, ym, 0].astype(BF16)
        part_b[part, ym, 1] = (part_f[part, ym, 1] + far_b[part].astype(F32)).astype(BF16)
        out.append(remote(part_b.at[part, ym], near_p.at[part], at_blk(ym, w), sends_sum))
        return out

    def reduce_own(part, left, right):
        low, high = own_sums(left, right)
        part_f[part, y, 0] = low
        part_f[part, y, 1] = high

    sends_sum = Sends()
    far_v = reduce_first(1, p_t, dosn)
    reduce_middle(1, p_t, dosn)

    sends_do.wait()
    def grads_half(half, carry):
        blocks = y + half * (7 - 2 * y) + 1
        deltas = [del_s[4 * half + h, pl.ds(0, 1)] for h in range(4)]

        def grads(j, carry):
            slot = 4 * half + j
            for h in range(4):
                ds = p_f[slot, h] * (dp_s[slot, h] - deltas[h])
                ds_t[slot, :, pl.ds(256 * h, 256)] = ds.astype(BF16)
            return carry

        return lax.fori_loop(0, blocks, grads, carry)

    lax.fori_loop(0, 2, grads_half, 0)

    far_k = reduce_first(0, ds_t, qsn)
    reduce_middle(0, ds_t, qsn)
    near_v = reduce_second(1, far_v)
    reduce_own(1, p_t, dosn)
    reduce_own(0, ds_t, qsn)
    near_k = reduce_second(0, far_k)
    def transpose_k(j, carry):
        kt[j] = kv[tile(j, 256), pl.ds(0, 128)].T
        return carry

    lax.fori_loop(0, 8, transpose_k, 0, unroll=2)

    def query_half(half, carry):
        blocks = y + half * (7 - 2 * y) + 1
        dqacc[...] = jnp.zeros_like(dqacc)

        def one(j, carry):
            for h in range(4):
                dqacc[h] += nn(kt[j], ds_t[4 * half + j, :, pl.ds(256 * h, 256)])
            return carry

        lax.fori_loop(0, blocks, one, 0)
        for h in range(4):
            dq = dqacc[h] * (inv_s[4 * half + h, pl.ds(0, 1)] * scale)
            dq = dq.T.astype(BF16)
            for ww in range(4):
                dqbuf[ww, tile(half, 64), pl.ds(128 * h, 128)] = dq[64 * ww : 64 * ww + 64]
        return carry

    lax.fori_loop(0, 2, query_half, 0)
    sends_out, far_out = Sends(), Arrivals()
    own_out = [local(dqbuf.at[w], dq_out.at[:, tile(w, 512)])]
    for d in (2, 1, 3):
        ww = (w + d) % 4
        dst = dq_out.at[:, tile(w, 512)]
        remote(dqbuf.at[ww], dst, at_blk(y, ww), sends_out, far_out)
    for copy in near_v:
        copy.wait_recv()

    def gathered(part, half):
        own = part_f[part, y, half]
        return own + near_m[part, half].astype(F32) + near_p[part, half].astype(F32)

    for half in range(2):
        value_grad = gathered(1, half).astype(BF16)
        for ww in range(4):
            at = 64 * ww if half == 0 else 64 * (3 - ww)
            rows_at = pl.ds(128 * ww + 64 * half, 64)
            gbuf[0, rows_at, pl.ds(128, 128)] = value_grad[at : at + 64]

    low_rows, high_rows = pl.ds(0, 256), pl.ds(256, 256)

    def gather_near(part):
        lanes = pl.ds(128 * part, 128)
        low, high = gbuf.at[0, low_rows, lanes], gbuf.at[0, high_rows, lanes]
        plus = remote(low, gbuf.at[3, low_rows, lanes], at_x(xp), sends_g)
        minus = remote(high, gbuf.at[1, high_rows, lanes], at_x(xm), sends_g)
        rest = remote(high, gbuf.at[3, high_rows, lanes], at_x(xp), sends_g)
        remote(low, gbuf.at[1, low_rows, lanes], at_x(xm), sends_g, rest)
        return plus, minus, rest

    def gather_far(part, near):
        lanes = pl.ds(128 * part, 128)
        near[0].wait_recv()
        src, dst = gbuf.at[3, low_rows, lanes], gbuf.at[2, low_rows, lanes]
        far = remote(src, dst, at_x(xp), sends_g)
        near[1].wait_recv()
        src, dst = gbuf.at[1, high_rows, lanes], gbuf.at[2, high_rows, lanes]
        return remote(src, dst, at_x(xm), sends_g, far)

    sends_g = Sends()
    g_v = gather_near(1)
    x_third = []

    def third_x(k):
        x_far[k].wait_recv()
        if k == 0:
            ref = xbuf.at[:, 0, w_other]
        else:
            ref = xbuf.at[(y + order[k - 1]) % 4, pl.ds(1, 3), w_other]
        x_third.append(remote(ref, ref, core_mate, sends_x))

    third_x(0)
    third_x(1)
    for copy in near_k:
        copy.wait_recv()
    for half in range(2):
        key_sum = gathered(0, half)
        key_grad = key_sum.astype(BF16)
        key_pre = (
            key_sum * cosb[half] + pltpu.roll(key_sum, 64, 1) * sinb[half]
        ).astype(BF16)
        for ww in range(4):
            at = 64 * ww if half == 0 else 64 * (3 - ww)
            gbuf[0, pl.ds(128 * ww + 64 * half, 64), pl.ds(0, 128)] = key_pre[at : at + 64]
            dkbuf[ww, pl.ds(64 * half, 64)] = key_grad[at : at + 64]
    g_k = gather_near(0)
    values_out = pl.ds(128, 128)
    own_out.append(local(dkbuf.at[w], dk_out.at[:, column]))
    own_out.append(local(gbuf.at[0, tile(w, 128), values_out], dv_out.at[:, column]))
    for d in (2, 1, 3):
        ww = (w + d) % 4
        values = gbuf.at[0, tile(ww, 128), values_out]
        remote(dkbuf.at[ww], dk_out.at[:, column], at_blk(y, ww), sends_out, far_out)
        remote(values, dv_out.at[:, column], at_blk(y, ww), sends_out, far_out)
    far_g_v = gather_far(1, g_v)
    third_x(2)

    def weights_of(part, to, rels):
        lanes = pl.ds(128 * part, 128)
        total = None
        for rel in rels:
            left = [xbuf[to, rel, ww].reshape(256, 128) for ww in range(4)]
            term = nn(jnp.concatenate(left, axis=1), gbuf[rel, :, lanes])
            total = term if total is None else total + term
        return total

    def near_tile(part, d):
        to = (y + d) % 4
        wacc[part, to] = weights_of(part, to, (0, 1, 3))

    def far_tile(part, d, arrivals=None):
        to = (y + d) % 4
        wb1[part, to] = (wacc[part, to] + weights_of(part, to, (2,))).astype(BF16)
        dst = r1.at[part, d - 1]
        return remote(wb1.at[part, to], dst, at_blk(to, w), sends_w, arrivals)

    def owner_sums(part, own, y_sums):
        total = own
        y_sums.wait_recv()
        for d in range(3):
            total = total + r1[part, d].astype(F32)
        wb1[part, y] = total.astype(BF16)
        for dz in (2, 1, 3, 0):
            zz = (zhi + dz) % 4
            for d in (2, 1, 3, 0):
                ww = (w + d) % 4
                piece = pl.ds(pl.multiple_of(64 * zz + 16 * ww, 16), 16)
                if dz or d:
                    remote(
                        wb1.at[part, y, piece], r2.at[part, zhi, w], at_owner(zz, ww),
                        sends_last, finals,
                    )
                else:
                    own_out.append(local(wb1.at[part, y, piece], r2.at[part, zhi, w]))

    sends_w, sends_last, finals = Sends(), Sends(), Arrivals()
    def wait_x(k):
        x_mate[k].wait_recv()
        x_third[k].wait_recv()

    wait_x(0)
    wait_x(1)
    g_v[2].wait_recv()
    near_tile(1, 2)
    far_g_k = gather_far(0, g_k)
    g_k[2].wait_recv()
    near_tile(0, 2)
    third_x(3)
    wait_x(2)
    near_tile(1, 1)
    near_tile(0, 1)
    far_g_v.wait_recv()
    y_sums_v = far_tile(1, 2)
    far_tile(1, 1, y_sums_v)
    wait_x(3)
    near_tile(1, 3)
    far_tile(1, 3, y_sums_v)
    near_tile(0, 3)
    third_x(4)
    far_g_k.wait_recv()
    y_sums_k = far_tile(0, 2)
    far_tile(0, 1, y_sums_k)
    far_tile(0, 3, y_sums_k)
    x_mate[4].wait_recv()
    x_third[4].wait_recv()
    own_v = weights_of(1, y, (0, 1, 2, 3))
    wacc[0, y] = weights_of(0, y, (0, 1, 2, 3))
    owner_sums(1, own_v, y_sums_v)
    owner_sums(0, wacc[0, y], y_sums_k)
    finals.wait_recv()
    for copy in own_out:
        copy.wait()
    far_out.wait_recv()
    assert count == [ARRIVALS, LOCALS, SENDS], count
    for sends in (
        sends_kv, sends_spread, sends_first, sends_x, sends_sum, sends_g, sends_out, sends_w,
        sends_last,
    ):
        sends.wait()


def place(*refs):
    sources, targets, stages = refs[:4], refs[4:8], refs[8:12]
    w_stage, sem_in, sem_out = refs[12:]
    pieces = pltpu.make_async_copy(sources[3], stages[3], sem_in.at[6])
    pieces.start()
    parts = []
    for source, target, stage in zip(sources[:3], targets[:3], stages[:3], strict=True):
        for side in range(4 if source.shape[1] == 2048 else 1):
            at = pl.ds(side * 32, 32) if source.shape[1] == 2048 else slice(None)
            i = len(parts)
            arrive = pltpu.make_async_copy(source.at[at], stage.at[at], sem_in.at[i])
            arrive.start()
            leave = pltpu.make_async_copy(stage.at[at], target.at[at], sem_out.at[i])
            parts.append((arrive, leave))
    pieces.wait()
    for part in range(2):
        for ww in range(4):
            total = stages[3][part, 0, ww].astype(F32)
            for zz in range(1, 4):
                total = total + stages[3][part, zz, ww].astype(F32)
            w_stage[:, pl.ds(512 * part + 128 * ww, 128)] = total
    last = pltpu.make_async_copy(w_stage, targets[3], sem_out.at[6])
    last.start()
    for arrive, leave in parts:
        arrive.wait()
        leave.start()
    for _, leave in parts:
        leave.wait()
    last.wait()


def body(queries, keys, values, out_grad, layer_input, lengths):
    anywhere = pl.BlockSpec(memory_space=pltpu.HBM)
    vmem = pltpu.VMEM
    shapes = (
        jax.ShapeDtypeStruct((128, 2048), BF16),
        jax.ShapeDtypeStruct((128, 512), BF16),
        jax.ShapeDtypeStruct((128, 512), BF16),
        jax.ShapeDtypeStruct((2, 4, 4, 16, 128), BF16),
    )
    weight = jax.ShapeDtypeStruct((16, 1024), F32)
    outs = pl.pallas_call(
        kernel,
        out_shape=shapes,
        in_specs=[pl.BlockSpec(memory_space=pltpu.SMEM)] + [anywhere] * 5,
        out_specs=(anywhere,) * 4,
        scratch_shapes=[
            vmem((2, 128, 512), BF16),
            vmem((4, 128, 512), BF16),
            vmem((4, 128, 512), BF16),
            vmem((2048, 256), BF16),
            vmem((128, 4096), BF16),
            vmem((4, 4, 4, 64, 128), BF16),
            vmem((4, 4, 4, 4, 64, 128), BF16),
            vmem((8, 256, 128), BF16),
            vmem((8, 256, 128), BF16),
            vmem((8, 256, 128), BF16),
            vmem((8, 256, 128), BF16),
            vmem((8, 128, 256), BF16),
            vmem((12, 4, 256, 256), F32),
            vmem((12, 4, 256, 256), F32),
            vmem((12, 256, 1024), BF16),
            vmem((12, 256, 1024), BF16),
            vmem((8, 8, 256), F32),
            vmem((8, 8, 256), F32),
            vmem((8, 8, 256), F32),
            vmem((4, 128, 256), F32),
            vmem((4, 128, 512), BF16),
            vmem((2, 4, 2, 256, 128), F32),
            vmem((2, 4, 2, 256, 128), BF16),
            vmem((2, 256, 128), BF16),
            vmem((2, 256, 128), BF16),
            vmem((2, 2, 256, 128), BF16),
            vmem((2, 2, 256, 128), BF16),
            vmem((4, 512, 256), BF16),
            vmem((4, 128, 128), BF16),
            vmem((2, 256, 128), F32),
            vmem((2, 256, 128), F32),
            vmem((2, 4, 256, 128), F32),
            vmem((2, 4, 256, 128), BF16),
            vmem((2, 3, 256, 128), BF16),
            pltpu.SemaphoreType.DMA((SENDS,)),
            pltpu.SemaphoreType.DMA((ARRIVALS,)),
            pltpu.SemaphoreType.DMA((LOCALS,)),
        ],
        compiler_params=pltpu.CompilerParams(
            collective_id=0, has_side_effects=True, vmem_limit_bytes=62 * 1024 * 1024
        ),
        name="attention_backward",
    )(lengths[0], queries[0], out_grad[0], keys[0], values[0], layer_input[0])
    outs = pl.pallas_call(
        place,
        out_shape=(*shapes[:3], weight),
        in_specs=[anywhere] * 4,
        out_specs=(anywhere,) * 4,
        scratch_shapes=[vmem(shape.shape, shape.dtype) for shape in shapes]
        + [vmem((16, 1024), F32), pltpu.SemaphoreType.DMA((7,)), pltpu.SemaphoreType.DMA((7,))],
        name="place_outputs",
    )(*outs)
    return (outs[0][None], outs[1][None], outs[2][None], outs[3])


def solution(mesh):
    placed = (P("dp", "blk", None),) * 5 + (P("dp", None),)
    return jax.shard_map(
        body,
        mesh=mesh,
        in_specs=placed,
        out_specs=(P("dp", "blk", None),) * 3 + (P(("dp", "blk"), None),),
        check_vma=False,
    )
```

```python
import math

import jax
import jax.numpy as jnp
from jax import lax
from jax.experimental import pallas as pl
from jax.experimental.pallas import tpu as pltpu
from jax.sharding import PartitionSpec as P

MESH = pl.DeviceIdType.MESH
F32 = jnp.float32
BF16 = jnp.bfloat16
HEAD = 128
ROPE_BASE = 500000.0
MASKED = -1e30
FAR = 1 << 20
SENDS = 11
ARRIVALS = 52
LOCALS = 18


def nn(a, b):
    return jnp.dot(a, b, preferred_element_type=F32)


def nt(a, b):
    return lax.dot_general(a, b, (((1,), (1,)), ((), ())), preferred_element_type=F32)


def kernel(
    len_ref, q_in, do_in, k_in, v_in, x_in,
    dq_out, dk_out, dv_out, r2,
    kvin, qbuf, dobuf, kv, xv, xt, xbuf, qs, dos, qsn, dosn, kt, p_f, dp_s, p_t, ds_t, top_s, inv_s, del_s, dqacc,
    dqbuf, part_f, part_b, far_a, far_b, near_m, near_p, gbuf, dkbuf, cosb, sinb, wacc, wb1, r1,
    send, recv, loc,
):
    b = lax.axis_index("blk")
    dp = lax.axis_index("dp")
    y, w = b // 4, b % 4
    core = w % 2
    zhi, xx = dp // 4, dp % 4
    yp, y2, ym = (y + 1) % 4, (y + 2) % 4, (y + 3) % 4
    xp, xm = (xx + 1) % 4, (xx + 3) % 4
    scale = 1.0 / math.sqrt(HEAD)
    prompt_len = len_ref[0]
    reject_start = len_ref[0] + len_ref[1]

    count = [0, 0, 0]

    def covering(size):
        if size % 8192:
            return kv.at[pl.ds(0, size // 256), pl.ds(0, 128)]
        if size <= 1 << 20:
            return kv.at[pl.ds(0, size // 512)]
        return ds_t.at[pl.ds(0, size >> 19)]

    def bytes_of(ref):
        return math.prod(ref.shape) * ref.dtype.itemsize

    def wait_bytes(sem, size):
        ref = covering(size)
        pltpu.make_async_copy(ref, ref, sem).wait()

    class Sends:
        def __init__(self):
            self.at = count[2]
            self.size = 0
            count[2] += 1

        def wait(self):
            wait_bytes(send.at[self.at], self.size)

    class Arrivals:
        def __init__(self):
            self.at = count[0]
            self.size = 0
            count[0] += 1

        def wait_recv(self):
            wait_bytes(recv.at[self.at], self.size)

    def remote(src, dst, device, sends, arrivals=None):
        arrivals = arrivals or Arrivals()
        pltpu.make_async_remote_copy(
            src_ref=src, dst_ref=dst, send_sem=send.at[sends.at], recv_sem=recv.at[arrivals.at],
            device_id=device, device_id_type=MESH,
        ).start()
        sends.size += bytes_of(src)
        arrivals.size += bytes_of(src)
        return arrivals

    def local(src, dst):
        i = count[1]
        count[1] += 1
        copy = pltpu.make_async_copy(src, dst, loc.at[i])
        copy.start()
        return copy

    def at_blk(yy, ww):
        return {"blk": 4 * yy + ww}

    def at_x(to):
        return {"dp": 4 * zhi + to}

    def at_owner(zz, ww):
        return {"dp": 4 * zz + xx, "blk": 4 * y + ww}

    def tile(i, size):
        return pl.ds(pl.multiple_of(i * size, size), size)

    barrier = pltpu.get_barrier_semaphore()
    for d in range(1, 4):
        for device in (at_blk((y + d) % 4, w), {"dp": 4 * zhi + (xx + d) % 4}):
            pl.semaphore_signal(barrier, 1, device_id=device, device_id_type=MESH)
    for dz in range(4):
        for d in range(4):
            if dz or d:
                pl.semaphore_signal(
                    barrier, 1, device_id=at_owner((zhi + dz) % 4, (w + d) % 4),
                    device_id_type=MESH,
                )
    staged = [local(ref, kvin.at[part]) for part, ref in ((0, k_in), (1, v_in))]
    for ref, stage in ((q_in, p_t), (do_in, ds_t)):
        for side in range(2):
            staged.append(
                local(ref.at[:, pl.ds(1024 * side, 1024)], stage.at[0, pl.ds(128 * side, 128)])
            )
    x_local = local(x_in, xv)
    kv_slots = (tile(4 * y + w, 64), tile(4 * (7 - y) + 3 - w, 64))
    own_kv = []
    for half in range(2):
        for part, ref in ((0, k_in), (1, v_in)):
            own_kv.append(
                local(
                    ref.at[pl.ds(64 * half, 64), tile(w, 128)],
                    kv.at[kv_slots[half], pl.ds(128 * part, 128)],
                )
            )
    own_q = [
        local(q_in.at[:, tile(w, 512)], qbuf.at[w]),
        local(do_in.at[:, tile(w, 512)], dobuf.at[w]),
    ]
    pl.semaphore_wait(barrier, 21)

    def row_slots(ww):
        return tile(4 * y + ww, 64), tile(4 * (7 - y) + 3 - ww, 64)

    for copy in staged[:2]:
        copy.wait()
    kv_first = {}
    sends_kv = Sends()
    for d in (1, 3, 2):
        ww = (w + d) % 4
        kv_first[d] = Arrivals()
        for half in range(2):
            for part in range(2):
                remote(
                    kvin.at[part, pl.ds(64 * half, 64), tile(ww, 128)],
                    kv.at[kv_slots[half], pl.ds(128 * part, 128)],
                    at_blk(y, ww), sends_kv, kv_first[d],
                )
    for copy in staged[2:]:
        copy.wait()
    sends_q, sends_do, q_first = Sends(), Sends(), Arrivals()
    for d in (1, 3, 2):
        ww = (w + d) % 4
        src = p_t.at[0, tile(ww // 2, 128), tile(ww % 2, 512)]
        remote(src, qbuf.at[w], at_blk(y, ww), sends_q, q_first)
    do_first = {1: Arrivals(), 0: Arrivals()}
    for half in (1, 0):
        for d in (1, 3, 2):
            ww = (w + d) % 4
            src = ds_t.at[0, tile(2 * (ww // 2) + half, 64), tile(ww % 2, 512)]
            dst = dobuf.at[w, pl.ds(64 * half, 64)]
            remote(src, dst, at_blk(y, ww), sends_do, do_first[half])

    sends_spread, kv_rest = Sends(), Arrivals()
    kv_plus, kv_minus = [], []

    def spread(ww):
        slots = row_slots(ww)
        low, high = kv.at[slots[0]], kv.at[slots[1]]
        kv_plus.append(remote(low, low, at_blk(yp, w), sends_spread))
        kv_minus.append(remote(high, high, at_blk(ym, w), sends_spread))
        remote(high, high, at_blk(yp, w), sends_spread, kv_rest)
        remote(low, low, at_blk(ym, w), sends_spread, kv_rest)

    for copy in own_kv:
        copy.wait()
    spread(w)

    x_local.wait()

    def transpose_x(i, carry):
        to = i % 8 // 2
        xt[to, pl.ds((i % 2) * 2, 2), i // 8] = xv[:, tile(i, 128)].T.reshape(2, 64, 128)
        return carry

    lax.fori_loop(0, 32, transpose_x, 0)
    column = tile(w, 128)
    w_other = (w + 2) % 4
    core_mate = at_blk(y, w + 1 - 2 * core)
    z_mate = at_blk(y, (w + 2) % 4)
    sends_x, sends_first, x_first = Sends(), Sends(), Arrivals()
    for d in (1, 3, 2):
        to = (xx + d) % 4
        remote(xt.at[to], xbuf.at[:, 4 - d, w], at_x(to), sends_first, x_first)
    x_far = [remote(xt.at[xx], xbuf.at[:, 0, w], z_mate, sends_x)]
    x_mate = [remote(xt.at[xx], xbuf.at[:, 0, w], core_mate, sends_x)]

    for d in (1, 3, 2):
        kv_first[d].wait_recv()
        spread((w + 4 - d) % 4)
    xbuf[:, 0, w] = xt[xx]
    lane_row = lax.broadcasted_iota(jnp.int32, (1, HEAD), 1)
    frequency = jnp.exp(
        -(2.0 * (lane_row % 64).astype(F32) / HEAD) * math.log(ROPE_BASE)
    )
    for half, block in ((0, y), (1, 7 - y)):
        position = 256 * block + lax.broadcasted_iota(jnp.int32, (256, HEAD), 0)
        angles = position.astype(F32) * frequency
        cosb[half] = jnp.cos(angles)
        sinb[half] = jnp.where(lane_row < 64, jnp.sin(angles), -jnp.sin(angles))

    kv_second = Arrivals()
    for k, d in enumerate((0, 1, 3, 2)):
        ww = (w + 4 - d) % 4
        kv_plus[k].wait_recv()
        ref = kv.at[tile(4 * ym + ww, 64)]
        remote(ref, ref, at_blk(yp, w), sends_spread, kv_second)
        kv_minus[k].wait_recv()
        ref = kv.at[tile(4 * (7 - yp) + 3 - ww, 64)]
        remote(ref, ref, at_blk(ym, w), sends_spread, kv_second)
    kv_rest.wait_recv()

    own_q[0].wait()
    q_first.wait_recv()

    def stack(buf, stacked, halves):
        for half in halves:
            for h in range(4):
                for ww in range(4):
                    piece = buf[ww, pl.ds(64 * half, 64), pl.ds(128 * h, 128)]
                    stacked[4 * half + h, pl.ds(64 * ww, 64)] = piece

    stack(qbuf, qs, (0, 1))

    lane = lax.broadcasted_iota(jnp.int32, (1, 256), 1)
    lane_high = (3 - lane // 64) * 64 + lane % 64
    rows = lax.broadcasted_iota(jnp.int32, (256, 256), 0)
    zero = jnp.zeros((8, 256), F32)

    def score_block(half, j):
        diagonal = y + half * (7 - 2 * y)
        query_pos = 256 * diagonal + lane + half * (lane_high - lane)
        rejected = query_pos >= reject_start
        key_pos = 256 * j + rows
        chosen = jnp.logical_and(key_pos >= prompt_len, key_pos < reject_start)
        shown = jnp.where(rejected, jnp.where(chosen, FAR, key_pos), key_pos)
        bias = jnp.where(shown <= query_pos, 0.0, MASKED)
        key = kv[tile(j, 256), pl.ds(0, 128)]
        out = []
        for h in range(4):
            s = nt(key, qs[4 * half + h]) + bias
            p_f[4 * half + j, h] = s
            out.append(jnp.max(s.reshape(32, 8, 256), axis=0))
        return out

    last_high = (5 - y) // 4

    def scores_half(half, carry):
        def scores(t, tops):
            j = t + (t - y2 + 8) // 8
            j = j + (j - (7 - y2) + 8) // 8
            new = score_block(half, j)
            return tuple(jnp.maximum(tops[h], new[h]) for h in range(4))

        blocks = half * (7 - y - last_high) + (1 - half) * (y + last_high)
        tops = lax.fori_loop(0, blocks, scores, (jnp.full((8, 256), MASKED, F32),) * 4)
        for h in range(4):
            top_s[4 * half + h] = tops[h]
        return carry

    lax.fori_loop(0, 2, scores_half, 0)
    kv_second.wait_recv()

    def last_block(i, carry):
        half = i * last_high + (1 - i)
        j = half * i * (7 - y2) + (1 - half * i) * y2
        new = score_block(half, j)
        for h in range(4):
            top_s[4 * half + h] = jnp.maximum(top_s[4 * half + h], new[h])
        return carry

    lax.fori_loop(0, 2, last_block, 0)

    own_q[1].wait()
    sends_q.wait()
    do_first[1].wait_recv()
    stack(dobuf, dos, (1,))

    def weights_half(half, carry):
        blocks = y + half * (7 - 2 * y) + 1
        tops = [jnp.max(top_s[4 * half + h], axis=0, keepdims=True) for h in range(4)]

        def weights(j, sums):
            value = kv[tile(j, 256), pl.ds(128, 128)]
            slot = 4 * half + j
            totals, dots = [], []
            for h in range(4):
                p = jnp.exp2((p_f[slot, h] - tops[h]) * (scale * math.log2(math.e)))
                p_f[slot, h] = p
                p_t[slot, :, pl.ds(256 * h, 256)] = p.astype(BF16)
                totals.append(sums[0][h] + jnp.sum(p.reshape(32, 8, 256), axis=0))
                d = nt(value, dos[4 * half + h])
                dp_s[slot, h] = d
                dots.append(sums[1][h] + jnp.sum((p * d).reshape(32, 8, 256), axis=0))
            return tuple(totals), tuple(dots)

        totals, dots = lax.fori_loop(0, blocks, weights, ((zero,) * 4, (zero,) * 4))
        for h in range(4):
            inverse = 1.0 / jnp.sum(totals[h], axis=0, keepdims=True)
            delta = jnp.sum(dots[h], axis=0, keepdims=True) * inverse
            inv_s[4 * half + h] = jnp.broadcast_to(inverse, (8, 256))
            del_s[4 * half + h] = jnp.broadcast_to(delta, (8, 256))
        return carry

    weights_half(1, 0)
    do_first[0].wait_recv()
    stack(dobuf, dos, (0,))
    weights_half(0, 0)

    order = (2, 1, 3, 0)
    x_first.wait_recv()
    for d in order:
        ref = xbuf.at[(y + d) % 4, pl.ds(1, 3), w]
        x_far.append(remote(ref, ref, z_mate, sends_x))
        x_mate.append(remote(ref, ref, core_mate, sends_x))
    def scale_rows(c, carry):
        per_row = jnp.broadcast_to(inv_s[c, pl.ds(0, 1)], (128, 256)).T
        dosn[c] = (dos[c].astype(F32) * per_row).astype(BF16)
        qsn[c] = (qs[c].astype(F32) * (per_row * scale)).astype(BF16)
        return carry

    lax.fori_loop(0, 8, scale_rows, 0, unroll=True)
    def sums_for(yy, left, right):
        g = (yy - y + 4) // 5
        low = nn(left[4 + yy], right[pl.ds(4, 4)].reshape(1024, 128))
        more = nn(
            left[g * (11 - yy) + (1 - g) * yy], right[pl.ds(4 * g, 4)].reshape(1024, 128)
        )
        keep = g.astype(F32)
        return low + more * (1.0 - keep), more * keep

    def own_sums(left, right):
        low = nn(left[4 + y], right[pl.ds(4, 4)].reshape(1024, 128))
        low = low + nn(left[y], right[pl.ds(0, 4)].reshape(1024, 128))
        return low, nn(left[11 - y], right[pl.ds(4, 4)].reshape(1024, 128))

    def reduce_first(part, left, right):
        low, high = sums_for(y2, left, right)
        part_b[part, y2, 0] = low.astype(BF16)
        part_b[part, y2, 1] = high.astype(BF16)
        return (
            remote(part_b.at[part, y2, 0], far_a.at[part], at_blk(yp, w), sends_sum),
            remote(part_b.at[part, y2, 1], far_b.at[part], at_blk(ym, w), sends_sum),
        )

    def reduce_middle(part, left, right):
        for yy in (yp, ym):
            low, high = sums_for(yy, left, right)
            part_f[part, yy, 0] = low
            part_f[part, yy, 1] = high

    def reduce_second(part, far):
        out = []
        far[0].wait_recv()
        part_b[part, yp, 0] = (part_f[part, yp, 0] + far_a[part].astype(F32)).astype(BF16)
        part_b[part, yp, 1] = part_f[part, yp, 1].astype(BF16)
        out.append(remote(part_b.at[part, yp], near_m.at[part], at_blk(yp, w), sends_sum))
        far[1].wait_recv()
        part_b[part, ym, 0] = part_f[part, ym, 0].astype(BF16)
        part_b[part, ym, 1] = (part_f[part, ym, 1] + far_b[part].astype(F32)).astype(BF16)
        out.append(remote(part_b.at[part, ym], near_p.at[part], at_blk(ym, w), sends_sum))
        return out

    def reduce_own(part, left, right):
        low, high = own_sums(left, right)
        part_f[part, y, 0] = low
        part_f[part, y, 1] = high

    sends_sum = Sends()
    far_v = reduce_first(1, p_t, dosn)
    reduce_middle(1, p_t, dosn)

    sends_do.wait()
    def grads_half(half, carry):
        blocks = y + half * (7 - 2 * y) + 1
        deltas = [del_s[4 * half + h, pl.ds(0, 1)] for h in range(4)]

        def grads(j, carry):
            slot = 4 * half + j
            for h in range(4):
                ds = p_f[slot, h] * (dp_s[slot, h] - deltas[h])
                ds_t[slot, :, pl.ds(256 * h, 256)] = ds.astype(BF16)
            return carry

        return lax.fori_loop(0, blocks, grads, carry)

    lax.fori_loop(0, 2, grads_half, 0)

    far_k = reduce_first(0, ds_t, qsn)
    reduce_middle(0, ds_t, qsn)
    near_v = reduce_second(1, far_v)
    reduce_own(1, p_t, dosn)
    reduce_own(0, ds_t, qsn)
    near_k = reduce_second(0, far_k)
    def transpose_k(j, carry):
        kt[j] = kv[tile(j, 256), pl.ds(0, 128)].T
        return carry

    lax.fori_loop(0, 8, transpose_k, 0, unroll=2)

    def query_half(half, carry):
        blocks = y + half * (7 - 2 * y) + 1
        dqacc[...] = jnp.zeros_like(dqacc)

        def one(j, carry):
            for h in range(4):
                dqacc[h] += nn(kt[j], ds_t[4 * half + j, :, pl.ds(256 * h, 256)])
            return carry

        lax.fori_loop(0, blocks, one, 0)
        for h in range(4):
            dq = dqacc[h] * (inv_s[4 * half + h, pl.ds(0, 1)] * scale)
            dq = dq.T.astype(BF16)
            for ww in range(4):
                dqbuf[ww, tile(half, 64), pl.ds(128 * h, 128)] = dq[64 * ww : 64 * ww + 64]
        return carry

    lax.fori_loop(0, 2, query_half, 0)
    sends_out, far_out = Sends(), Arrivals()
    own_out = [local(dqbuf.at[w], dq_out.at[:, tile(w, 512)])]
    for d in (2, 1, 3):
        ww = (w + d) % 4
        dst = dq_out.at[:, tile(w, 512)]
        remote(dqbuf.at[ww], dst, at_blk(y, ww), sends_out, far_out)
    for copy in near_v:
        copy.wait_recv()

    def gathered(part, half):
        own = part_f[part, y, half]
        return own + near_m[part, half].astype(F32) + near_p[part, half].astype(F32)

    for half in range(2):
        value_grad = gathered(1, half).astype(BF16)
        for ww in range(4):
            at = 64 * ww if half == 0 else 64 * (3 - ww)
            rows_at = pl.ds(128 * ww + 64 * half, 64)
            gbuf[0, rows_at, pl.ds(128, 128)] = value_grad[at : at + 64]

    low_rows, high_rows = pl.ds(0, 256), pl.ds(256, 256)

    def gather_near(part):
        lanes = pl.ds(128 * part, 128)
        low, high = gbuf.at[0, low_rows, lanes], gbuf.at[0, high_rows, lanes]
        plus = remote(low, gbuf.at[3, low_rows, lanes], at_x(xp), sends_g)
        minus = remote(high, gbuf.at[1, high_rows, lanes], at_x(xm), sends_g)
        rest = remote(high, gbuf.at[3, high_rows, lanes], at_x(xp), sends_g)
        remote(low, gbuf.at[1, low_rows, lanes], at_x(xm), sends_g, rest)
        return plus, minus, rest

    def gather_far(part, near):
        lanes = pl.ds(128 * part, 128)
        near[0].wait_recv()
        src, dst = gbuf.at[3, low_rows, lanes], gbuf.at[2, low_rows, lanes]
        far = remote(src, dst, at_x(xp), sends_g)
        near[1].wait_recv()
        src, dst = gbuf.at[1, high_rows, lanes], gbuf.at[2, high_rows, lanes]
        return remote(src, dst, at_x(xm), sends_g, far)

    sends_g = Sends()
    g_v = gather_near(1)
    x_third = []

    def third_x(k):
        x_far[k].wait_recv()
        if k == 0:
            ref = xbuf.at[:, 0, w_other]
        else:
            ref = xbuf.at[(y + order[k - 1]) % 4, pl.ds(1, 3), w_other]
        x_third.append(remote(ref, ref, core_mate, sends_x))

    third_x(0)
    third_x(1)
    for copy in near_k:
        copy.wait_recv()
    for half in range(2):
        key_sum = gathered(0, half)
        key_grad = key_sum.astype(BF16)
        key_pre = (
            key_sum * cosb[half] + pltpu.roll(key_sum, 64, 1) * sinb[half]
        ).astype(BF16)
        for ww in range(4):
            at = 64 * ww if half == 0 else 64 * (3 - ww)
            gbuf[0, pl.ds(128 * ww + 64 * half, 64), pl.ds(0, 128)] = key_pre[at : at + 64]
            dkbuf[ww, pl.ds(64 * half, 64)] = key_grad[at : at + 64]
    g_k = gather_near(0)
    values_out = pl.ds(128, 128)
    own_out.append(local(dkbuf.at[w], dk_out.at[:, column]))
    own_out.append(local(gbuf.at[0, tile(w, 128), values_out], dv_out.at[:, column]))
    for d in (2, 1, 3):
        ww = (w + d) % 4
        values = gbuf.at[0, tile(ww, 128), values_out]
        remote(dkbuf.at[ww], dk_out.at[:, column], at_blk(y, ww), sends_out, far_out)
        remote(values, dv_out.at[:, column], at_blk(y, ww), sends_out, far_out)
    far_g_v = gather_far(1, g_v)
    third_x(2)

    def weights_of(part, to, rels):
        lanes = pl.ds(128 * part, 128)
        total = None
        for rel in rels:
            left = [xbuf[to, rel, ww].reshape(256, 128) for ww in range(4)]
            term = nn(jnp.concatenate(left, axis=1), gbuf[rel, :, lanes])
            total = term if total is None else total + term
        return total

    def near_tile(part, d):
        to = (y + d) % 4
        wacc[part, to] = weights_of(part, to, (0, 1, 3))

    def far_tile(part, d, arrivals=None):
        to = (y + d) % 4
        wb1[part, to] = (wacc[part, to] + weights_of(part, to, (2,))).astype(BF16)
        dst = r1.at[part, d - 1]
        return remote(wb1.at[part, to], dst, at_blk(to, w), sends_w, arrivals)

    def owner_sums(part, own, y_sums):
        total = own
        y_sums.wait_recv()
        for d in range(3):
            total = total + r1[part, d].astype(F32)
        wb1[part, y] = total.astype(BF16)
        for dz in (2, 1, 3, 0):
            zz = (zhi + dz) % 4
            for d in (2, 1, 3, 0):
                ww = (w + d) % 4
                piece = pl.ds(pl.multiple_of(64 * zz + 16 * ww, 16), 16)
                if dz or d:
                    remote(
                        wb1.at[part, y, piece], r2.at[part, zhi, w], at_owner(zz, ww),
                        sends_last, finals,
                    )
                else:
                    own_out.append(local(wb1.at[part, y, piece], r2.at[part, zhi, w]))

    sends_w, sends_last, finals = Sends(), Sends(), Arrivals()
    def wait_x(k):
        x_mate[k].wait_recv()
        x_third[k].wait_recv()

    wait_x(0)
    wait_x(1)
    g_v[2].wait_recv()
    near_tile(1, 2)
    far_g_k = gather_far(0, g_k)
    g_k[2].wait_recv()
    near_tile(0, 2)
    third_x(3)
    wait_x(2)
    near_tile(1, 1)
    near_tile(0, 1)
    far_g_v.wait_recv()
    y_sums_v = far_tile(1, 2)
    far_tile(1, 1, y_sums_v)
    wait_x(3)
    near_tile(1, 3)
    far_tile(1, 3, y_sums_v)
    near_tile(0, 3)
    third_x(4)
    far_g_k.wait_recv()
    y_sums_k = far_tile(0, 2)
    far_tile(0, 1, y_sums_k)
    far_tile(0, 3, y_sums_k)
    x_mate[4].wait_recv()
    x_third[4].wait_recv()
    own_v = weights_of(1, y, (0, 1, 2, 3))
    wacc[0, y] = weights_of(0, y, (0, 1, 2, 3))
    owner_sums(1, own_v, y_sums_v)
    owner_sums(0, wacc[0, y], y_sums_k)
    finals.wait_recv()
    for copy in own_out:
        copy.wait()
    far_out.wait_recv()
    assert count == [ARRIVALS, LOCALS, SENDS], count
    for sends in (
        sends_kv, sends_spread, sends_first, sends_x, sends_sum, sends_g, sends_out, sends_w,
        sends_last,
    ):
        sends.wait()


def place(*refs):
    sources, targets, stages = refs[:4], refs[4:8], refs[8:12]
    w_stage, sem_in, sem_out = refs[12:]
    pieces = pltpu.make_async_copy(sources[3], stages[3], sem_in.at[6])
    pieces.start()
    parts = []
    for source, target, stage in zip(sources[:3], targets[:3], stages[:3], strict=True):
        for side in range(4 if source.shape[1] == 2048 else 1):
            at = pl.ds(side * 32, 32) if source.shape[1] == 2048 else slice(None)
            i = len(parts)
            arrive = pltpu.make_async_copy(source.at[at], stage.at[at], sem_in.at[i])
            arrive.start()
            leave = pltpu.make_async_copy(stage.at[at], target.at[at], sem_out.at[i])
            parts.append((arrive, leave))
    pieces.wait()
    for part in range(2):
        for ww in range(4):
            total = stages[3][part, 0, ww].astype(F32)
            for zz in range(1, 4):
                total = total + stages[3][part, zz, ww].astype(F32)
            w_stage[:, pl.ds(512 * part + 128 * ww, 128)] = total
    last = pltpu.make_async_copy(w_stage, targets[3], sem_out.at[6])
    last.start()
    for arrive, leave in parts:
        arrive.wait()
        leave.start()
    for _, leave in parts:
        leave.wait()
    last.wait()


def body(queries, keys, values, out_grad, layer_input, lengths):
    anywhere = pl.BlockSpec(memory_space=pltpu.HBM)
    vmem = pltpu.VMEM
    shapes = (
        jax.ShapeDtypeStruct((128, 2048), BF16),
        jax.ShapeDtypeStruct((128, 512), BF16),
        jax.ShapeDtypeStruct((128, 512), BF16),
        jax.ShapeDtypeStruct((2, 4, 4, 16, 128), BF16),
    )
    weight = jax.ShapeDtypeStruct((16, 1024), F32)
    outs = pl.pallas_call(
        kernel,
        out_shape=shapes,
        in_specs=[pl.BlockSpec(memory_space=pltpu.SMEM)] + [anywhere] * 5,
        out_specs=(anywhere,) * 4,
        scratch_shapes=[
            vmem((2, 128, 512), BF16),
            vmem((4, 128, 512), BF16),
            vmem((4, 128, 512), BF16),
            vmem((2048, 256), BF16),
            vmem((128, 4096), BF16),
            vmem((4, 4, 4, 64, 128), BF16),
            vmem((4, 4, 4, 4, 64, 128), BF16),
            vmem((8, 256, 128), BF16),
            vmem((8, 256, 128), BF16),
            vmem((8, 256, 128), BF16),
            vmem((8, 256, 128), BF16),
            vmem((8, 128, 256), BF16),
            vmem((12, 4, 256, 256), F32),
            vmem((12, 4, 256, 256), F32),
            vmem((12, 256, 1024), BF16),
            vmem((12, 256, 1024), BF16),
            vmem((8, 8, 256), F32),
            vmem((8, 8, 256), F32),
            vmem((8, 8, 256), F32),
            vmem((4, 128, 256), F32),
            vmem((4, 128, 512), BF16),
            vmem((2, 4, 2, 256, 128), F32),
            vmem((2, 4, 2, 256, 128), BF16),
            vmem((2, 256, 128), BF16),
            vmem((2, 256, 128), BF16),
            vmem((2, 2, 256, 128), BF16),
            vmem((2, 2, 256, 128), BF16),
            vmem((4, 512, 256), BF16),
            vmem((4, 128, 128), BF16),
            vmem((2, 256, 128), F32),
            vmem((2, 256, 128), F32),
            vmem((2, 4, 256, 128), F32),
            vmem((2, 4, 256, 128), BF16),
            vmem((2, 3, 256, 128), BF16),
            pltpu.SemaphoreType.DMA((SENDS,)),
            pltpu.SemaphoreType.DMA((ARRIVALS,)),
            pltpu.SemaphoreType.DMA((LOCALS,)),
        ],
        compiler_params=pltpu.CompilerParams(
            collective_id=0, has_side_effects=True, vmem_limit_bytes=62 * 1024 * 1024
        ),
        name="attention_backward",
    )(lengths[0], queries[0], out_grad[0], keys[0], values[0], layer_input[0])
    outs = pl.pallas_call(
        place,
        out_shape=(*shapes[:3], weight),
        in_specs=[anywhere] * 4,
        out_specs=(anywhere,) * 4,
        scratch_shapes=[vmem(shape.shape, shape.dtype) for shape in shapes]
        + [vmem((16, 1024), F32), pltpu.SemaphoreType.DMA((7,)), pltpu.SemaphoreType.DMA((7,))],
        name="place_outputs",
    )(*outs)
    return (outs[0][None], outs[1][None], outs[2][None], outs[3])


def solution(mesh):
    placed = (P("dp", "blk", None),) * 5 + (P("dp", None),)
    return jax.shard_map(
        body,
        mesh=mesh,
        in_specs=placed,
        out_specs=(P("dp", "blk", None),) * 3 + (P(("dp", "blk"), None),),
        check_vma=False,
    )
```
